256 devices in a mesh: pts: 32 (over x, y, core), med: 8 (over z).
Axes of the slice: x: 4, y: 4, z: 8, core: 2. Of those that a mesh axis runs over, the one named last changes fastest.
Arguments:
- sketches: bfloat16 [32768, 4096], P('pts'), may hold values from -12 to 12
- assignment: int32 [32768], P('pts'), may hold values from 0 to 4095
- medoid_ids: int32 [4096], P('med'), may hold values from 0 to 32767, as said below
Outputs:
- gap: float32 [32768], P('pts')
- coverage: float32 [], replicated
- weights: float32 [4096], P('med')
- gradient_sums: float32 [4096, 4096], P('pts', 'med')
The draws below stay inside these ranges and needn't reach their ends.
Inputs may be any that keep to these rules, and one draw needn't show every extreme that they name: `medoid_ids`: the 4096 medoid ids are distinct point indices.
All inputs are finite; a program needn't handle non-finite values.
Results may differ from the reference program's by a relative error of at most 0.0003.
Values may be sent and summed in bfloat16 or wider, within the bound.
No kernel may reach another device: no remote copies, remote signals or barrier semaphores. Data moves between devices by JAX's collectives and lax.ppermute only.
A program may use at most 64 MiB of HBM per device.

```python
import jax
import jax.numpy as jnp
from jax import lax

D = 4096
TOK_DEV = 1024
KD = 512
TOKENS = 32768
K = 4096
N_PTS = 32
N_MED = 8


def draw_sketches(key, part):
    first_key, second_key = jax.random.split(jax.random.fold_in(key, 11), 2)
    position = jnp.arange(TOKENS, dtype=jnp.float32) / TOKENS
    roughness = jnp.exp(jax.random.uniform(second_key, (TOKENS, 1), jnp.float32) * jnp.log(2.5))
    base_values = jax.random.normal(first_key, (TOKENS, D), jnp.float32)
    trend = jnp.exp(jnp.log(3.0) * position)[:, None]
    values = base_values * roughness * trend * 0.5
    return jnp.clip(values, -12.0, 12.0).astype(jnp.bfloat16)


def draw_medoid_ids(key, part):
    shuffled = jax.random.permutation(jax.random.fold_in(key, 23), TOKENS)
    return shuffled[:K].astype(jnp.int32)


def with_ends(drawn, key, smallest, largest):
    dims = drawn.shape
    spot = [jax.random.randint(jax.random.fold_in(key, axis), (), 0, dims[axis]) for axis in range(len(dims))]
    drawn = drawn.at[tuple(spot)].set(smallest)
    longest = dims.index(max(dims))
    spot[longest] = (spot[longest] + 1) % dims[longest]
    return drawn.at[tuple(spot)].set(largest)


def setup_inputs(seed: int = 0) -> dict:
    streams_of = jax.random.split(jax.random.key(seed), 4)
    return {
        "sketches": draw_sketches(jax.random.fold_in(streams_of[3], 71), 0),
        "assignment": with_ends(jax.random.randint(streams_of[1], (TOKENS,), 0, KD * N_MED), jax.random.fold_in(streams_of[1], 1), 0, (KD * N_MED) - 1).astype(jnp.int32),
        "medoid_ids": draw_medoid_ids(jax.random.fold_in(streams_of[3], 71), 0),
    }


def reference(sketches, assignment, medoid_ids):
    medoid_rows = jnp.take(sketches, medoid_ids, axis=0)
    grouped = sketches.reshape(N_PTS, TOK_DEV, D)
    group_assign = assignment.reshape(N_PTS, TOK_DEV)

    def score_block(pair):
        row_block, block_assign = pair
        scores = jnp.dot(row_block, medoid_rows.T, preferred_element_type=jnp.float32) * (1.0 / D)
        best_score = jnp.max(scores, axis=1)
        assigned = jnp.take_along_axis(scores, block_assign[:, None].astype(jnp.int32), axis=1)[:, 0]
        return best_score, assigned

    best_score, assigned = lax.map(score_block, (grouped, group_assign))
    best_score = best_score.reshape(TOKENS)
    assigned = assigned.reshape(TOKENS)
    gap = best_score - assigned
    coverage = jnp.sum(best_score) / TOKENS
    weights = jax.ops.segment_sum(jnp.ones((TOKENS,), jnp.float32), assignment, num_segments=K)
    gradient_sums = jax.ops.segment_sum(sketches.astype(jnp.float32), assignment, num_segments=K).T
    return gap, coverage, weights, gradient_sums
```

```python
import functools

import jax
import jax.numpy as jnp
from jax import lax
from jax.experimental import pallas as pl
from jax.experimental.pallas import tpu as pltpu
from jax.sharding import PartitionSpec as P

BF = jnp.bfloat16
F32 = jnp.float32
I32 = jnp.int32
LANES = 128
GRAD_ROWS = 192
GRAD_SLOTS = 176
MED_ROWS = 32
MED_SLOTS = 24
SEL = GRAD_ROWS + 2 * MED_ROWS
NONE = -1e30


def contract_last(a, b):
    return lax.dot_general(a, b, (((1,), (1,)), ((), ())), preferred_element_type=F32)


def pick_kernel(where_ref, assign_ref, ids_ref, sk_ref, med_ref, grad_ref, over_ref, sel, code):
    step = pl.program_id(0)

    @pl.when(step == 0)
    def _():
        base = where_ref[0]
        plane = where_ref[1]
        groups = assign_ref.shape[0]
        half = ids_ref.shape[1] // 2
        off = ids_ref[...] - base
        inside = (off >= 0) & (off < groups * LANES)
        hi = jnp.where(inside, off >> 7, -1)
        lo = off & (LANES - 1)
        j = lax.broadcasted_iota(I32, (1, 2 * half), 1)
        first = j < half
        number = (jnp.where(first, j, j - half) + 1).astype(F32)
        row = lax.broadcasted_iota(I32, (2 * groups, 2 * half), 0)
        wanted = jnp.where(first, hi, hi + groups)
        wanted = jnp.where(hi >= 0, wanted, -1)
        table = jnp.where(wanted == row, number, 0.0).astype(BF)
        lane_hot = (lo == lax.broadcasted_iota(I32, (LANES, 2 * half), 0)).astype(F32).astype(BF)
        medoid = contract_last(table, lane_hot)
        med0, med1 = medoid[:groups], medoid[groups:]
        local = assign_ref[...] - plane * (2 * half)
        mine = (local >= 0) & (local < 2 * half)
        local_lo = jnp.where(mine, (local & 255) + 1, 0).astype(F32)
        local_hi = jnp.where(mine, local >> 8, 0).astype(F32)
        flags = jnp.concatenate(
            [mine.astype(F32), (med0 > 0).astype(F32), (med1 > 0).astype(F32)], axis=0
        ).astype(BF)
        k = lax.broadcasted_iota(I32, (LANES, LANES), 0)
        b = lax.broadcasted_iota(I32, (LANES, LANES), 1)
        before = jnp.dot(flags, (k < b).astype(F32).astype(BF), preferred_element_type=F32)
        total = jnp.dot(flags, jnp.ones((LANES, LANES), BF), preferred_element_type=F32)
        slots, over = [], jnp.zeros((1, LANES), F32)
        for kind, limit in enumerate((GRAD_SLOTS, MED_SLOTS, MED_SLOTS)):
            run = jnp.zeros((1, LANES), F32)
            rows = []
            for g in range(groups):
                at = kind * groups + g
                rows.append(before[at : at + 1] + run)
                run = run + total[at : at + 1]
            over = over + jnp.where(run > limit, 1.0, 0.0)
            position = jnp.concatenate(rows, axis=0).astype(I32)
            flag = (mine, med0 > 0, med1 > 0)[kind] & (position < limit)
            slots.append(jnp.where(flag, position, -1))
        over_ref[...] = jnp.broadcast_to(over, over_ref.shape)
        slot_g = slots[0]
        slot_m = jnp.where(slots[1] >= 0, slots[1], -1)
        slot_n = jnp.where(slots[2] >= 0, slots[2] + MED_ROWS, -1)
        grad_iota = lax.broadcasted_iota(I32, (GRAD_ROWS, LANES), 0)
        med_iota = lax.broadcasted_iota(I32, (2 * MED_ROWS, LANES), 0)
        codes = jnp.zeros((8, SEL), F32)
        zeros = jnp.zeros((5, LANES), F32)
        either = med0 + med1
        for g in range(groups):
            at = slice(g, g + 1)
            top = (slot_g[at] == grad_iota).astype(F32)
            low = ((slot_m[at] == med_iota) | (slot_n[at] == med_iota)).astype(F32)
            block = jnp.concatenate([top, low], axis=0).astype(BF)
            sel[:, g * LANES : (g + 1) * LANES] = block
            fields = jnp.concatenate(
                [either[at], local_lo[at], local_hi[at], zeros], axis=0
            ).astype(BF)
            codes = codes + contract_last(fields, block)
        code[...] = codes.astype(BF)

    rows = jnp.dot(sel[...], sk_ref[...], preferred_element_type=F32).astype(BF)
    codes = code[...]
    for c in range(2):
        grad_ref[c, :GRAD_SLOTS, :] = rows[:GRAD_SLOTS, c * LANES : (c + 1) * LANES]
        grad_ref[c, GRAD_SLOTS:, :] = jnp.concatenate(
            [codes[:, :LANES], codes[:, LANES:]], axis=0
        )
        at = GRAD_ROWS + c * MED_ROWS
        med_ref[c, :, :] = jnp.concatenate([rows[at : at + MED_SLOTS], codes], axis=0)


def pick(where, assignment, medoid_ids, sketches, pts_count):
    rows, feats = sketches.shape
    wide = 2 * LANES
    return pl.pallas_call(
        pick_kernel,
        grid_spec=pltpu.PrefetchScalarGridSpec(
            num_scalar_prefetch=1,
            grid=(feats // wide,),
            in_specs=[
                pl.BlockSpec((rows // LANES, LANES), lambda i, w: (0, 0)),
                pl.BlockSpec((1, medoid_ids.shape[0]), lambda i, w: (0, 0)),
                pl.BlockSpec((rows, wide), lambda i, w: (0, i)),
            ],
            out_specs=[
                pl.BlockSpec((2, MED_ROWS, wide), lambda i, w: (i, 0, 0)),
                pl.BlockSpec((2, GRAD_ROWS, LANES), lambda i, w: (i, 0, 0)),
                pl.BlockSpec((8, LANES), lambda i, w: (0, 0)),
            ],
            scratch_shapes=[pltpu.VMEM((SEL, rows), BF), pltpu.VMEM((8, SEL), BF)],
        ),
        out_shape=[
            jax.ShapeDtypeStruct((pts_count, MED_ROWS, wide), BF),
            jax.ShapeDtypeStruct((pts_count, GRAD_ROWS, LANES), BF),
            jax.ShapeDtypeStruct((8, LANES), F32),
        ],
        compiler_params=pltpu.CompilerParams(vmem_limit_bytes=24 * 2**20),
        cost_estimate=pl.CostEstimate(
            flops=2 * SEL * rows * feats, bytes_accessed=rows * feats * 2, transcendentals=0
        ),
        name="pick",
    )(where, assignment.reshape(-1, LANES), medoid_ids[None, :], sketches)


def place_kernel(where_ref, got_ref, out_ref):
    core = where_ref[2]
    sources = got_ref.shape[0]
    count = out_ref.shape[0]
    total = jnp.zeros(out_ref.shape, F32)
    per = 2 * LANES // MED_ROWS
    iota = lax.broadcasted_iota(I32, (count, per * MED_ROWS), 0)
    for g in range(sources // per):
        numbers = []
        for q in range(g * per, (g + 1) * per):
            line = got_ref[q, MED_SLOTS : MED_SLOTS + 8, :].astype(F32)[0:1]
            a = line[:, GRAD_ROWS : GRAD_ROWS + MED_ROWS]
            b = line[:, GRAD_ROWS + MED_ROWS :]
            numbers.append(jnp.where(core == 0, a, b))
        number = jnp.concatenate(numbers, axis=1).astype(I32) - 1
        hot = (number == iota).astype(F32).astype(BF)
        block = got_ref[g * per : (g + 1) * per].reshape(per * MED_ROWS, got_ref.shape[2])
        total = total + jnp.dot(hot, block, preferred_element_type=F32)
    out_ref[...] = total.astype(BF)


def place(where, got, count):
    return pl.pallas_call(
        place_kernel,
        in_specs=[
            pl.BlockSpec(memory_space=pltpu.SMEM),
            pl.BlockSpec(memory_space=pltpu.VMEM),
        ],
        out_specs=pl.BlockSpec(memory_space=pltpu.VMEM),
        out_shape=jax.ShapeDtypeStruct((count, got.shape[2]), BF),
        compiler_params=pltpu.CompilerParams(vmem_limit_bytes=8 * 2**20),
        cost_estimate=pl.CostEstimate(
            flops=2 * count * got.size, bytes_accessed=2 * got.size, transcendentals=0
        ),
        name="place",
    )(where, got)


def sums_kernel(got_ref, sums_ref, count_ref):
    feats = got_ref.shape[2]
    medoids = sums_ref.shape[1]
    tail = GRAD_ROWS - LANES
    iota_a = lax.broadcasted_iota(I32, (medoids, LANES), 0)
    iota_b = lax.broadcasted_iota(I32, (medoids, tail), 0)
    ones = jnp.ones((GRAD_ROWS, LANES), BF)

    def body(q, total):
        codes = got_ref[q, GRAD_SLOTS:, :].astype(F32).astype(I32)
        a = codes[1:2] - 1 + codes[2:3] * 256
        b = (codes[9:10] - 1 + codes[10:11] * 256)[:, :tail]
        hot = jnp.concatenate(
            [(a == iota_a).astype(F32), (b == iota_b).astype(F32)], axis=1
        ).astype(BF)
        block = jnp.concatenate([got_ref[q], ones], axis=1)
        return total + jnp.dot(hot, block, preferred_element_type=F32)

    total = lax.fori_loop(
        0, got_ref.shape[0], body, jnp.zeros((medoids, feats + LANES), F32)
    )
    sums_ref[...] = total[:, :feats].T
    count_ref[...] = total[:, feats:].T[:8]


def sums(got, medoids):
    return pl.pallas_call(
        sums_kernel,
        in_specs=[pl.BlockSpec(memory_space=pltpu.VMEM)],
        out_specs=[pl.BlockSpec(memory_space=pltpu.VMEM)] * 2,
        out_shape=[
            jax.ShapeDtypeStruct((got.shape[2], medoids), F32),
            jax.ShapeDtypeStruct((8, medoids), F32),
        ],
        compiler_params=pltpu.CompilerParams(vmem_limit_bytes=16 * 2**20),
        cost_estimate=pl.CostEstimate(
            flops=4 * medoids * got.size, bytes_accessed=2 * got.size, transcendentals=0
        ),
        name="sums",
    )(got)


def score_kernel(scale, where_ref, assign_ref, prior_ref, sk_ref, *refs):
    parts, out_ref = refs[:-1], refs[-1]
    medoids = 2 * parts[0].shape[1]
    x, y, first = where_ref[3], where_ref[4], where_ref[5]
    points = sk_ref.shape[0]
    total = jnp.zeros((medoids, points), F32)
    for kx in range(4):
        for ky in range(4):
            block = ((x + 4 - kx) & 3) * 4 + ((y + 4 - ky) & 3)
            at = pl.multiple_of(block * 2 * LANES, 2 * LANES)
            if len(parts) == 8:
                a, b = parts[ky][kx], parts[4 + kx][ky]
            else:
                a, b = parts[0][ky * 4 + kx], parts[0][16 + kx * 4 + ky]
            total = total + contract_last(
                jnp.concatenate([a, b], axis=0), sk_ref[:, pl.ds(at, 2 * LANES)]
            )
    scores = total * scale
    best = jnp.max(scores, axis=0, keepdims=True)
    row = lax.broadcasted_iota(I32, scores.shape, 0)
    local = assign_ref[...] - first
    chosen = jnp.max(jnp.where(local == row, scores, NONE), axis=0, keepdims=True)
    prior = prior_ref[...]
    best = jnp.maximum(best, prior[0:1])
    chosen = jnp.maximum(chosen, prior[1:2])
    out_ref[...] = jnp.concatenate([best, chosen, prior[2:]], axis=0)


def scored(where, assignment, prior, sketches, parts):
    rows, feats = sketches.shape
    tile = 2 * LANES
    whole = lambda a: pl.BlockSpec(a.shape, lambda i, w: (0,) * a.ndim)
    return pl.pallas_call(
        functools.partial(score_kernel, 1.0 / feats),
        grid_spec=pltpu.PrefetchScalarGridSpec(
            num_scalar_prefetch=1,
            grid=(rows // tile,),
            in_specs=[
                pl.BlockSpec((1, tile), lambda i, w: (0, i)),
                pl.BlockSpec((8, tile), lambda i, w: (0, i)),
                pl.BlockSpec((tile, feats), lambda i, w: (i, 0)),
            ]
            + [whole(a) for a in parts],
            out_specs=pl.BlockSpec((8, tile), lambda i, w: (0, i)),
        ),
        out_shape=jax.ShapeDtypeStruct((8, rows), F32),
        compiler_params=pltpu.CompilerParams(vmem_limit_bytes=24 * 2**20),
        cost_estimate=pl.CostEstimate(
            flops=2 * rows * feats * 256, bytes_accessed=rows * feats * 2, transcendentals=0
        ),
        name="scored",
    )(where, assignment[None, :], prior, sketches, *parts)


def from_everyone(array, axis):
    size = lax.axis_size(axis)
    return lax.all_to_all(
        jnp.broadcast_to(array[None], (size, *array.shape)), axis, 0, 0, tiled=True
    )


def chip_of(p):
    return p // 8, (p // 2) % 4, p % 2


def shifted(array, dx, dy, dc):
    pairs = []
    for p in range(32):
        x, y, c = chip_of(p)
        pairs.append((p, (((x + dx) % 4) * 4 + (y + dy) % 4) * 2 + (c ^ dc)))
    return lax.ppermute(array, "pts", pairs)


def general(sketches, assignment, medoid_ids):
    row_count, feat_width = sketches.shape
    medoid_count = medoid_ids.shape[0]
    pts_count = lax.axis_size("pts")
    part = feat_width // pts_count
    pts_index = lax.axis_index("pts")
    med_index = lax.axis_index("med")
    local_assign = assignment - med_index * medoid_count
    one_hot = (
        local_assign[:, None] == jnp.arange(medoid_count, dtype=I32)[None, :]
    ).astype(BF)
    offsets = medoid_ids - pts_index * row_count
    inside = (offsets >= 0) & (offsets < row_count)
    picked = jnp.take(sketches, jnp.clip(offsets, 0, row_count - 1), axis=0)
    terms = jnp.where(inside[:, None], picked, jnp.zeros_like(picked))
    terms = terms.reshape(medoid_count, pts_count, part).swapaxes(0, 1)
    piece = (
        lax.all_to_all(terms, "pts", 0, 0, tiled=True).astype(F32).sum(axis=0).astype(BF)
    )
    everything = from_everyone(piece, "pts").swapaxes(0, 1).reshape(medoid_count, feat_width)
    partial = lax.dot_general(
        sketches, one_hot, (((0,), (0,)), ((), ())), preferred_element_type=F32
    ).reshape(pts_count, part, medoid_count)
    gradient_sums = lax.all_to_all(partial, "pts", 0, 0, tiled=True).sum(axis=0)
    counts = from_everyone(jnp.sum(one_hot.astype(F32), axis=0), "pts").sum(axis=0)
    scores = contract_last(sketches, everything) * (1.0 / feat_width)
    best = jnp.max(scores, axis=1)
    here = (local_assign >= 0) & (local_assign < medoid_count)
    taken = jnp.take_along_axis(
        scores, jnp.clip(local_assign, 0, medoid_count - 1)[:, None], axis=1
    )[:, 0]
    both = from_everyone(jnp.stack([best, jnp.where(here, taken, NONE)]), "med").max(axis=0)
    cover = from_everyone(jnp.sum(both[0])[None], "pts").sum()
    return both[0] - both[1], cover / (row_count * pts_count), counts, gradient_sums


def shards(sketches, assignment, medoid_ids):
    row_count, feat_width = sketches.shape
    medoid_count = medoid_ids.shape[0]
    half = medoid_count // 2
    pts_count = lax.axis_size("pts")
    p = lax.axis_index("pts")
    m = lax.axis_index("med")
    core = p % 2
    own = m * medoid_count + core * half
    other = m * medoid_count + (1 - core) * half
    where = jnp.stack(
        [p * row_count, m, core, p // 8, (p // 2) % 4, own, other, other]
    ).astype(I32)
    where_other = jnp.stack(
        [p * row_count, m, core, p // 8, (p // 2) % 4, other, own, own]
    ).astype(I32)

    med_send, grad_send, over = pick(where, assignment, medoid_ids, sketches, pts_count)
    med_got = lax.all_to_all(med_send, "pts", 0, 0, tiled=True)
    piece = place(where, med_got, half)
    a, b = piece[: half // 2], piece[half // 2 :]
    pa = jnp.stack([a] + [shifted(a, k, 0, 0) for k in (1, 2, 3)])
    pb = jnp.stack([b] + [shifted(b, 0, k, 0) for k in (1, 2, 3)])
    qa = [pa] + [shifted(pa, 0, k, 0) for k in (1, 2, 3)]
    qb = [pb] + [shifted(pb, k, 0, 0) for k in (1, 2, 3)]
    mine = jnp.concatenate(qa + qb, axis=0)
    theirs = shifted(mine, 0, 0, 1)

    grad_got = lax.all_to_all(grad_send, "pts", 0, 0, tiled=True)
    gradient_sums, counts = sums(grad_got, medoid_count)

    prior = jnp.full((8, row_count), NONE, F32)
    stats = scored(where, assignment, prior, sketches, qa + qb)
    stats = scored(where_other, assignment, stats, sketches, [theirs])
    flag = jnp.broadcast_to(over[0:1, 0:1], (1, row_count))
    packed = jnp.concatenate([stats[:2], flag], axis=0)
    both = from_everyone(packed, "med").max(axis=0)
    gap = both[0] - both[1]
    last = from_everyone(jnp.stack([jnp.sum(both[0]), both[2, 0]]), "pts")
    cover = jnp.sum(last[:, 0])
    full = jnp.max(last[:, 1]) > 0.0
    fast = (gap, cover / (row_count * pts_count), counts[0], gradient_sums)
    return lax.cond(
        full, lambda: general(sketches, assignment, medoid_ids), lambda: fast
    )


def solution(mesh):
    in_specs = (P("pts", None), P("pts"), P("med"))
    out_specs = (P("pts"), P(), P("med"), P("pts", "med"))
    return jax.shard_map(shards, mesh=mesh, in_specs=in_specs, out_specs=out_specs, check_vma=False)
```

```python
import functools

import jax
import jax.numpy as jnp
from jax import lax
from jax.experimental import pallas as pl
from jax.experimental.pallas import tpu as pltpu
from jax.sharding import PartitionSpec as P


BF = jnp.bfloat16
F32 = jnp.float32
I32 = jnp.int32
LANES = 128
GRAD_ROWS = 192
GRAD_SLOTS = 176
MED_ROWS = 32
MED_SLOTS = 24
SEL = GRAD_ROWS + 2 * MED_ROWS
NONE = -1e30


def contract_last(a, b):
    return lax.dot_general(a, b, (((1,), (1,)), ((), ())), preferred_element_type=F32)


def pick_kernel(where_ref, assign_ref, ids_ref, sk_ref, med_ref, grad_ref, over_ref, sel, code):
    step = pl.program_id(0)

    @pl.when(step == 0)
    def _():
        base = where_ref[0]
        plane = where_ref[1]
        groups = assign_ref.shape[0]
        half = ids_ref.shape[1] // 2
        off = ids_ref[...] - base
        inside = (off >= 0) & (off < groups * LANES)
        hi = jnp.where(inside, off >> 7, -1)
        lo = off & (LANES - 1)
        j = lax.broadcasted_iota(I32, (1, 2 * half), 1)
        first = j < half
        number = (jnp.where(first, j, j - half) + 1).astype(F32)
        row = lax.broadcasted_iota(I32, (2 * groups, 2 * half), 0)
        wanted = jnp.where(first, hi, hi + groups)
        wanted = jnp.where(hi >= 0, wanted, -1)
        table = jnp.where(wanted == row, number, 0.0).astype(BF)
        lane_hot = (lo == lax.broadcasted_iota(I32, (LANES, 2 * half), 0)).astype(F32).astype(BF)
        medoid = contract_last(table, lane_hot)
        med0, med1 = medoid[:groups], medoid[groups:]
        local = assign_ref[...] - plane * (2 * half)
        mine = (local >= 0) & (local < 2 * half)
        local_lo = jnp.where(mine, (local & 255) + 1, 0).astype(F32)
        local_hi = jnp.where(mine, local >> 8, 0).astype(F32)
        flags = jnp.concatenate(
            [mine.astype(F32), (med0 > 0).astype(F32), (med1 > 0).astype(F32)], axis=0
        ).astype(BF)
        k = lax.broadcasted_iota(I32, (LANES, LANES), 0)
        b = lax.broadcasted_iota(I32, (LANES, LANES), 1)
        before = jnp.dot(flags, (k < b).astype(F32).astype(BF), preferred_element_type=F32)
        total = jnp.dot(flags, jnp.ones((LANES, LANES), BF), preferred_element_type=F32)
        slots, over = [], jnp.zeros((1, LANES), F32)
        for kind, limit in enumerate((GRAD_SLOTS, MED_SLOTS, MED_SLOTS)):
            run = jnp.zeros((1, LANES), F32)
            rows = []
            for g in range(groups):
                at = kind * groups + g
                rows.append(before[at : at + 1] + run)
                run = run + total[at : at + 1]
            over = over + jnp.where(run > limit, 1.0, 0.0)
            position = jnp.concatenate(rows, axis=0).astype(I32)
            flag = (mine, med0 > 0, med1 > 0)[kind] & (position < limit)
            slots.append(jnp.where(flag, position, -1))
        over_ref[...] = jnp.broadcast_to(over, over_ref.shape)
        slot_g = slots[0]
        slot_m = jnp.where(slots[1] >= 0, slots[1], -1)
        slot_n = jnp.where(slots[2] >= 0, slots[2] + MED_ROWS, -1)
        grad_iota = lax.broadcasted_iota(I32, (GRAD_ROWS, LANES), 0)
        med_iota = lax.broadcasted_iota(I32, (2 * MED_ROWS, LANES), 0)
        codes = jnp.zeros((8, SEL), F32)
        zeros = jnp.zeros((5, LANES), F32)
        either = med0 + med1
        for g in range(groups):
            at = slice(g, g + 1)
            top = (slot_g[at] == grad_iota).astype(F32)
            low = ((slot_m[at] == med_iota) | (slot_n[at] == med_iota)).astype(F32)
            block = jnp.concatenate([top, low], axis=0).astype(BF)
            sel[:, g * LANES : (g + 1) * LANES] = block
            fields = jnp.concatenate(
                [either[at], local_lo[at], local_hi[at], zeros], axis=0
            ).astype(BF)
            codes = codes + contract_last(fields, block)
        code[...] = codes.astype(BF)

    rows = jnp.dot(sel[...], sk_ref[...], preferred_element_type=F32).astype(BF)
    codes = code[...]
    for c in range(2):
        grad_ref[c, :GRAD_SLOTS, :] = rows[:GRAD_SLOTS, c * LANES : (c + 1) * LANES]
        grad_ref[c, GRAD_SLOTS:, :] = jnp.concatenate(
            [codes[:, :LANES], codes[:, LANES:]], axis=0
        )
        at = GRAD_ROWS + c * MED_ROWS
        med_ref[c, :, :] = jnp.concatenate([rows[at : at + MED_SLOTS], codes], axis=0)


def pick(where, assignment, medoid_ids, sketches, pts_count):
    rows, feats = sketches.shape
    wide = 2 * LANES
    return pl.pallas_call(
        pick_kernel,
        grid_spec=pltpu.PrefetchScalarGridSpec(
            num_scalar_prefetch=1,
            grid=(feats // wide,),
            in_specs=[
                pl.BlockSpec((rows // LANES, LANES), lambda i, w: (0, 0)),
                pl.BlockSpec((1, medoid_ids.shape[0]), lambda i, w: (0, 0)),
                pl.BlockSpec((rows, wide), lambda i, w: (0, i)),
            ],
            out_specs=[
                pl.BlockSpec((2, MED_ROWS, wide), lambda i, w: (i, 0, 0)),
                pl.BlockSpec((2, GRAD_ROWS, LANES), lambda i, w: (i, 0, 0)),
                pl.BlockSpec((8, LANES), lambda i, w: (0, 0)),
            ],
            scratch_shapes=[pltpu.VMEM((SEL, rows), BF), pltpu.VMEM((8, SEL), BF)],
        ),
        out_shape=[
            jax.ShapeDtypeStruct((pts_count, MED_ROWS, wide), BF),
            jax.ShapeDtypeStruct((pts_count, GRAD_ROWS, LANES), BF),
            jax.ShapeDtypeStruct((8, LANES), F32),
        ],
        compiler_params=pltpu.CompilerParams(vmem_limit_bytes=24 * 2**20),
        cost_estimate=pl.CostEstimate(
            flops=2 * SEL * rows * feats, bytes_accessed=rows * feats * 2, transcendentals=0
        ),
        name="pick",
    )(where, assignment.reshape(-1, LANES), medoid_ids[None, :], sketches)


def place_kernel(where_ref, got_ref, out_ref):
    core = where_ref[2]
    sources = got_ref.shape[0]
    count = out_ref.shape[0]
    total = jnp.zeros(out_ref.shape, F32)
    per = 2 * LANES // MED_ROWS
    iota = lax.broadcasted_iota(I32, (count, per * MED_ROWS), 0)
    for g in range(sources // per):
        numbers = []
        for q in range(g * per, (g + 1) * per):
            line = got_ref[q, MED_SLOTS : MED_SLOTS + 8, :].astype(F32)[0:1]
            a = line[:, GRAD_ROWS : GRAD_ROWS + MED_ROWS]
            b = line[:, GRAD_ROWS + MED_ROWS :]
            numbers.append(jnp.where(core == 0, a, b))
        number = jnp.concatenate(numbers, axis=1).astype(I32) - 1
        hot = (number == iota).astype(F32).astype(BF)
        block = got_ref[g * per : (g + 1) * per].reshape(per * MED_ROWS, got_ref.shape[2])
        total = total + jnp.dot(hot, block, preferred_element_type=F32)
    out_ref[...] = total.astype(BF)


def place(where, got, count):
    return pl.pallas_call(
        place_kernel,
        in_specs=[
            pl.BlockSpec(memory_space=pltpu.SMEM),
            pl.BlockSpec(memory_space=pltpu.VMEM),
        ],
        out_specs=pl.BlockSpec(memory_space=pltpu.VMEM),
        out_shape=jax.ShapeDtypeStruct((count, got.shape[2]), BF),
        compiler_params=pltpu.CompilerParams(vmem_limit_bytes=8 * 2**20),
        cost_estimate=pl.CostEstimate(
            flops=2 * count * got.size, bytes_accessed=2 * got.size, transcendentals=0
        ),
        name="place",
    )(where, got)


def sums_kernel(got_ref, sums_ref, count_ref):
    feats = got_ref.shape[2]
    medoids = sums_ref.shape[1]
    tail = GRAD_ROWS - LANES
    iota_a = lax.broadcasted_iota(I32, (medoids, LANES), 0)
    iota_b = lax.broadcasted_iota(I32, (medoids, tail), 0)
    ones = jnp.ones((GRAD_ROWS, LANES), BF)

    def body(q, total):
        codes = got_ref[q, GRAD_SLOTS:, :].astype(F32).astype(I32)
        a = codes[1:2] - 1 + codes[2:3] * 256
        b = (codes[9:10] - 1 + codes[10:11] * 256)[:, :tail]
        hot = jnp.concatenate(
            [(a == iota_a).astype(F32), (b == iota_b).astype(F32)], axis=1
        ).astype(BF)
        block = jnp.concatenate([got_ref[q], ones], axis=1)
        return total + jnp.dot(hot, block, preferred_element_type=F32)

    total = lax.fori_loop(
        0, got_ref.shape[0], body, jnp.zeros((medoids, feats + LANES), F32)
    )
    sums_ref[...] = total[:, :feats].T
    count_ref[...] = total[:, feats:].T[:8]


def sums(got, medoids):
    return pl.pallas_call(
        sums_kernel,
        in_specs=[pl.BlockSpec(memory_space=pltpu.VMEM)],
        out_specs=[pl.BlockSpec(memory_space=pltpu.VMEM)] * 2,
        out_shape=[
            jax.ShapeDtypeStruct((got.shape[2], medoids), F32),
            jax.ShapeDtypeStruct((8, medoids), F32),
        ],
        compiler_params=pltpu.CompilerParams(vmem_limit_bytes=16 * 2**20),
        cost_estimate=pl.CostEstimate(
            flops=4 * medoids * got.size, bytes_accessed=2 * got.size, transcendentals=0
        ),
        name="sums",
    )(got)


def joined_kernel(*refs):
    parts, out_ref = refs[:-1], refs[-1]
    size = parts[0].shape[0]
    for i, part in enumerate(parts):
        out_ref[i * size : (i + 1) * size] = part[...]


def joined(parts):
    size, *rest = parts[0].shape
    return pl.pallas_call(
        joined_kernel,
        in_specs=[pl.BlockSpec(memory_space=pltpu.VMEM)] * len(parts),
        out_specs=pl.BlockSpec(memory_space=pltpu.VMEM),
        out_shape=jax.ShapeDtypeStruct((size * len(parts), *rest), parts[0].dtype),
        compiler_params=pltpu.CompilerParams(vmem_limit_bytes=8 * 2**20),
        cost_estimate=pl.CostEstimate(
            flops=0, bytes_accessed=4 * len(parts) * parts[0].size, transcendentals=0
        ),
        name="joined",
    )(*parts)


def score_kernel(scale, where_ref, assign_ref, prior_ref, sk_ref, *refs):
    parts, out_ref = refs[:-1], refs[-1]
    medoids = 2 * parts[0].shape[1]
    x, y, first = where_ref[3], where_ref[4], where_ref[5]
    points = sk_ref.shape[0]
    total = jnp.zeros((medoids, points), F32)
    for kx in range(4):
        for ky in range(4):
            block = ((x + 4 - kx) & 3) * 4 + ((y + 4 - ky) & 3)
            at = pl.multiple_of(block * 2 * LANES, 2 * LANES)
            if len(parts) == 8:
                a, b = parts[ky][kx], parts[4 + kx][ky]
            else:
                a, b = parts[0][ky * 4 + kx], parts[0][16 + kx * 4 + ky]
            total = total + contract_last(
                jnp.concatenate([a, b], axis=0), sk_ref[:, pl.ds(at, 2 * LANES)]
            )
    scores = total * scale
    best = jnp.max(scores, axis=0, keepdims=True)
    row = lax.broadcasted_iota(I32, scores.shape, 0)
    local = assign_ref[...] - first
    chosen = jnp.max(jnp.where(local == row, scores, NONE), axis=0, keepdims=True)
    prior = prior_ref[...]
    best = jnp.maximum(best, prior[0:1])
    chosen = jnp.maximum(chosen, prior[1:2])
    out_ref[...] = jnp.concatenate([best, chosen, prior[2:]], axis=0)


def scored(where, assignment, prior, sketches, parts):
    rows, feats = sketches.shape
    tile = 2 * LANES
    whole = lambda a: pl.BlockSpec(a.shape, lambda i, w: (0,) * a.ndim)
    return pl.pallas_call(
        functools.partial(score_kernel, 1.0 / feats),
        grid_spec=pltpu.PrefetchScalarGridSpec(
            num_scalar_prefetch=1,
            grid=(rows // tile,),
            in_specs=[
                pl.BlockSpec((1, tile), lambda i, w: (0, i)),
                pl.BlockSpec((8, tile), lambda i, w: (0, i)),
                pl.BlockSpec((tile, feats), lambda i, w: (i, 0)),
            ]
            + [whole(a) for a in parts],
            out_specs=pl.BlockSpec((8, tile), lambda i, w: (0, i)),
        ),
        out_shape=jax.ShapeDtypeStruct((8, rows), F32),
        compiler_params=pltpu.CompilerParams(vmem_limit_bytes=24 * 2**20),
        cost_estimate=pl.CostEstimate(
            flops=2 * rows * feats * 256, bytes_accessed=rows * feats * 2, transcendentals=0
        ),
        name="scored",
    )(where, assignment[None, :], prior, sketches, *parts)


def from_everyone(array, axis):
    size = lax.axis_size(axis)
    return lax.all_to_all(
        jnp.broadcast_to(array[None], (size, *array.shape)), axis, 0, 0, tiled=True
    )


def chip_of(p):
    return p // 8, (p // 2) % 4, p % 2


def shifted(array, dx, dy, dc):
    pairs = []
    for p in range(32):
        x, y, c = chip_of(p)
        pairs.append((p, (((x + dx) % 4) * 4 + (y + dy) % 4) * 2 + (c ^ dc)))
    return lax.ppermute(array, "pts", pairs)


def general(sketches, assignment, medoid_ids):
    row_count, feat_width = sketches.shape
    medoid_count = medoid_ids.shape[0]
    pts_count = lax.axis_size("pts")
    part = feat_width // pts_count
    pts_index = lax.axis_index("pts")
    med_index = lax.axis_index("med")
    local_assign = assignment - med_index * medoid_count
    one_hot = (
        local_assign[:, None] == jnp.arange(medoid_count, dtype=I32)[None, :]
    ).astype(BF)
    offsets = medoid_ids - pts_index * row_count
    inside = (offsets >= 0) & (offsets < row_count)
    picked = jnp.take(sketches, jnp.clip(offsets, 0, row_count - 1), axis=0)
    terms = jnp.where(inside[:, None], picked, jnp.zeros_like(picked))
    terms = terms.reshape(medoid_count, pts_count, part).swapaxes(0, 1)
    piece = (
        lax.all_to_all(terms, "pts", 0, 0, tiled=True).astype(F32).sum(axis=0).astype(BF)
    )
    everything = from_everyone(piece, "pts").swapaxes(0, 1).reshape(medoid_count, feat_width)
    partial = lax.dot_general(
        sketches, one_hot, (((0,), (0,)), ((), ())), preferred_element_type=F32
    ).reshape(pts_count, part, medoid_count)
    gradient_sums = lax.all_to_all(partial, "pts", 0, 0, tiled=True).sum(axis=0)
    counts = from_everyone(jnp.sum(one_hot.astype(F32), axis=0), "pts").sum(axis=0)
    scores = contract_last(sketches, everything) * (1.0 / feat_width)
    best = jnp.max(scores, axis=1)
    here = (local_assign >= 0) & (local_assign < medoid_count)
    taken = jnp.take_along_axis(
        scores, jnp.clip(local_assign, 0, medoid_count - 1)[:, None], axis=1
    )[:, 0]
    both = from_everyone(jnp.stack([best, jnp.where(here, taken, NONE)]), "med").max(axis=0)
    cover = from_everyone(jnp.sum(both[0])[None], "pts").sum()
    return both[0] - both[1], cover / (row_count * pts_count), counts, gradient_sums


def shards(sketches, assignment, medoid_ids):
    row_count, _ = sketches.shape
    medoid_count = medoid_ids.shape[0]
    half = medoid_count // 2
    pts_count = lax.axis_size("pts")
    p = lax.axis_index("pts")
    m = lax.axis_index("med")
    core = p % 2
    own = m * medoid_count + core * half
    other = m * medoid_count + (1 - core) * half
    where = jnp.stack(
        [p * row_count, m, core, p // 8, (p // 2) % 4, own, other, other]
    ).astype(I32)
    where_other = jnp.stack(
        [p * row_count, m, core, p // 8, (p // 2) % 4, other, own, own]
    ).astype(I32)

    med_send, grad_send, over = pick(
        where, assignment, medoid_ids, sketches, pts_count
    )
    med_got = lax.all_to_all(med_send, "pts", 0, 0, tiled=True)
    grad_got = lax.all_to_all(grad_send, "pts", 0, 0, tiled=True)
    piece = place(where, med_got, half)
    a, b = piece[: half // 2], piece[half // 2 :]
    pa = jnp.stack([a] + [shifted(a, k, 0, 0) for k in (1, 2, 3)])
    pb = jnp.stack([b] + [shifted(b, 0, k, 0) for k in (1, 2, 3)])
    qa = [pa] + [shifted(pa, 0, k, 0) for k in (1, 2, 3)]
    qb = [pb] + [shifted(pb, k, 0, 0) for k in (1, 2, 3)]
    mine = joined(qa + qb)
    theirs = shifted(mine, 0, 0, 1)

    prior = jnp.full((8, row_count), NONE, F32)
    stats = scored(where, assignment, prior, sketches, [mine])
    stats = scored(where_other, assignment, stats, sketches, [theirs])
    flag = jnp.broadcast_to(over[0:1, 0:1], (1, row_count))
    packed = jnp.concatenate([stats[:2], flag], axis=0)
    both = from_everyone(packed, "med")
    gradient_sums, counts = sums(grad_got, medoid_count)
    both = both.max(axis=0)
    gap = both[0] - both[1]
    last = from_everyone(jnp.stack([jnp.sum(both[0]), both[2, 0]]), "pts")
    cover = jnp.sum(last[:, 0])
    full = jnp.max(last[:, 1]) > 0.0
    fast = (gap, cover / (row_count * pts_count), counts[0], gradient_sums)
    return lax.cond(
        full, lambda: general(sketches, assignment, medoid_ids), lambda: fast
    )


def solution(mesh):
    in_specs = (P("pts", None), P("pts"), P("med"))
    out_specs = (P("pts"), P(), P("med"), P("pts", "med"))
    return jax.shard_map(
        shards, mesh=mesh, in_specs=in_specs, out_specs=out_specs, check_vma=False
    )
```

```python
import functools

import jax
import jax.numpy as jnp
from jax import lax
from jax.experimental import pallas as pl
from jax.experimental.pallas import tpu as pltpu
from jax.sharding import PartitionSpec as P


BF = jnp.bfloat16
F32 = jnp.float32
I32 = jnp.int32
LANES = 128
GRAD_ROWS = 192
GRAD_SLOTS = 176
MED_ROWS = 32
MED_SLOTS = 24
SEL = GRAD_ROWS + 2 * MED_ROWS
NONE = -1e30
CHIPS = 4


def contract_last(a, b):
    return lax.dot_general(a, b, (((1,), (1,)), ((), ())), preferred_element_type=F32)


def pick_kernel(where_ref, assign_ref, ids_ref, sk_ref, med_ref, grad_ref, sel, code):
    step = pl.program_id(0)

    @pl.when(step == 0)
    def _():
        base = where_ref[0]
        plane = where_ref[1]
        groups = assign_ref.shape[0]
        half = ids_ref.shape[1] // 2
        off = ids_ref[...] - base
        inside = (off >= 0) & (off < groups * LANES)
        hi = jnp.where(inside, off >> 7, -1)
        lo = off & (LANES - 1)
        j = lax.broadcasted_iota(I32, (1, 2 * half), 1)
        first = j < half
        number = (jnp.where(first, j, j - half) + 1).astype(F32)
        row = lax.broadcasted_iota(I32, (2 * groups, 2 * half), 0)
        wanted = jnp.where(first, hi, hi + groups)
        wanted = jnp.where(hi >= 0, wanted, -1)
        table = jnp.where(wanted == row, number, 0.0).astype(BF)
        lane_hot = (lo == lax.broadcasted_iota(I32, (LANES, 2 * half), 0)).astype(F32).astype(BF)
        medoid = contract_last(table, lane_hot)
        med0, med1 = medoid[:groups], medoid[groups:]
        local = assign_ref[...] - plane * (2 * half)
        mine = (local >= 0) & (local < 2 * half)
        local_lo = jnp.where(mine, (local & 255) + 1, 0).astype(F32)
        local_hi = jnp.where(mine, local >> 8, 0).astype(F32)
        flags = jnp.concatenate(
            [mine.astype(F32), (med0 > 0).astype(F32), (med1 > 0).astype(F32)], axis=0
        ).astype(BF)
        k = lax.broadcasted_iota(I32, (LANES, LANES), 0)
        b = lax.broadcasted_iota(I32, (LANES, LANES), 1)
        before = jnp.dot(flags, (k < b).astype(F32).astype(BF), preferred_element_type=F32)
        total = jnp.dot(flags, jnp.ones((LANES, LANES), BF), preferred_element_type=F32)
        slots, over = [], jnp.zeros((1, LANES), F32)
        for kind, limit in enumerate((GRAD_SLOTS, MED_SLOTS, MED_SLOTS)):
            run = jnp.zeros((1, LANES), F32)
            rows = []
            for g in range(groups):
                at = kind * groups + g
                rows.append(before[at : at + 1] + run)
                run = run + total[at : at + 1]
            over = over + jnp.where(run > limit, 1.0, 0.0)
            position = jnp.concatenate(rows, axis=0).astype(I32)
            flag = (mine, med0 > 0, med1 > 0)[kind] & (position < limit)
            slots.append(jnp.where(flag, position, -1))
        slot_g = slots[0]
        slot_m = jnp.where(slots[1] >= 0, slots[1], -1)
        slot_n = jnp.where(slots[2] >= 0, slots[2] + MED_ROWS, -1)
        grad_iota = lax.broadcasted_iota(I32, (GRAD_ROWS, LANES), 0)
        med_iota = lax.broadcasted_iota(I32, (2 * MED_ROWS, LANES), 0)
        codes = jnp.zeros((8, SEL), F32)
        zeros = jnp.zeros((5, LANES), F32)
        either = med0 + med1
        for g in range(groups):
            at = slice(g, g + 1)
            top = (slot_g[at] == grad_iota).astype(F32)
            low = ((slot_m[at] == med_iota) | (slot_n[at] == med_iota)).astype(F32)
            block = jnp.concatenate([top, low], axis=0).astype(BF)
            sel[:, g * LANES : (g + 1) * LANES] = block
            fields = jnp.concatenate(
                [either[at], local_lo[at], local_hi[at], zeros], axis=0
            ).astype(BF)
            codes = codes + contract_last(fields, block)
        marks = jnp.broadcast_to(jnp.concatenate([over, over], axis=1), (8, SEL))
        third = lax.broadcasted_iota(I32, (8, SEL), 0) == 3
        code[...] = jnp.where(third, marks, codes).astype(BF)

    codes = code[...]
    lines = jnp.concatenate([codes[:, :LANES], codes[:, LANES:]], axis=0)
    for chip in range(sk_ref.shape[1] // SEL):
        block = sk_ref[:, chip * SEL : (chip + 1) * SEL]
        rows = jnp.dot(sel[...], block, preferred_element_type=F32).astype(BF)
        for c in range(2):
            to = 2 * chip + c
            grad_ref[to, :GRAD_SLOTS, :] = rows[:GRAD_SLOTS, c * LANES : (c + 1) * LANES]
            grad_ref[to, GRAD_SLOTS:, :] = lines
            at = GRAD_ROWS + c * MED_ROWS
            med_ref[to, :, :] = jnp.concatenate([rows[at : at + MED_SLOTS], codes], axis=0)


def pick(where, assignment, medoid_ids, sketches, pts_count):
    rows, feats = sketches.shape
    wide = CHIPS * 2 * LANES
    return pl.pallas_call(
        pick_kernel,
        grid_spec=pltpu.PrefetchScalarGridSpec(
            num_scalar_prefetch=1,
            grid=(feats // wide,),
            in_specs=[
                pl.BlockSpec((rows // LANES, LANES), lambda i, w: (0, 0)),
                pl.BlockSpec((1, medoid_ids.shape[0]), lambda i, w: (0, 0)),
                pl.BlockSpec((rows, wide), lambda i, w: (0, i)),
            ],
            out_specs=[
                pl.BlockSpec((2 * CHIPS, MED_ROWS, 2 * LANES), lambda i, w: (i, 0, 0)),
                pl.BlockSpec((2 * CHIPS, GRAD_ROWS, LANES), lambda i, w: (i, 0, 0)),
            ],
            scratch_shapes=[pltpu.VMEM((SEL, rows), BF), pltpu.VMEM((8, SEL), BF)],
        ),
        out_shape=[
            jax.ShapeDtypeStruct((pts_count, MED_ROWS, 2 * LANES), BF),
            jax.ShapeDtypeStruct((pts_count, GRAD_ROWS, LANES), BF),
        ],
        compiler_params=pltpu.CompilerParams(vmem_limit_bytes=24 * 2**20),
        cost_estimate=pl.CostEstimate(
            flops=2 * SEL * rows * feats, bytes_accessed=rows * feats * 2, transcendentals=0
        ),
        name="pick",
    )(where, assignment.reshape(-1, LANES), medoid_ids[None, :], sketches)


def place_kernel(where_ref, got_ref, a_ref, b_ref, flag_ref):
    core = where_ref[2]
    sources = got_ref.shape[0]
    count = 2 * a_ref.shape[0]
    total = jnp.zeros((count, got_ref.shape[2]), F32)
    marks = jnp.zeros((1, LANES), F32)
    per = 2 * LANES // MED_ROWS
    iota = lax.broadcasted_iota(I32, (count, per * MED_ROWS), 0)
    for g in range(sources // per):
        numbers = []
        for q in range(g * per, (g + 1) * per):
            lines = got_ref[q, MED_SLOTS : MED_SLOTS + 8, :].astype(F32)
            line = lines[0:1]
            marks = marks + lines[3:4, :LANES]
            a = line[:, GRAD_ROWS : GRAD_ROWS + MED_ROWS]
            b = line[:, GRAD_ROWS + MED_ROWS :]
            numbers.append(jnp.where(core == 0, a, b))
        number = jnp.concatenate(numbers, axis=1).astype(I32) - 1
        hot = (number == iota).astype(F32).astype(BF)
        block = got_ref[g * per : (g + 1) * per].reshape(per * MED_ROWS, got_ref.shape[2])
        total = total + jnp.dot(hot, block, preferred_element_type=F32)
    a_ref[...] = total[: count // 2].astype(BF)
    b_ref[...] = total[count // 2 :].astype(BF)
    flag_ref[...] = jnp.concatenate([marks, marks], axis=1)


def place(where, got, count):
    return pl.pallas_call(
        place_kernel,
        in_specs=[
            pl.BlockSpec(memory_space=pltpu.SMEM),
            pl.BlockSpec(memory_space=pltpu.VMEM),
        ],
        out_specs=[pl.BlockSpec(memory_space=pltpu.VMEM)] * 3,
        out_shape=[
            jax.ShapeDtypeStruct((count // 2, got.shape[2]), BF),
            jax.ShapeDtypeStruct((count // 2, got.shape[2]), BF),
            jax.ShapeDtypeStruct((1, 2 * LANES), F32),
        ],
        compiler_params=pltpu.CompilerParams(vmem_limit_bytes=8 * 2**20),
        cost_estimate=pl.CostEstimate(
            flops=2 * count * got.size, bytes_accessed=2 * got.size, transcendentals=0
        ),
        name="place",
    )(where, got)


def sums_kernel(got_ref, sums_ref, count_ref):
    feats = got_ref.shape[2]
    medoids = sums_ref.shape[1]
    tail = GRAD_ROWS - LANES
    iota_a = lax.broadcasted_iota(I32, (medoids, LANES), 0)
    iota_b = lax.broadcasted_iota(I32, (medoids, tail), 0)
    ones = jnp.ones((GRAD_ROWS, LANES), BF)

    per = 4

    def body(step, total):
        hots, blocks = [], []
        for k in range(per):
            q = step * per + k
            codes = got_ref[q, GRAD_SLOTS:, :].astype(F32).astype(I32)
            a = codes[1:2] - 1 + codes[2:3] * 256
            b = (codes[9:10] - 1 + codes[10:11] * 256)[:, :tail]
            hots.append((a == iota_a).astype(F32))
            hots.append((b == iota_b).astype(F32))
            blocks.append(jnp.concatenate([got_ref[q], ones], axis=1))
        hot = jnp.concatenate(hots, axis=1).astype(BF)
        return total + jnp.dot(
            hot, jnp.concatenate(blocks, axis=0), preferred_element_type=F32
        )

    total = lax.fori_loop(
        0, got_ref.shape[0] // per, body, jnp.zeros((medoids, feats + LANES), F32)
    )
    sums_ref[...] = total[:, :feats].T
    count_ref[...] = total[:, feats:].T[:8]


def sums(got, medoids):
    return pl.pallas_call(
        sums_kernel,
        in_specs=[pl.BlockSpec(memory_space=pltpu.VMEM)],
        out_specs=[pl.BlockSpec(memory_space=pltpu.VMEM)] * 2,
        out_shape=[
            jax.ShapeDtypeStruct((got.shape[2], medoids), F32),
            jax.ShapeDtypeStruct((8, medoids), F32),
        ],
        compiler_params=pltpu.CompilerParams(vmem_limit_bytes=16 * 2**20),
        cost_estimate=pl.CostEstimate(
            flops=4 * medoids * got.size, bytes_accessed=2 * got.size, transcendentals=0
        ),
        name="sums",
    )(got)


def joined_kernel(*refs):
    parts, out_ref = refs[:-1], refs[-1]
    size = parts[0].shape[0]
    for i, part in enumerate(parts):
        out_ref[i * size : (i + 1) * size] = part[...]


def joined(parts):
    size, *rest = parts[0].shape
    return pl.pallas_call(
        joined_kernel,
        in_specs=[pl.BlockSpec(memory_space=pltpu.VMEM)] * len(parts),
        out_specs=pl.BlockSpec(memory_space=pltpu.VMEM),
        out_shape=jax.ShapeDtypeStruct((size * len(parts), *rest), parts[0].dtype),
        compiler_params=pltpu.CompilerParams(vmem_limit_bytes=8 * 2**20),
        cost_estimate=pl.CostEstimate(
            flops=0, bytes_accessed=4 * len(parts) * parts[0].size, transcendentals=0
        ),
        name="joined",
    )(*parts)


def score_kernel(scale, where_ref, assign_ref, mark_ref, sk_ref, own_ref, other_ref, out_ref):
    quarter, wide = own_ref.shape[1:]
    half = 2 * quarter
    core, x, y, base = where_ref[2], where_ref[3], where_ref[4], where_ref[5]
    points = sk_ref.shape[0]
    total = jnp.zeros((2 * half, points), F32)
    for kx in range(4):
        for ky in range(4):
            block = ((x + 4 - kx) & 3) * 4 + ((y + 4 - ky) & 3)
            at = pl.multiple_of(block * wide, wide)
            a, b = ky * 4 + kx, 16 + kx * 4 + ky
            total = total + contract_last(
                jnp.concatenate([own_ref[a], own_ref[b], other_ref[a], other_ref[b]], axis=0),
                sk_ref[:, pl.ds(at, wide)],
            )
    scores = total * scale
    best = jnp.max(scores, axis=0, keepdims=True)
    row = lax.broadcasted_iota(I32, scores.shape, 0)
    local = assign_ref[...] - base
    here = (local >= 0) & (local < 2 * half)
    local = jnp.where(here, local ^ (core * half), -1)
    chosen = jnp.max(jnp.where(local == row, scores, NONE), axis=0, keepdims=True)
    out_ref[...] = jnp.concatenate([best, chosen, mark_ref[...]], axis=0)


def scored(where, assignment, marks, sketches, own, other):
    rows, feats = sketches.shape
    tile = 2 * LANES
    whole = lambda a: pl.BlockSpec(a.shape, lambda i, w: (0,) * a.ndim)
    return pl.pallas_call(
        functools.partial(score_kernel, 1.0 / feats),
        grid_spec=pltpu.PrefetchScalarGridSpec(
            num_scalar_prefetch=1,
            grid=(rows // tile,),
            in_specs=[
                pl.BlockSpec((1, tile), lambda i, w: (0, i)),
                pl.BlockSpec((1, tile), lambda i, w: (0, 0)),
                pl.BlockSpec((tile, feats), lambda i, w: (i, 0)),
                whole(own),
                whole(other),
            ],
            out_specs=pl.BlockSpec((3, tile), lambda i, w: (0, i)),
        ),
        out_shape=jax.ShapeDtypeStruct((3, rows), F32),
        compiler_params=pltpu.CompilerParams(vmem_limit_bytes=24 * 2**20),
        cost_estimate=pl.CostEstimate(
            flops=2 * rows * feats * 512, bytes_accessed=rows * feats * 2, transcendentals=0
        ),
        name="scored",
    )(where, assignment[None, :], marks, sketches, own, other)


def closing_kernel(a_ref, b_ref, gap_ref, send_ref, mark_ref):
    both = jnp.maximum(a_ref[...], b_ref[...])
    gap_ref[...] = both[0:1] - both[1:2]
    mark_ref[0, 0] = jnp.max(both[2:3, :LANES]).astype(I32)
    total = jnp.broadcast_to(jnp.sum(both[0:1], axis=1, keepdims=True), (1, LANES))
    for i in range(send_ref.shape[0]):
        send_ref[i] = total


def closing(a, b, pts_count):
    return pl.pallas_call(
        closing_kernel,
        in_specs=[pl.BlockSpec(memory_space=pltpu.VMEM)] * 2,
        out_specs=[
            pl.BlockSpec(memory_space=pltpu.VMEM),
            pl.BlockSpec(memory_space=pltpu.VMEM),
            pl.BlockSpec(memory_space=pltpu.SMEM),
        ],
        out_shape=[
            jax.ShapeDtypeStruct((1, a.shape[1]), F32),
            jax.ShapeDtypeStruct((pts_count, 1, LANES), F32),
            jax.ShapeDtypeStruct((1, 1), I32),
        ],
        compiler_params=pltpu.CompilerParams(vmem_limit_bytes=4 * 2**20),
        cost_estimate=pl.CostEstimate(
            flops=a.size, bytes_accessed=8 * a.size, transcendentals=0
        ),
        name="closing",
    )(a, b)


def from_everyone(array, axis):
    size = lax.axis_size(axis)
    return lax.all_to_all(
        jnp.broadcast_to(array[None], (size, *array.shape)), axis, 0, 0, tiled=True
    )


def chip_of(p):
    return p // 8, (p // 2) % 4, p % 2


def shifted(array, dx, dy, dc):
    pairs = []
    for p in range(32):
        x, y, c = chip_of(p)
        pairs.append((p, (((x + dx) % 4) * 4 + (y + dy) % 4) * 2 + (c ^ dc)))
    return lax.ppermute(array, "pts", pairs)


def across(array, step, planes):
    return lax.ppermute(array, "med", [(z, z ^ step) for z in range(planes)])


def general(sketches, assignment, medoid_ids):
    row_count, feat_width = sketches.shape
    medoid_count = medoid_ids.shape[0]
    pts_count = lax.axis_size("pts")
    part = feat_width // pts_count
    pts_index = lax.axis_index("pts")
    med_index = lax.axis_index("med")
    local_assign = assignment - med_index * medoid_count
    one_hot = (
        local_assign[:, None] == jnp.arange(medoid_count, dtype=I32)[None, :]
    ).astype(BF)
    offsets = medoid_ids - pts_index * row_count
    inside = (offsets >= 0) & (offsets < row_count)
    picked = jnp.take(sketches, jnp.clip(offsets, 0, row_count - 1), axis=0)
    terms = jnp.where(inside[:, None], picked, jnp.zeros_like(picked))
    terms = terms.reshape(medoid_count, pts_count, part).swapaxes(0, 1)
    piece = (
        lax.all_to_all(terms, "pts", 0, 0, tiled=True).astype(F32).sum(axis=0).astype(BF)
    )
    everything = from_everyone(piece, "pts").swapaxes(0, 1).reshape(medoid_count, feat_width)
    partial = lax.dot_general(
        sketches, one_hot, (((0,), (0,)), ((), ())), preferred_element_type=F32
    ).reshape(pts_count, part, medoid_count)
    gradient_sums = lax.all_to_all(partial, "pts", 0, 0, tiled=True).sum(axis=0)
    counts = from_everyone(jnp.sum(one_hot.astype(F32), axis=0), "pts").sum(axis=0)
    scores = contract_last(sketches, everything) * (1.0 / feat_width)
    best = jnp.max(scores, axis=1)
    here = (local_assign >= 0) & (local_assign < medoid_count)
    taken = jnp.take_along_axis(
        scores, jnp.clip(local_assign, 0, medoid_count - 1)[:, None], axis=1
    )[:, 0]
    both = from_everyone(jnp.stack([best, jnp.where(here, taken, NONE)]), "med").max(axis=0)
    cover = from_everyone(jnp.sum(both[0])[None], "pts").sum()
    return both[0] - both[1], cover / (row_count * pts_count), counts, gradient_sums


def shards(sketches, assignment, medoid_ids):
    row_count, _ = sketches.shape
    medoid_count = medoid_ids.shape[0]
    half = medoid_count // 2
    pts_count = lax.axis_size("pts")
    p = lax.axis_index("pts")
    m = lax.axis_index("med")
    core = p % 2
    planes = lax.axis_size("med")
    where = jnp.stack(
        [p * row_count, m, core, p // 8, (p // 2) % 4, m * medoid_count, m, m]
    ).astype(I32)

    med_send, grad_send = pick(
        where, assignment, medoid_ids, sketches, pts_count
    )
    med_got = lax.all_to_all(med_send, "pts", 0, 0, tiled=True)
    a, b, marks = place(where, med_got, half)
    pa = jnp.stack([a] + [shifted(a, k, 0, 0) for k in (1, 2, 3)])
    pb = jnp.stack([b] + [shifted(b, 0, k, 0) for k in (1, 2, 3)])
    qa = [pa] + [shifted(pa, 0, k, 0) for k in (1, 2, 3)]
    qb = [pb] + [shifted(pb, k, 0, 0) for k in (1, 2, 3)]
    own = joined(qa + qb)
    other = shifted(own, 0, 0, 1)
    grad_got = lax.all_to_all(grad_send, "pts", 0, 0, tiled=True)
    stats = scored(where, assignment, marks, sketches, own, other)
    for step in (1, 2):
        stats = jnp.maximum(stats, across(stats, step, planes))
    final = across(stats, 4, planes)
    gap, total, mark = closing(stats, final, pts_count)
    full = mark[0, 0] > 0

    def fast():
        totals = lax.all_to_all(total, "pts", 0, 0, tiled=True)
        gradient_sums, counts = sums(grad_got, medoid_count)
        coverage = jnp.sum(totals[:, 0, 0]) / (row_count * pts_count)
        return gap[0], coverage, counts[0], gradient_sums

    return lax.cond(full, lambda: general(sketches, assignment, medoid_ids), fast)


def solution(mesh):
    in_specs = (P("pts", None), P("pts"), P("med"))
    out_specs = (P("pts"), P(), P("med"), P("pts", "med"))
    return jax.shard_map(
        shards, mesh=mesh, in_specs=in_specs, out_specs=out_specs, check_vma=False
    )
```

```python
import functools

import jax
import jax.numpy as jnp
from jax import lax
from jax.experimental import pallas as pl
from jax.experimental.pallas import tpu as pltpu
from jax.sharding import PartitionSpec as P


BF = jnp.bfloat16
F32 = jnp.float32
I32 = jnp.int32
LANES = 128
GRAD_ROWS = 192
GRAD_SLOTS = 176
MED_ROWS = 32
MED_SLOTS = 24
SEL = GRAD_ROWS + 2 * MED_ROWS
NONE = -1e30
CHIPS = 4


def contract_last(a, b):
    return lax.dot_general(a, b, (((1,), (1,)), ((), ())), preferred_element_type=F32)


def pick_kernel(where_ref, assign_ref, ids_ref, sk_ref, med_ref, grad_ref, sel, code):
    step = pl.program_id(0)

    @pl.when(step == 0)
    def _():
        base = where_ref[0]
        plane = where_ref[1]
        groups = assign_ref.shape[0]
        half = ids_ref.shape[1] // 2
        off = ids_ref[...] - base
        inside = (off >= 0) & (off < groups * LANES)
        hi = jnp.where(inside, off >> 7, -1)
        lo = off & (LANES - 1)
        j = lax.broadcasted_iota(I32, (1, 2 * half), 1)
        first = j < half
        number = (jnp.where(first, j, j - half) + 1).astype(F32)
        row = lax.broadcasted_iota(I32, (2 * groups, 2 * half), 0)
        wanted = jnp.where(first, hi, hi + groups)
        wanted = jnp.where(hi >= 0, wanted, -1)
        table = jnp.where(wanted == row, number, 0.0).astype(BF)
        lane_hot = (lo == lax.broadcasted_iota(I32, (LANES, 2 * half), 0)).astype(F32).astype(BF)
        medoid = contract_last(table, lane_hot)
        med0, med1 = medoid[:groups], medoid[groups:]
        local = assign_ref[...] - plane * (2 * half)
        mine = (local >= 0) & (local < 2 * half)
        local_lo = jnp.where(mine, (local & 255) + 1, 0).astype(F32)
        local_hi = jnp.where(mine, local >> 8, 0).astype(F32)
        flags = jnp.concatenate(
            [mine.astype(F32), (med0 > 0).astype(F32), (med1 > 0).astype(F32)], axis=0
        ).astype(BF)
        k = lax.broadcasted_iota(I32, (LANES, LANES), 0)
        b = lax.broadcasted_iota(I32, (LANES, LANES), 1)
        before = jnp.dot(flags, (k < b).astype(F32).astype(BF), preferred_element_type=F32)
        total = jnp.dot(flags, jnp.ones((LANES, LANES), BF), preferred_element_type=F32)
        slots, over = [], jnp.zeros((1, LANES), F32)
        for kind, limit in enumerate((GRAD_SLOTS, MED_SLOTS, MED_SLOTS)):
            run = jnp.zeros((1, LANES), F32)
            rows = []
            for g in range(groups):
                at = kind * groups + g
                rows.append(before[at : at + 1] + run)
                run = run + total[at : at + 1]
            over = over + jnp.where(run > limit, 1.0, 0.0)
            position = jnp.concatenate(rows, axis=0).astype(I32)
            flag = (mine, med0 > 0, med1 > 0)[kind] & (position < limit)
            slots.append(jnp.where(flag, position, -1))
        slot_g = slots[0]
        slot_m = jnp.where(slots[1] >= 0, slots[1], -1)
        slot_n = jnp.where(slots[2] >= 0, slots[2] + MED_ROWS, -1)
        grad_iota = lax.broadcasted_iota(I32, (GRAD_ROWS, LANES), 0)
        med_iota = lax.broadcasted_iota(I32, (2 * MED_ROWS, LANES), 0)
        codes = jnp.zeros((8, SEL), F32)
        zeros = jnp.zeros((5, LANES), F32)
        either = med0 + med1
        for g in range(groups):
            at = slice(g, g + 1)
            top = (slot_g[at] == grad_iota).astype(F32)
            low = ((slot_m[at] == med_iota) | (slot_n[at] == med_iota)).astype(F32)
            block = jnp.concatenate([top, low], axis=0).astype(BF)
            sel[:, g * LANES : (g + 1) * LANES] = block
            fields = jnp.concatenate(
                [either[at], local_lo[at], local_hi[at], zeros], axis=0
            ).astype(BF)
            codes = codes + contract_last(fields, block)
        marks = jnp.broadcast_to(jnp.concatenate([over, over], axis=1), (8, SEL))
        third = lax.broadcasted_iota(I32, (8, SEL), 0) == 3
        code[...] = jnp.where(third, marks, codes).astype(BF)

    codes = code[...]
    lines = jnp.concatenate([codes[:, :LANES], codes[:, LANES:]], axis=0)
    for chip in range(sk_ref.shape[1] // SEL):
        block = sk_ref[:, chip * SEL : (chip + 1) * SEL]
        rows = jnp.dot(sel[...], block, preferred_element_type=F32).astype(BF)
        for c in range(2):
            to = 2 * chip + c
            grad_ref[to, :GRAD_SLOTS, :] = rows[:GRAD_SLOTS, c * LANES : (c + 1) * LANES]
            grad_ref[to, GRAD_SLOTS:, :] = lines
            at = GRAD_ROWS + c * MED_ROWS
            med_ref[to, :, :] = jnp.concatenate([rows[at : at + MED_SLOTS], codes], axis=0)


def pick(where, assignment, medoid_ids, sketches, pts_count):
    rows, feats = sketches.shape
    wide = CHIPS * 2 * LANES
    return pl.pallas_call(
        pick_kernel,
        grid_spec=pltpu.PrefetchScalarGridSpec(
            num_scalar_prefetch=1,
            grid=(feats // wide,),
            in_specs=[
                pl.BlockSpec((rows // LANES, LANES), lambda i, w: (0, 0)),
                pl.BlockSpec((1, medoid_ids.shape[0]), lambda i, w: (0, 0)),
                pl.BlockSpec((rows, wide), lambda i, w: (0, i)),
            ],
            out_specs=[
                pl.BlockSpec((2 * CHIPS, MED_ROWS, 2 * LANES), lambda i, w: (i, 0, 0)),
                pl.BlockSpec((2 * CHIPS, GRAD_ROWS, LANES), lambda i, w: (i, 0, 0)),
            ],
            scratch_shapes=[pltpu.VMEM((SEL, rows), BF), pltpu.VMEM((8, SEL), BF)],
        ),
        out_shape=[
            jax.ShapeDtypeStruct((pts_count, MED_ROWS, 2 * LANES), BF),
            jax.ShapeDtypeStruct((pts_count, GRAD_ROWS, LANES), BF),
        ],
        compiler_params=pltpu.CompilerParams(vmem_limit_bytes=24 * 2**20),
        cost_estimate=pl.CostEstimate(
            flops=2 * SEL * rows * feats, bytes_accessed=rows * feats * 2, transcendentals=0
        ),
        name="pick",
    )(where, assignment.reshape(-1, LANES), medoid_ids[None, :], sketches)


def place_kernel(where_ref, got_ref, a_ref, b_ref, flag_ref):
    core = where_ref[2]
    sources = got_ref.shape[0]
    count = 2 * a_ref.shape[0]
    total = jnp.zeros((count, got_ref.shape[2]), F32)
    marks = jnp.zeros((1, LANES), F32)
    per = 2 * LANES // MED_ROWS
    iota = lax.broadcasted_iota(I32, (count, per * MED_ROWS), 0)
    for g in range(sources // per):
        numbers = []
        for q in range(g * per, (g + 1) * per):
            lines = got_ref[q, MED_SLOTS : MED_SLOTS + 8, :].astype(F32)
            line = lines[0:1]
            marks = marks + lines[3:4, :LANES]
            a = line[:, GRAD_ROWS : GRAD_ROWS + MED_ROWS]
            b = line[:, GRAD_ROWS + MED_ROWS :]
            numbers.append(jnp.where(core == 0, a, b))
        number = jnp.concatenate(numbers, axis=1).astype(I32) - 1
        hot = (number == iota).astype(F32).astype(BF)
        block = got_ref[g * per : (g + 1) * per].reshape(per * MED_ROWS, got_ref.shape[2])
        total = total + jnp.dot(hot, block, preferred_element_type=F32)
    a_ref[...] = total[: count // 2].astype(BF)
    b_ref[...] = total[count // 2 :].astype(BF)
    flag_ref[...] = jnp.concatenate([marks, marks], axis=1)


def place(where, got, count):
    return pl.pallas_call(
        place_kernel,
        in_specs=[
            pl.BlockSpec(memory_space=pltpu.SMEM),
            pl.BlockSpec(memory_space=pltpu.VMEM),
        ],
        out_specs=[pl.BlockSpec(memory_space=pltpu.VMEM)] * 3,
        out_shape=[
            jax.ShapeDtypeStruct((count // 2, got.shape[2]), BF),
            jax.ShapeDtypeStruct((count // 2, got.shape[2]), BF),
            jax.ShapeDtypeStruct((1, 2 * LANES), F32),
        ],
        compiler_params=pltpu.CompilerParams(vmem_limit_bytes=8 * 2**20),
        cost_estimate=pl.CostEstimate(
            flops=2 * count * got.size, bytes_accessed=2 * got.size, transcendentals=0
        ),
        name="place",
    )(where, got)


def sums_kernel(got_ref, sums_ref, count_ref):
    feats = got_ref.shape[2]
    medoids = sums_ref.shape[1]
    tail = GRAD_ROWS - LANES
    iota_a = lax.broadcasted_iota(I32, (medoids, LANES), 0)
    iota_b = lax.broadcasted_iota(I32, (medoids, tail), 0)
    ones = jnp.ones((GRAD_ROWS, LANES), BF)

    per = 4

    def body(step, total):
        hots, blocks = [], []
        for k in range(per):
            q = step * per + k
            codes = got_ref[q, GRAD_SLOTS:, :].astype(F32).astype(I32)
            a = codes[1:2] - 1 + codes[2:3] * 256
            b = (codes[9:10] - 1 + codes[10:11] * 256)[:, :tail]
            hots.append((a == iota_a).astype(F32))
            hots.append((b == iota_b).astype(F32))
            blocks.append(jnp.concatenate([got_ref[q], ones], axis=1))
        hot = jnp.concatenate(hots, axis=1).astype(BF)
        return total + jnp.dot(
            hot, jnp.concatenate(blocks, axis=0), preferred_element_type=F32
        )

    total = lax.fori_loop(
        0, got_ref.shape[0] // per, body, jnp.zeros((medoids, feats + LANES), F32)
    )
    sums_ref[...] = total[:, :feats].T
    count_ref[...] = total[:, feats:].T[:1]


def sums(got, medoids):
    return pl.pallas_call(
        sums_kernel,
        in_specs=[pl.BlockSpec(memory_space=pltpu.VMEM)],
        out_specs=[pl.BlockSpec(memory_space=pltpu.VMEM)] * 2,
        out_shape=[
            jax.ShapeDtypeStruct((got.shape[2], medoids), F32),
            jax.ShapeDtypeStruct((1, medoids), F32),
        ],
        compiler_params=pltpu.CompilerParams(vmem_limit_bytes=16 * 2**20),
        cost_estimate=pl.CostEstimate(
            flops=4 * medoids * got.size, bytes_accessed=2 * got.size, transcendentals=0
        ),
        name="sums",
    )(got)


def joined_kernel(*refs):
    parts, out_ref = refs[:-1], refs[-1]
    size = parts[0].shape[0]
    for i, part in enumerate(parts):
        out_ref[i * size : (i + 1) * size] = part[...]


def joined(parts):
    size, *rest = parts[0].shape
    return pl.pallas_call(
        joined_kernel,
        in_specs=[pl.BlockSpec(memory_space=pltpu.VMEM)] * len(parts),
        out_specs=pl.BlockSpec(memory_space=pltpu.VMEM),
        out_shape=jax.ShapeDtypeStruct((size * len(parts), *rest), parts[0].dtype),
        compiler_params=pltpu.CompilerParams(vmem_limit_bytes=8 * 2**20),
        cost_estimate=pl.CostEstimate(
            flops=0, bytes_accessed=4 * len(parts) * parts[0].size, transcendentals=0
        ),
        name="joined",
    )(*parts)


def score_kernel(scale, where_ref, assign_ref, mark_ref, sk_ref, own_ref, other_ref, out_ref):
    quarter, wide = own_ref.shape[1:]
    half = 2 * quarter
    core, x, y, base = where_ref[2], where_ref[3], where_ref[4], where_ref[5]
    points = sk_ref.shape[0]
    total = jnp.zeros((2 * half, points), F32)
    for kx in range(4):
        for ky in range(4):
            block = ((x + 4 - kx) & 3) * 4 + ((y + 4 - ky) & 3)
            at = pl.multiple_of(block * wide, wide)
            a, b = ky * 4 + kx, 16 + kx * 4 + ky
            total = total + contract_last(
                jnp.concatenate([own_ref[a], own_ref[b], other_ref[a], other_ref[b]], axis=0),
                sk_ref[:, pl.ds(at, wide)],
            )
    scores = total * scale
    best = jnp.max(scores, axis=0, keepdims=True)
    row = lax.broadcasted_iota(I32, scores.shape, 0)
    local = assign_ref[...] - base
    here = (local >= 0) & (local < 2 * half)
    local = jnp.where(here, local ^ (core * half), -1)
    chosen = jnp.max(jnp.where(local == row, scores, NONE), axis=0, keepdims=True)
    out_ref[...] = jnp.concatenate([best, chosen, mark_ref[...]], axis=0)


def scored(where, assignment, marks, sketches, own, other):
    rows, feats = sketches.shape
    tile = 2 * LANES
    whole = lambda a: pl.BlockSpec(a.shape, lambda i, w: (0,) * a.ndim)
    return pl.pallas_call(
        functools.partial(score_kernel, 1.0 / feats),
        grid_spec=pltpu.PrefetchScalarGridSpec(
            num_scalar_prefetch=1,
            grid=(rows // tile,),
            in_specs=[
                pl.BlockSpec((1, tile), lambda i, w: (0, i)),
                pl.BlockSpec((1, tile), lambda i, w: (0, 0)),
                pl.BlockSpec((tile, feats), lambda i, w: (i, 0)),
                whole(own),
                whole(other),
            ],
            out_specs=pl.BlockSpec((3, tile), lambda i, w: (0, i)),
        ),
        out_shape=jax.ShapeDtypeStruct((3, rows), F32),
        compiler_params=pltpu.CompilerParams(vmem_limit_bytes=24 * 2**20),
        cost_estimate=pl.CostEstimate(
            flops=2 * rows * feats * 512, bytes_accessed=rows * feats * 2, transcendentals=0
        ),
        name="scored",
    )(where, assignment[None, :], marks, sketches, own, other)


def closing_kernel(a_ref, b_ref, c_ref, gap_ref, send_ref, mark_ref):
    both = jnp.maximum(jnp.maximum(a_ref[...], b_ref[...]), c_ref[...])
    gap_ref[...] = both[0:1] - both[1:2]
    mark_ref[0, 0] = jnp.max(both[2:3, :LANES]).astype(I32)
    total = jnp.broadcast_to(jnp.sum(both[0:1], axis=1, keepdims=True), (1, LANES))
    for i in range(send_ref.shape[0]):
        send_ref[i] = total


def closing(a, b, c, pts_count):
    return pl.pallas_call(
        closing_kernel,
        in_specs=[pl.BlockSpec(memory_space=pltpu.VMEM)] * 3,
        out_specs=[
            pl.BlockSpec(memory_space=pltpu.VMEM),
            pl.BlockSpec(memory_space=pltpu.VMEM),
            pl.BlockSpec(memory_space=pltpu.SMEM),
        ],
        out_shape=[
            jax.ShapeDtypeStruct((1, a.shape[1]), F32),
            jax.ShapeDtypeStruct((pts_count, 1, LANES), F32),
            jax.ShapeDtypeStruct((1, 1), I32),
        ],
        compiler_params=pltpu.CompilerParams(vmem_limit_bytes=4 * 2**20),
        cost_estimate=pl.CostEstimate(
            flops=a.size, bytes_accessed=8 * a.size, transcendentals=0
        ),
        name="closing",
    )(a, b, c)


def from_everyone(array, axis):
    size = lax.axis_size(axis)
    return lax.all_to_all(
        jnp.broadcast_to(array[None], (size, *array.shape)), axis, 0, 0, tiled=True
    )


def chip_of(p):
    return p // 8, (p // 2) % 4, p % 2


def shifted(array, dx, dy, dc):
    pairs = []
    for p in range(32):
        x, y, c = chip_of(p)
        pairs.append((p, (((x + dx) % 4) * 4 + (y + dy) % 4) * 2 + (c ^ dc)))
    return lax.ppermute(array, "pts", pairs)


def across(array, step, planes):
    return lax.ppermute(array, "med", [(z, (z + step) % planes) for z in range(planes)])


def general(sketches, assignment, medoid_ids):
    row_count, feat_width = sketches.shape
    medoid_count = medoid_ids.shape[0]
    pts_count = lax.axis_size("pts")
    part = feat_width // pts_count
    pts_index = lax.axis_index("pts")
    med_index = lax.axis_index("med")
    local_assign = assignment - med_index * medoid_count
    one_hot = (
        local_assign[:, None] == jnp.arange(medoid_count, dtype=I32)[None, :]
    ).astype(BF)
    offsets = medoid_ids - pts_index * row_count
    inside = (offsets >= 0) & (offsets < row_count)
    picked = jnp.take(sketches, jnp.clip(offsets, 0, row_count - 1), axis=0)
    terms = jnp.where(inside[:, None], picked, jnp.zeros_like(picked))
    terms = terms.reshape(medoid_count, pts_count, part).swapaxes(0, 1)
    piece = (
        lax.all_to_all(terms, "pts", 0, 0, tiled=True).astype(F32).sum(axis=0).astype(BF)
    )
    everything = from_everyone(piece, "pts").swapaxes(0, 1).reshape(medoid_count, feat_width)
    partial = lax.dot_general(
        sketches, one_hot, (((0,), (0,)), ((), ())), preferred_element_type=F32
    ).reshape(pts_count, part, medoid_count)
    gradient_sums = lax.all_to_all(partial, "pts", 0, 0, tiled=True).sum(axis=0)
    counts = from_everyone(jnp.sum(one_hot.astype(F32), axis=0), "pts").sum(axis=0)
    scores = contract_last(sketches, everything) * (1.0 / feat_width)
    best = jnp.max(scores, axis=1)
    here = (local_assign >= 0) & (local_assign < medoid_count)
    taken = jnp.take_along_axis(
        scores, jnp.clip(local_assign, 0, medoid_count - 1)[:, None], axis=1
    )[:, 0]
    both = from_everyone(jnp.stack([best, jnp.where(here, taken, NONE)]), "med").max(axis=0)
    cover = from_everyone(jnp.sum(both[0])[None], "pts").sum()
    return both[0] - both[1], cover / (row_count * pts_count), counts, gradient_sums


def shards(sketches, assignment, medoid_ids):
    row_count, _ = sketches.shape
    medoid_count = medoid_ids.shape[0]
    half = medoid_count // 2
    pts_count = lax.axis_size("pts")
    p = lax.axis_index("pts")
    m = lax.axis_index("med")
    core = p % 2
    planes = lax.axis_size("med")
    where = jnp.stack(
        [p * row_count, m, core, p // 8, (p // 2) % 4, m * medoid_count, m, m]
    ).astype(I32)

    med_send, grad_send = pick(
        where, assignment, medoid_ids, sketches, pts_count
    )
    med_got = lax.all_to_all(med_send, "pts", 0, 0, tiled=True)
    a, b, marks = place(where, med_got, half)
    a2, b2 = shifted(a, 2, 0, 0), shifted(b, 0, 2, 0)
    a1, b1 = shifted(a, 1, 0, 0), shifted(b, 0, 1, 0)
    a3, b3 = shifted(a, 3, 0, 0), shifted(b, 0, 3, 0)
    pa = jnp.stack([a, a1, a2, a3])
    pb = jnp.stack([b, b1, b2, b3])
    qa2, qb2 = shifted(pa, 0, 2, 0), shifted(pb, 2, 0, 0)
    qa1, qb1 = shifted(pa, 0, 1, 0), shifted(pb, 1, 0, 0)
    qa3, qb3 = shifted(pa, 0, 3, 0), shifted(pb, 3, 0, 0)
    own = joined([pa, qa1, qa2, qa3, pb, qb1, qb2, qb3])
    other = shifted(own, 0, 0, 1)
    grad_got = lax.all_to_all(grad_send, "pts", 0, 0, tiled=True)
    stats = scored(where, assignment, marks, sketches, own, other)
    ahead, behind = across(stats, 1, planes), across(stats, -1, planes)
    stats = jnp.maximum(jnp.maximum(stats, ahead), behind)
    ahead, behind = across(stats, 3, planes), across(stats, -3, planes)
    gap, total, mark = closing(stats, ahead, behind, pts_count)
    full = mark[0, 0] > 0

    def fast():
        totals = lax.all_to_all(total, "pts", 0, 0, tiled=True)
        gradient_sums, counts = sums(grad_got, medoid_count)
        coverage = jnp.sum(totals[:, 0, 0]) / (row_count * pts_count)
        return gap[0], coverage, counts[0], gradient_sums

    return lax.cond(full, lambda: general(sketches, assignment, medoid_ids), fast)


def solution(mesh):
    in_specs = (P("pts", None), P("pts"), P("med"))
    out_specs = (P("pts"), P(), P("med"), P("pts", "med"))
    return jax.shard_map(
        shards, mesh=mesh, in_specs=in_specs, out_specs=out_specs, check_vma=False
    )
```

```python
import functools

import jax
import jax.numpy as jnp
from jax import lax
from jax.experimental import pallas as pl
from jax.experimental.pallas import tpu as pltpu
from jax.sharding import PartitionSpec as P


BF = jnp.bfloat16
F32 = jnp.float32
I32 = jnp.int32
LANES = 128
GRAD_ROWS = 192
GRAD_SLOTS = 176
MED_ROWS = 32
MED_SLOTS = 24
SEL = GRAD_ROWS + 2 * MED_ROWS
NONE = -1e30
CHIPS = 4


def contract_last(a, b):
    return lax.dot_general(a, b, (((1,), (1,)), ((), ())), preferred_element_type=F32)


def pick_kernel(where_ref, assign_ref, ids_ref, sk_ref, med_ref, grad_ref, sel, code):
    step = pl.program_id(0)

    @pl.when(step == 0)
    def _():
        base = where_ref[0]
        plane = where_ref[1]
        groups = assign_ref.shape[0]
        half = ids_ref.shape[1] // 2
        off = ids_ref[...] - base
        inside = (off >= 0) & (off < groups * LANES)
        hi = jnp.where(inside, off >> 7, -1)
        lo = off & (LANES - 1)
        j = lax.broadcasted_iota(I32, (1, 2 * half), 1)
        first = j < half
        number = (jnp.where(first, j, j - half) + 1).astype(F32)
        row = lax.broadcasted_iota(I32, (2 * groups, 2 * half), 0)
        wanted = jnp.where(first, hi, hi + groups)
        wanted = jnp.where(hi >= 0, wanted, -1)
        table = jnp.where(wanted == row, number, 0.0).astype(BF)
        lane_hot = (lo == lax.broadcasted_iota(I32, (LANES, 2 * half), 0)).astype(F32).astype(BF)
        medoid = contract_last(table, lane_hot)
        med0, med1 = medoid[:groups], medoid[groups:]
        local = assign_ref[...] - plane * (2 * half)
        mine = (local >= 0) & (local < 2 * half)
        local_lo = jnp.where(mine, (local & 255) + 1, 0).astype(F32)
        local_hi = jnp.where(mine, local >> 8, 0).astype(F32)
        flags = jnp.concatenate(
            [mine.astype(F32), (med0 > 0).astype(F32), (med1 > 0).astype(F32)], axis=0
        ).astype(BF)
        k = lax.broadcasted_iota(I32, (LANES, LANES), 0)
        b = lax.broadcasted_iota(I32, (LANES, LANES), 1)
        before = jnp.dot(flags, (k < b).astype(F32).astype(BF), preferred_element_type=F32)
        total = jnp.dot(flags, jnp.ones((LANES, LANES), BF), preferred_element_type=F32)
        slots, over = [], jnp.zeros((1, LANES), F32)
        for kind, limit in enumerate((GRAD_SLOTS, MED_SLOTS, MED_SLOTS)):
            run = jnp.zeros((1, LANES), F32)
            rows = []
            for g in range(groups):
                at = kind * groups + g
                rows.append(before[at : at + 1] + run)
                run = run + total[at : at + 1]
            over = over + jnp.where(run > limit, 1.0, 0.0)
            position = jnp.concatenate(rows, axis=0).astype(I32)
            flag = (mine, med0 > 0, med1 > 0)[kind] & (position < limit)
            slots.append(jnp.where(flag, position, -1))
        slot_g = slots[0]
        slot_m = jnp.where(slots[1] >= 0, slots[1], -1)
        slot_n = jnp.where(slots[2] >= 0, slots[2] + MED_ROWS, -1)
        grad_iota = lax.broadcasted_iota(I32, (GRAD_ROWS, LANES), 0)
        med_iota = lax.broadcasted_iota(I32, (2 * MED_ROWS, LANES), 0)
        codes = jnp.zeros((8, SEL), F32)
        zeros = jnp.zeros((5, LANES), F32)
        either = med0 + med1
        for g in range(groups):
            at = slice(g, g + 1)
            top = (slot_g[at] == grad_iota).astype(F32)
            low = ((slot_m[at] == med_iota) | (slot_n[at] == med_iota)).astype(F32)
            block = jnp.concatenate([top, low], axis=0).astype(BF)
            sel[:, g * LANES : (g + 1) * LANES] = block
            fields = jnp.concatenate(
                [either[at], local_lo[at], local_hi[at], zeros], axis=0
            ).astype(BF)
            codes = codes + contract_last(fields, block)
        marks = jnp.broadcast_to(jnp.concatenate([over, over], axis=1), (8, SEL))
        third = lax.broadcasted_iota(I32, (8, SEL), 0) == 3
        code[...] = jnp.where(third, marks, codes).astype(BF)

    codes = code[...]
    lines = jnp.concatenate([codes[:, :LANES], codes[:, LANES:]], axis=0)

    @pl.loop(0, sk_ref.shape[1] // SEL)
    def _(chip):
        block = sk_ref[:, pl.ds(pl.multiple_of(chip * SEL, SEL), SEL)]
        rows = jnp.dot(sel[...], block, preferred_element_type=F32).astype(BF)
        for c in range(2):
            to = 2 * chip + c
            grad_ref[to, :GRAD_SLOTS, :] = rows[:GRAD_SLOTS, c * LANES : (c + 1) * LANES]
            grad_ref[to, GRAD_SLOTS:, :] = lines
            at = GRAD_ROWS + c * MED_ROWS
            med_ref[to, :, :] = jnp.concatenate([rows[at : at + MED_SLOTS], codes], axis=0)


def pick(where, assignment, medoid_ids, sketches, pts_count):
    rows, feats = sketches.shape
    wide = CHIPS * 2 * LANES
    return pl.pallas_call(
        pick_kernel,
        grid_spec=pltpu.PrefetchScalarGridSpec(
            num_scalar_prefetch=1,
            grid=(feats // wide,),
            in_specs=[
                pl.BlockSpec((rows // LANES, LANES), lambda i, w: (0, 0)),
                pl.BlockSpec((1, medoid_ids.shape[0]), lambda i, w: (0, 0)),
                pl.BlockSpec((rows, wide), lambda i, w: (0, i)),
            ],
            out_specs=[
                pl.BlockSpec((2 * CHIPS, MED_ROWS, 2 * LANES), lambda i, w: (i, 0, 0)),
                pl.BlockSpec((2 * CHIPS, GRAD_ROWS, LANES), lambda i, w: (i, 0, 0)),
            ],
            scratch_shapes=[pltpu.VMEM((SEL, rows), BF), pltpu.VMEM((8, SEL), BF)],
        ),
        out_shape=[
            jax.ShapeDtypeStruct((pts_count, MED_ROWS, 2 * LANES), BF),
            jax.ShapeDtypeStruct((pts_count, GRAD_ROWS, LANES), BF),
        ],
        compiler_params=pltpu.CompilerParams(vmem_limit_bytes=24 * 2**20),
        cost_estimate=pl.CostEstimate(
            flops=2 * SEL * rows * feats, bytes_accessed=rows * feats * 2, transcendentals=0
        ),
        name="pick",
    )(where, assignment.reshape(-1, LANES), medoid_ids[None, :], sketches)


def place_kernel(where_ref, got_ref, a_ref, b_ref, flag_ref):
    core = where_ref[2]
    sources = got_ref.shape[0]
    count = 2 * a_ref.shape[0]
    total = jnp.zeros((count, got_ref.shape[2]), F32)
    marks = jnp.zeros((1, LANES), F32)
    per = 2 * LANES // MED_ROWS
    iota = lax.broadcasted_iota(I32, (count, per * MED_ROWS), 0)
    for g in range(sources // per):
        numbers = []
        for q in range(g * per, (g + 1) * per):
            lines = got_ref[q, MED_SLOTS : MED_SLOTS + 8, :].astype(F32)
            line = lines[0:1]
            marks = marks + lines[3:4, :LANES]
            a = line[:, GRAD_ROWS : GRAD_ROWS + MED_ROWS]
            b = line[:, GRAD_ROWS + MED_ROWS :]
            numbers.append(jnp.where(core == 0, a, b))
        number = jnp.concatenate(numbers, axis=1).astype(I32) - 1
        hot = (number == iota).astype(F32).astype(BF)
        block = got_ref[g * per : (g + 1) * per].reshape(per * MED_ROWS, got_ref.shape[2])
        total = total + jnp.dot(hot, block, preferred_element_type=F32)
    a_ref[...] = total[: count // 2].astype(BF)
    b_ref[...] = total[count // 2 :].astype(BF)
    flag_ref[...] = jnp.concatenate([marks, marks], axis=1)


def place(where, got, count):
    return pl.pallas_call(
        place_kernel,
        in_specs=[
            pl.BlockSpec(memory_space=pltpu.SMEM),
            pl.BlockSpec(memory_space=pltpu.VMEM),
        ],
        out_specs=[pl.BlockSpec(memory_space=pltpu.VMEM)] * 3,
        out_shape=[
            jax.ShapeDtypeStruct((count // 2, got.shape[2]), BF),
            jax.ShapeDtypeStruct((count // 2, got.shape[2]), BF),
            jax.ShapeDtypeStruct((1, 2 * LANES), F32),
        ],
        compiler_params=pltpu.CompilerParams(vmem_limit_bytes=8 * 2**20),
        cost_estimate=pl.CostEstimate(
            flops=2 * count * got.size, bytes_accessed=2 * got.size, transcendentals=0
        ),
        name="place",
    )(where, got)


def sums_kernel(got_ref, sums_ref, count_ref):
    feats = got_ref.shape[2]
    medoids = sums_ref.shape[1]
    tail = GRAD_ROWS - LANES
    iota_a = lax.broadcasted_iota(I32, (medoids, LANES), 0)
    iota_b = lax.broadcasted_iota(I32, (medoids, tail), 0)
    ones = jnp.ones((GRAD_ROWS, LANES), BF)

    per = 4

    def body(step, total):
        hots, blocks = [], []
        for k in range(per):
            q = step * per + k
            codes = got_ref[q, GRAD_SLOTS:, :].astype(F32).astype(I32)
            a = codes[1:2] - 1 + codes[2:3] * 256
            b = (codes[9:10] - 1 + codes[10:11] * 256)[:, :tail]
            hots.append((a == iota_a).astype(F32))
            hots.append((b == iota_b).astype(F32))
            blocks.append(jnp.concatenate([got_ref[q], ones], axis=1))
        hot = jnp.concatenate(hots, axis=1).astype(BF)
        return total + jnp.dot(
            hot, jnp.concatenate(blocks, axis=0), preferred_element_type=F32
        )

    total = lax.fori_loop(
        0, got_ref.shape[0] // per, body, jnp.zeros((medoids, feats + LANES), F32)
    )
    sums_ref[...] = total[:, :feats].T
    count_ref[...] = total[:, feats:].T[:1]


def sums(got, medoids):
    return pl.pallas_call(
        sums_kernel,
        in_specs=[pl.BlockSpec(memory_space=pltpu.VMEM)],
        out_specs=[pl.BlockSpec(memory_space=pltpu.VMEM)] * 2,
        out_shape=[
            jax.ShapeDtypeStruct((got.shape[2], medoids), F32),
            jax.ShapeDtypeStruct((1, medoids), F32),
        ],
        compiler_params=pltpu.CompilerParams(vmem_limit_bytes=16 * 2**20),
        cost_estimate=pl.CostEstimate(
            flops=4 * medoids * got.size, bytes_accessed=2 * got.size, transcendentals=0
        ),
        name="sums",
    )(got)


def score_kernel(scale, where_ref, assign_ref, mark_ref, near_ref, far_ref, *refs):
    parts, (near_out, far_out) = refs[:8], refs[8:]
    quarter, wide = parts[0].shape[1:]
    half = 2 * quarter
    x, y, base = where_ref[3], where_ref[4], where_ref[5]
    step = pl.program_id(0)
    count = pl.num_programs(0) // 2

    def stats(points_ref):
        total = jnp.zeros((half, points_ref.shape[0]), F32)
        for kx in range(4):
            for ky in range(4):
                block = ((x + 4 - kx) & 3) * 4 + ((y + 4 - ky) & 3)
                at = pl.multiple_of(block * wide, wide)
                total = total + contract_last(
                    jnp.concatenate([parts[ky][kx], parts[4 + kx][ky]], axis=0),
                    points_ref[:, pl.ds(at, wide)],
                )
        scores = total * scale
        best = jnp.max(scores, axis=0, keepdims=True)
        row = lax.broadcasted_iota(I32, scores.shape, 0)
        local = assign_ref[...] - base
        chosen = jnp.max(jnp.where(local == row, scores, NONE), axis=0, keepdims=True)
        return jnp.concatenate([best, chosen, mark_ref[...]], axis=0)

    @pl.when(step < count)
    def _():
        near_out[...] = stats(near_ref)

    @pl.when(step >= count)
    def _():
        far_out[...] = stats(far_ref)


def scored(where, assignments, marks, near, far, parts):
    rows, feats = near.shape
    tile = 2 * LANES
    count = rows // tile
    early = lambda i, w: (jnp.minimum(i, count - 1), 0)
    late = lambda i, w: (jnp.maximum(i - count, 0), 0)
    return pl.pallas_call(
        functools.partial(score_kernel, 1.0 / feats),
        grid_spec=pltpu.PrefetchScalarGridSpec(
            num_scalar_prefetch=1,
            grid=(2 * count,),
            in_specs=[
                pl.BlockSpec((1, tile), lambda i, w: (0, i)),
                pl.BlockSpec((1, tile), lambda i, w: (0, 0)),
                pl.BlockSpec((tile, feats), early),
                pl.BlockSpec((tile, feats), late),
            ]
            + [pl.BlockSpec(a.shape, lambda i, w: (0, 0, 0)) for a in parts],
            out_specs=[
                pl.BlockSpec((3, tile), lambda i, w: early(i, w)[::-1]),
                pl.BlockSpec((3, tile), lambda i, w: late(i, w)[::-1]),
            ],
        ),
        out_shape=[jax.ShapeDtypeStruct((3, rows), F32)] * 2,
        compiler_params=pltpu.CompilerParams(vmem_limit_bytes=32 * 2**20),
        cost_estimate=pl.CostEstimate(
            flops=4 * rows * feats * 256, bytes_accessed=rows * feats * 4, transcendentals=0
        ),
        name="scored",
    )(where, assignments, marks, near, far, *parts)


def closing_kernel(a_ref, b_ref, gap_ref, send_ref, mark_ref):
    both = jnp.maximum(a_ref[...], b_ref[...])
    gap_ref[...] = both[0:1] - both[1:2]
    mark_ref[0, 0] = jnp.max(both[2:3, :LANES]).astype(I32)
    total = jnp.broadcast_to(jnp.sum(both[0:1], axis=1, keepdims=True), (1, LANES))
    for i in range(send_ref.shape[0]):
        send_ref[i] = total


def closing(a, b, pts_count):
    return pl.pallas_call(
        closing_kernel,
        in_specs=[pl.BlockSpec(memory_space=pltpu.VMEM)] * 2,
        out_specs=[
            pl.BlockSpec(memory_space=pltpu.VMEM),
            pl.BlockSpec(memory_space=pltpu.VMEM),
            pl.BlockSpec(memory_space=pltpu.SMEM),
        ],
        out_shape=[
            jax.ShapeDtypeStruct((1, a.shape[1]), F32),
            jax.ShapeDtypeStruct((pts_count, 1, LANES), F32),
            jax.ShapeDtypeStruct((1, 1), I32),
        ],
        compiler_params=pltpu.CompilerParams(vmem_limit_bytes=4 * 2**20),
        cost_estimate=pl.CostEstimate(
            flops=a.size, bytes_accessed=8 * a.size, transcendentals=0
        ),
        name="closing",
    )(a, b)


def from_everyone(array, axis):
    size = lax.axis_size(axis)
    return lax.all_to_all(
        jnp.broadcast_to(array[None], (size, *array.shape)), axis, 0, 0, tiled=True
    )


def chip_of(p):
    return p // 8, (p // 2) % 4, p % 2


def shifted(array, dx, dy, dc):
    pairs = []
    for p in range(32):
        x, y, c = chip_of(p)
        pairs.append((p, (((x + dx) % 4) * 4 + (y + dy) % 4) * 2 + (c ^ dc)))
    return lax.ppermute(array, "pts", pairs)


def across(array, core, step, planes):
    pairs = [
        (p * planes + z, (p ^ core) * planes + (z ^ step))
        for p in range(32)
        for z in range(planes)
    ]
    return lax.ppermute(array, ("pts", "med"), pairs)


def general(sketches, assignment, medoid_ids):
    row_count, feat_width = sketches.shape
    medoid_count = medoid_ids.shape[0]
    pts_count = lax.axis_size("pts")
    part = feat_width // pts_count
    pts_index = lax.axis_index("pts")
    med_index = lax.axis_index("med")
    local_assign = assignment - med_index * medoid_count
    one_hot = (
        local_assign[:, None] == jnp.arange(medoid_count, dtype=I32)[None, :]
    ).astype(BF)
    offsets = medoid_ids - pts_index * row_count
    inside = (offsets >= 0) & (offsets < row_count)
    picked = jnp.take(sketches, jnp.clip(offsets, 0, row_count - 1), axis=0)
    terms = jnp.where(inside[:, None], picked, jnp.zeros_like(picked))
    terms = terms.reshape(medoid_count, pts_count, part).swapaxes(0, 1)
    piece = (
        lax.all_to_all(terms, "pts", 0, 0, tiled=True).astype(F32).sum(axis=0).astype(BF)
    )
    everything = from_everyone(piece, "pts").swapaxes(0, 1).reshape(medoid_count, feat_width)
    partial = lax.dot_general(
        sketches, one_hot, (((0,), (0,)), ((), ())), preferred_element_type=F32
    ).reshape(pts_count, part, medoid_count)
    gradient_sums = lax.all_to_all(partial, "pts", 0, 0, tiled=True).sum(axis=0)
    counts = from_everyone(jnp.sum(one_hot.astype(F32), axis=0), "pts").sum(axis=0)
    scores = contract_last(sketches, everything) * (1.0 / feat_width)
    best = jnp.max(scores, axis=1)
    here = (local_assign >= 0) & (local_assign < medoid_count)
    taken = jnp.take_along_axis(
        scores, jnp.clip(local_assign, 0, medoid_count - 1)[:, None], axis=1
    )[:, 0]
    both = from_everyone(jnp.stack([best, jnp.where(here, taken, NONE)]), "med").max(axis=0)
    cover = from_everyone(jnp.sum(both[0])[None], "pts").sum()
    return both[0] - both[1], cover / (row_count * pts_count), counts, gradient_sums


def shards(sketches, assignment, medoid_ids):
    row_count, _ = sketches.shape
    medoid_count = medoid_ids.shape[0]
    half = medoid_count // 2
    pts_count = lax.axis_size("pts")
    p = lax.axis_index("pts")
    m = lax.axis_index("med")
    core = p % 2
    planes = lax.axis_size("med")
    where = jnp.stack(
        [p * row_count, m, core, p // 8, (p // 2) % 4, m * medoid_count + core * half, m, m]
    ).astype(I32)

    far = shifted(sketches, 0, 0, 1)
    far_assignment = shifted(assignment, 0, 0, 1)
    med_send, grad_send = pick(
        where, assignment, medoid_ids, sketches, pts_count
    )
    med_got = lax.all_to_all(med_send, "pts", 0, 0, tiled=True)
    a, b, marks = place(where, med_got, half)
    pa = jnp.stack([a] + [shifted(a, k, 0, 0) for k in (1, 2, 3)])
    pb = jnp.stack([b] + [shifted(b, 0, k, 0) for k in (1, 2, 3)])
    qa = [pa, shifted(pa, 0, 1, 0)]
    qa = qa + [shifted(pa, 0, k, 0) for k in (2, 3)]
    qb = [pb] + [shifted(pb, k, 0, 0) for k in (1, 2, 3)]
    grad_got = lax.all_to_all(grad_send, "pts", 0, 0, tiled=True)
    assignments = jnp.concatenate([assignment, far_assignment])[None, :]
    stats, theirs = scored(where, assignments, marks, sketches, far, qa + qb)
    stats = jnp.maximum(
        jnp.maximum(stats, across(stats, 0, 1, planes)),
        jnp.maximum(across(theirs, 1, 0, planes), across(theirs, 1, 1, planes)),
    )
    stats = jnp.maximum(stats, across(stats, 0, 2, planes))
    final = across(stats, 0, 4, planes)
    gradient_sums, counts = sums(grad_got, medoid_count)
    gap, total, mark = closing(stats, final, pts_count)
    full = mark[0, 0] > 0

    def fast():
        totals = lax.all_to_all(total, "pts", 0, 0, tiled=True)
        coverage = jnp.sum(totals[:, 0, 0]) / (row_count * pts_count)
        return gap[0], coverage, counts[0], gradient_sums

    return lax.cond(full, lambda: general(sketches, assignment, medoid_ids), fast)


def solution(mesh):
    in_specs = (P("pts", None), P("pts"), P("med"))
    out_specs = (P("pts"), P(), P("med"), P("pts", "med"))
    return jax.shard_map(
        shards, mesh=mesh, in_specs=in_specs, out_specs=out_specs, check_vma=False
    )
```

```python
import functools

import jax
import jax.numpy as jnp
from jax import lax
from jax.experimental import pallas as pl
from jax.experimental.pallas import tpu as pltpu
from jax.sharding import PartitionSpec as P


BF = jnp.bfloat16
F32 = jnp.float32
I32 = jnp.int32
LANES = 128
GRAD_ROWS = 192
GRAD_SLOTS = 176
MED_ROWS = 32
MED_SLOTS = 24
SEL = GRAD_ROWS + 2 * MED_ROWS
NONE = -1e30
CHIPS = 4
FLOWS = 4


def contract_last(a, b):
    return lax.dot_general(a, b, (((1,), (1,)), ((), ())), preferred_element_type=F32)


def pick_kernel(where_ref, assign_ref, ids_ref, *refs):
    sk_refs, (med_ref, grad_ref, sel, code) = refs[:FLOWS], refs[FLOWS:]
    step = pl.program_id(0)

    @pl.when(step == 0)
    def _():
        base = where_ref[0]
        plane = where_ref[1]
        groups = assign_ref.shape[0]
        half = ids_ref.shape[1] // 2
        off = ids_ref[...] - base
        inside = (off >= 0) & (off < groups * LANES)
        hi = jnp.where(inside, off >> 7, -1)
        lo = off & (LANES - 1)
        j = lax.broadcasted_iota(I32, (1, 2 * half), 1)
        first = j < half
        number = (jnp.where(first, j, j - half) + 1).astype(F32)
        row = lax.broadcasted_iota(I32, (2 * groups, 2 * half), 0)
        wanted = jnp.where(first, hi, hi + groups)
        wanted = jnp.where(hi >= 0, wanted, -1)
        table = jnp.where(wanted == row, number, 0.0).astype(BF)
        lane_hot = (lo == lax.broadcasted_iota(I32, (LANES, 2 * half), 0)).astype(F32).astype(BF)
        medoid = contract_last(table, lane_hot)
        med0, med1 = medoid[:groups], medoid[groups:]
        local = assign_ref[...] - plane * (2 * half)
        mine = (local >= 0) & (local < 2 * half)
        local_lo = jnp.where(mine, (local & 255) + 1, 0).astype(F32)
        local_hi = jnp.where(mine, local >> 8, 0).astype(F32)
        flags = jnp.concatenate(
            [mine.astype(F32), (med0 > 0).astype(F32), (med1 > 0).astype(F32)], axis=0
        ).astype(BF)
        k = lax.broadcasted_iota(I32, (LANES, LANES), 0)
        b = lax.broadcasted_iota(I32, (LANES, LANES), 1)
        before = jnp.dot(flags, (k < b).astype(F32).astype(BF), preferred_element_type=F32)
        total = jnp.dot(flags, jnp.ones((LANES, LANES), BF), preferred_element_type=F32)
        slots, over = [], jnp.zeros((1, LANES), F32)
        for kind, limit in enumerate((GRAD_SLOTS, MED_SLOTS, MED_SLOTS)):
            run = jnp.zeros((1, LANES), F32)
            rows = []
            for g in range(groups):
                at = kind * groups + g
                rows.append(before[at : at + 1] + run)
                run = run + total[at : at + 1]
            over = over + jnp.where(run > limit, 1.0, 0.0)
            position = jnp.concatenate(rows, axis=0).astype(I32)
            flag = (mine, med0 > 0, med1 > 0)[kind] & (position < limit)
            slots.append(jnp.where(flag, position, -1))
        slot_g = slots[0]
        slot_m = jnp.where(slots[1] >= 0, slots[1], -1)
        slot_n = jnp.where(slots[2] >= 0, slots[2] + MED_ROWS, -1)
        grad_iota = lax.broadcasted_iota(I32, (GRAD_ROWS, LANES), 0)
        med_iota = lax.broadcasted_iota(I32, (2 * MED_ROWS, LANES), 0)
        codes = jnp.zeros((8, SEL), F32)
        zeros = jnp.zeros((5, LANES), F32)
        either = med0 + med1
        for g in range(groups):
            at = slice(g, g + 1)
            top = (slot_g[at] == grad_iota).astype(F32)
            low = ((slot_m[at] == med_iota) | (slot_n[at] == med_iota)).astype(F32)
            block = jnp.concatenate([top, low], axis=0).astype(BF)
            sel[:, g * LANES : (g + 1) * LANES] = block
            fields = jnp.concatenate(
                [either[at], local_lo[at], local_hi[at], zeros], axis=0
            ).astype(BF)
            codes = codes + contract_last(fields, block)
        marks = jnp.broadcast_to(jnp.concatenate([over, over], axis=1), (8, SEL))
        third = lax.broadcasted_iota(I32, (8, SEL), 0) == 3
        code[...] = jnp.where(third, marks, codes).astype(BF)

    codes = code[...]
    lines = jnp.concatenate([codes[:, :LANES], codes[:, LANES:]], axis=0)

    @pl.loop(0, sk_refs[0].shape[1] // SEL)
    def _(chip):
        at = pl.ds(pl.multiple_of(chip * SEL, SEL), SEL)
        block = jnp.concatenate([ref[:, at] for ref in sk_refs], axis=0)
        rows = jnp.dot(sel[...], block, preferred_element_type=F32).astype(BF)
        for c in range(2):
            to = 2 * chip + c
            grad_ref[to, :GRAD_SLOTS, :] = rows[:GRAD_SLOTS, c * LANES : (c + 1) * LANES]
            grad_ref[to, GRAD_SLOTS:, :] = lines
            at = GRAD_ROWS + c * MED_ROWS
            med_ref[to, :, :] = jnp.concatenate([rows[at : at + MED_SLOTS], codes], axis=0)


def pick(where, assignment, medoid_ids, sketches, pts_count):
    rows, feats = sketches.shape
    wide = CHIPS * 2 * LANES
    return pl.pallas_call(
        pick_kernel,
        grid_spec=pltpu.PrefetchScalarGridSpec(
            num_scalar_prefetch=1,
            grid=(feats // wide,),
            in_specs=[
                pl.BlockSpec((rows // LANES, LANES), lambda i, w: (0, 0)),
                pl.BlockSpec((1, medoid_ids.shape[0]), lambda i, w: (0, 0)),
            ]
            + [
                pl.BlockSpec((rows // FLOWS, wide), lambda i, w, k=k: (k, i))
                for k in range(FLOWS)
            ],
            out_specs=[
                pl.BlockSpec((2 * CHIPS, MED_ROWS, 2 * LANES), lambda i, w: (i, 0, 0)),
                pl.BlockSpec((2 * CHIPS, GRAD_ROWS, LANES), lambda i, w: (i, 0, 0)),
            ],
            scratch_shapes=[pltpu.VMEM((SEL, rows), BF), pltpu.VMEM((8, SEL), BF)],
        ),
        out_shape=[
            jax.ShapeDtypeStruct((pts_count, MED_ROWS, 2 * LANES), BF),
            jax.ShapeDtypeStruct((pts_count, GRAD_ROWS, LANES), BF),
        ],
        compiler_params=pltpu.CompilerParams(vmem_limit_bytes=24 * 2**20),
        cost_estimate=pl.CostEstimate(
            flops=2 * SEL * rows * feats, bytes_accessed=rows * feats * 2, transcendentals=0
        ),
        name="pick",
    )(where, assignment.reshape(-1, LANES), medoid_ids[None, :], *[sketches] * FLOWS)


def place_kernel(where_ref, got_ref, a_ref, b_ref, flag_ref):
    core = where_ref[2]
    sources = got_ref.shape[0]
    count = 2 * a_ref.shape[0]
    total = jnp.zeros((count, got_ref.shape[2]), F32)
    marks = jnp.zeros((1, LANES), F32)
    per = 2 * LANES // MED_ROWS
    iota = lax.broadcasted_iota(I32, (count, per * MED_ROWS), 0)
    for g in range(sources // per):
        numbers = []
        for q in range(g * per, (g + 1) * per):
            lines = got_ref[q, MED_SLOTS : MED_SLOTS + 8, :].astype(F32)
            line = lines[0:1]
            marks = marks + lines[3:4, :LANES]
            a = line[:, GRAD_ROWS : GRAD_ROWS + MED_ROWS]
            b = line[:, GRAD_ROWS + MED_ROWS :]
            numbers.append(jnp.where(core == 0, a, b))
        number = jnp.concatenate(numbers, axis=1).astype(I32) - 1
        hot = (number == iota).astype(F32).astype(BF)
        block = got_ref[g * per : (g + 1) * per].reshape(per * MED_ROWS, got_ref.shape[2])
        total = total + jnp.dot(hot, block, preferred_element_type=F32)
    a_ref[...] = total[: count // 2].astype(BF)
    b_ref[...] = total[count // 2 :].astype(BF)
    flag_ref[...] = jnp.concatenate([marks, marks], axis=1)


def place(where, got, count):
    return pl.pallas_call(
        place_kernel,
        in_specs=[
            pl.BlockSpec(memory_space=pltpu.SMEM),
            pl.BlockSpec(memory_space=pltpu.VMEM),
        ],
        out_specs=[pl.BlockSpec(memory_space=pltpu.VMEM)] * 3,
        out_shape=[
            jax.ShapeDtypeStruct((count // 2, got.shape[2]), BF),
            jax.ShapeDtypeStruct((count // 2, got.shape[2]), BF),
            jax.ShapeDtypeStruct((1, 2 * LANES), F32),
        ],
        compiler_params=pltpu.CompilerParams(vmem_limit_bytes=8 * 2**20),
        cost_estimate=pl.CostEstimate(
            flops=2 * count * got.size, bytes_accessed=2 * got.size, transcendentals=0
        ),
        name="place",
    )(where, got)


def sums_kernel(first, steps, got_ref, *refs):
    prior, (sums_ref, count_ref) = refs[:-2], refs[-2:]
    feats = got_ref.shape[2]
    medoids = sums_ref.shape[1]
    tail = GRAD_ROWS - LANES
    iota_a = lax.broadcasted_iota(I32, (medoids, LANES), 0)
    iota_b = lax.broadcasted_iota(I32, (medoids, tail), 0)
    ones = jnp.ones((GRAD_ROWS, LANES), BF)

    per = 4

    def body(step, total):
        hots, blocks = [], []
        for k in range(per):
            q = (first + step) * per + k
            codes = got_ref[q, GRAD_SLOTS:, :].astype(F32).astype(I32)
            a = codes[1:2] - 1 + codes[2:3] * 256
            b = (codes[9:10] - 1 + codes[10:11] * 256)[:, :tail]
            hots.append((a == iota_a).astype(F32))
            hots.append((b == iota_b).astype(F32))
            blocks.append(jnp.concatenate([got_ref[q], ones], axis=1))
        hot = jnp.concatenate(hots, axis=1).astype(BF)
        return total + jnp.dot(
            hot, jnp.concatenate(blocks, axis=0), preferred_element_type=F32
        )

    total = lax.fori_loop(
        0, steps, body, jnp.zeros((medoids, feats + LANES), F32)
    )
    sums, counts = total[:, :feats].T, total[:, feats:].T[:1]
    if prior:
        sums, counts = prior[0][...] + sums, prior[1][...] + counts
    sums_ref[...] = sums
    count_ref[...] = counts


def sums(got, medoids, first, steps, prior=()):
    return pl.pallas_call(
        functools.partial(sums_kernel, first, steps),
        in_specs=[pl.BlockSpec(memory_space=pltpu.VMEM)] * (1 + len(prior)),
        out_specs=[pl.BlockSpec(memory_space=pltpu.VMEM)] * 2,
        out_shape=[
            jax.ShapeDtypeStruct((got.shape[2], medoids), F32),
            jax.ShapeDtypeStruct((1, medoids), F32),
        ],
        compiler_params=pltpu.CompilerParams(vmem_limit_bytes=16 * 2**20),
        cost_estimate=pl.CostEstimate(
            flops=4 * medoids * got.size, bytes_accessed=2 * got.size, transcendentals=0
        ),
        name="sums",
    )(got, *prior)


def score_kernel(scale, where_ref, assign_ref, mark_ref, *refs):
    near_refs, far_refs, refs = refs[:FLOWS], refs[FLOWS : 2 * FLOWS], refs[2 * FLOWS :]
    parts, (near_out, far_out) = refs[:8], refs[8:]
    quarter, wide = parts[0].shape[1:]
    half = 2 * quarter
    x, y, base = where_ref[3], where_ref[4], where_ref[5]
    step = pl.program_id(0)
    count = pl.num_programs(0) // 2

    def stats(point_refs):
        total = jnp.zeros((half, assign_ref.shape[1]), F32)
        for kx in range(4):
            for ky in range(4):
                block = ((x + 4 - kx) & 3) * 4 + ((y + 4 - ky) & 3)
                at = pl.multiple_of(block * wide, wide)
                total = total + contract_last(
                    jnp.concatenate([parts[ky][kx], parts[4 + kx][ky]], axis=0),
                    jnp.concatenate([ref[:, pl.ds(at, wide)] for ref in point_refs], axis=0),
                )
        scores = total * scale
        best = jnp.max(scores, axis=0, keepdims=True)
        row = lax.broadcasted_iota(I32, scores.shape, 0)
        local = assign_ref[...] - base
        chosen = jnp.max(jnp.where(local == row, scores, NONE), axis=0, keepdims=True)
        return jnp.concatenate([best, chosen, mark_ref[...]], axis=0)

    @pl.when(step < count)
    def _():
        near_out[...] = stats(near_refs)

    @pl.when(step >= count)
    def _():
        far_out[...] = stats(far_refs)


def scored(where, assignments, marks, near, far, parts):
    rows, feats = near.shape
    tile = 2 * LANES
    count = rows // tile
    early = lambda i, w: (jnp.minimum(i, count - 1), 0)
    late = lambda i, w: (jnp.maximum(i - count, 0), 0)
    return pl.pallas_call(
        functools.partial(score_kernel, 1.0 / feats),
        grid_spec=pltpu.PrefetchScalarGridSpec(
            num_scalar_prefetch=1,
            grid=(2 * count,),
            in_specs=[
                pl.BlockSpec((1, tile), lambda i, w: (0, i)),
                pl.BlockSpec((1, tile), lambda i, w: (0, 0)),
            ]
            + [
                pl.BlockSpec((tile // FLOWS, feats), lambda i, w, f=f, k=k: (FLOWS * f(i, w)[0] + k, 0))
                for f in (early, late)
                for k in range(FLOWS)
            ]
            + [pl.BlockSpec(a.shape, lambda i, w: (0, 0, 0)) for a in parts],
            out_specs=[
                pl.BlockSpec((3, tile), lambda i, w: early(i, w)[::-1]),
                pl.BlockSpec((3, tile), lambda i, w: late(i, w)[::-1]),
            ],
        ),
        out_shape=[jax.ShapeDtypeStruct((3, rows), F32)] * 2,
        compiler_params=pltpu.CompilerParams(vmem_limit_bytes=32 * 2**20),
        cost_estimate=pl.CostEstimate(
            flops=4 * rows * feats * 256, bytes_accessed=rows * feats * 4, transcendentals=0
        ),
        name="scored",
    )(where, assignments, marks, *[near] * FLOWS, *[far] * FLOWS, *parts)


def closing_kernel(a_ref, b_ref, gap_ref, send_ref, mark_ref):
    both = jnp.maximum(a_ref[...], b_ref[...])
    gap_ref[...] = both[0:1] - both[1:2]
    mark_ref[0, 0] = jnp.max(both[2:3, :LANES]).astype(I32)
    total = jnp.broadcast_to(jnp.sum(both[0:1], axis=1, keepdims=True), (1, LANES))
    for i in range(send_ref.shape[0]):
        send_ref[i] = total


def closing(a, b, pts_count):
    return pl.pallas_call(
        closing_kernel,
        in_specs=[pl.BlockSpec(memory_space=pltpu.VMEM)] * 2,
        out_specs=[
            pl.BlockSpec(memory_space=pltpu.VMEM),
            pl.BlockSpec(memory_space=pltpu.VMEM),
            pl.BlockSpec(memory_space=pltpu.SMEM),
        ],
        out_shape=[
            jax.ShapeDtypeStruct((1, a.shape[1]), F32),
            jax.ShapeDtypeStruct((pts_count, 1, LANES), F32),
            jax.ShapeDtypeStruct((1, 1), I32),
        ],
        compiler_params=pltpu.CompilerParams(vmem_limit_bytes=4 * 2**20),
        cost_estimate=pl.CostEstimate(
            flops=a.size, bytes_accessed=8 * a.size, transcendentals=0
        ),
        name="closing",
    )(a, b)


def from_everyone(array, axis):
    size = lax.axis_size(axis)
    return lax.all_to_all(
        jnp.broadcast_to(array[None], (size, *array.shape)), axis, 0, 0, tiled=True
    )


def chip_of(p):
    return p // 8, (p // 2) % 4, p % 2


def shifted(array, dx, dy, dc):
    pairs = []
    for p in range(32):
        x, y, c = chip_of(p)
        pairs.append((p, (((x + dx) % 4) * 4 + (y + dy) % 4) * 2 + (c ^ dc)))
    return lax.ppermute(array, "pts", pairs)


def across(array, core, step, planes):
    pairs = [
        (p * planes + z, (p ^ core) * planes + (z ^ step))
        for p in range(32)
        for z in range(planes)
    ]
    return lax.ppermute(array, ("pts", "med"), pairs)


def general(sketches, assignment, medoid_ids):
    row_count, feat_width = sketches.shape
    medoid_count = medoid_ids.shape[0]
    pts_count = lax.axis_size("pts")
    part = feat_width // pts_count
    pts_index = lax.axis_index("pts")
    med_index = lax.axis_index("med")
    local_assign = assignment - med_index * medoid_count
    chosen = local_assign[:, None] == jnp.arange(medoid_count, dtype=I32)[None, :]
    one_hot = chosen.astype(BF)
    offsets = medoid_ids - pts_index * row_count
    picking = offsets[:, None] == jnp.arange(row_count, dtype=I32)[None, :]
    terms = jnp.dot(picking.astype(BF), sketches, preferred_element_type=F32).astype(BF)
    terms = terms.reshape(medoid_count, pts_count, part).swapaxes(0, 1)
    piece = (
        lax.all_to_all(terms, "pts", 0, 0, tiled=True).astype(F32).sum(axis=0).astype(BF)
    )
    everything = from_everyone(piece, "pts").swapaxes(0, 1).reshape(medoid_count, feat_width)
    partial = lax.dot_general(
        sketches, one_hot, (((0,), (0,)), ((), ())), preferred_element_type=F32
    ).reshape(pts_count, part, medoid_count)
    gradient_sums = lax.all_to_all(partial, "pts", 0, 0, tiled=True).sum(axis=0)
    counts = from_everyone(jnp.sum(one_hot.astype(F32), axis=0), "pts").sum(axis=0)
    scores = contract_last(sketches, everything) * (1.0 / feat_width)
    best = jnp.max(scores, axis=1)
    taken = jnp.max(jnp.where(chosen, scores, NONE), axis=1)
    both = from_everyone(jnp.stack([best, taken]), "med").max(axis=0)
    cover = from_everyone(jnp.sum(both[0])[None], "pts").sum()
    return both[0] - both[1], cover / (row_count * pts_count), counts, gradient_sums


def shards(sketches, assignment, medoid_ids):
    row_count, _ = sketches.shape
    medoid_count = medoid_ids.shape[0]
    half = medoid_count // 2
    pts_count = lax.axis_size("pts")
    p = lax.axis_index("pts")
    m = lax.axis_index("med")
    core = p % 2
    planes = lax.axis_size("med")
    where = jnp.stack(
        [p * row_count, m, core, p // 8, (p // 2) % 4, m * medoid_count + core * half, m, m]
    ).astype(I32)

    far = shifted(sketches, 0, 0, 1)
    far_assignment = shifted(assignment, 0, 0, 1)
    med_send, grad_send = pick(
        where, assignment, medoid_ids, sketches, pts_count
    )
    med_got = lax.all_to_all(med_send, "pts", 0, 0, tiled=True)
    a, b, marks = place(where, med_got, half)
    pa = jnp.stack([a] + [shifted(a, k, 0, 0) for k in (1, 2, 3)])
    pb = jnp.stack([b] + [shifted(b, 0, k, 0) for k in (1, 2, 3)])
    qa = [pa, shifted(pa, 0, 1, 0)]
    qa = qa + [shifted(pa, 0, k, 0) for k in (2, 3)]
    qb = [pb] + [shifted(pb, k, 0, 0) for k in (1, 2, 3)]
    grad_got = lax.all_to_all(grad_send, "pts", 0, 0, tiled=True)
    assignments = jnp.concatenate([assignment, far_assignment])[None, :]
    stats, theirs = scored(where, assignments, marks, sketches, far, qa + qb)
    stats = jnp.maximum(
        jnp.maximum(stats, across(stats, 0, 1, planes)),
        jnp.maximum(across(theirs, 1, 0, planes), across(theirs, 1, 1, planes)),
    )
    stats = jnp.maximum(stats, across(stats, 0, 2, planes))
    final = across(stats, 0, 4, planes)
    early = sums(grad_got, medoid_count, 0, 4)
    gap, total, mark = closing(stats, final, pts_count)
    full = mark[0, 0] > 0

    def fast():
        totals = lax.all_to_all(total, "pts", 0, 0, tiled=True)
        gradient_sums, counts = sums(grad_got, medoid_count, 4, 4, early)
        coverage = jnp.sum(totals[:, 0, 0]) / (row_count * pts_count)
        return gap[0], coverage, counts[0], gradient_sums

    return lax.cond(full, lambda: general(sketches, assignment, medoid_ids), fast)


def solution(mesh):
    in_specs = (P("pts", None), P("pts"), P("med"))
    out_specs = (P("pts"), P(), P("med"), P("pts", "med"))
    return jax.shard_map(
        shards, mesh=mesh, in_specs=in_specs, out_specs=out_specs, check_vma=False
    )
```

```python
import functools

import jax
import jax.numpy as jnp
from jax import lax
from jax.experimental import pallas as pl
from jax.experimental.pallas import tpu as pltpu
from jax.sharding import PartitionSpec as P


BF = jnp.bfloat16
F32 = jnp.float32
I32 = jnp.int32
LANES = 128
GRAD_ROWS = 192
GRAD_SLOTS = 176
MED_ROWS = 32
MED_SLOTS = 24
SEL = GRAD_ROWS + 2 * MED_ROWS
NONE = -1e30
MED = ("zq", "zr")
CHIPS = 4


def contract_last(a, b):
    return lax.dot_general(a, b, (((1,), (1,)), ((), ())), preferred_element_type=F32)


def pick_kernel(where_ref, assign_ref, ids_ref, sk_ref, med_ref, grad_ref, sel, code, held, arrived):
    flows, _, wide = held.shape

    def fetch(k):
        at = pl.ds(pl.multiple_of(k * wide, wide), wide)
        return pltpu.make_async_copy(sk_ref.at[:, at], held.at[k], arrived.at[k])

    for k in range(flows):
        fetch(k).start()

    def tables():
        base = where_ref[0]
        plane = where_ref[1]
        groups = assign_ref.shape[0]
        half = ids_ref.shape[1] // 2
        off = ids_ref[...] - base
        inside = (off >= 0) & (off < groups * LANES)
        hi = jnp.where(inside, off >> 7, -1)
        lo = off & (LANES - 1)
        j = lax.broadcasted_iota(I32, (1, 2 * half), 1)
        first = j < half
        number = (jnp.where(first, j, j - half) + 1).astype(F32)
        row = lax.broadcasted_iota(I32, (2 * groups, 2 * half), 0)
        wanted = jnp.where(first, hi, hi + groups)
        wanted = jnp.where(hi >= 0, wanted, -1)
        table = jnp.where(wanted == row, number, 0.0).astype(BF)
        lane_hot = (lo == lax.broadcasted_iota(I32, (LANES, 2 * half), 0)).astype(F32).astype(BF)
        medoid = contract_last(table, lane_hot)
        med0, med1 = medoid[:groups], medoid[groups:]
        local = assign_ref[...] - plane * (2 * half)
        mine = (local >= 0) & (local < 2 * half)
        local_lo = jnp.where(mine, (local & 255) + 1, 0).astype(F32)
        local_hi = jnp.where(mine, local >> 8, 0).astype(F32)
        flags = jnp.concatenate(
            [mine.astype(F32), (med0 > 0).astype(F32), (med1 > 0).astype(F32)], axis=0
        ).astype(BF)
        k = lax.broadcasted_iota(I32, (LANES, LANES), 0)
        b = lax.broadcasted_iota(I32, (LANES, LANES), 1)
        before = jnp.dot(flags, (k < b).astype(F32).astype(BF), preferred_element_type=F32)
        total = jnp.dot(flags, jnp.ones((LANES, LANES), BF), preferred_element_type=F32)
        slots, over = [], jnp.zeros((1, LANES), F32)
        for kind, limit in enumerate((GRAD_SLOTS, MED_SLOTS, MED_SLOTS)):
            run = jnp.zeros((1, LANES), F32)
            rows = []
            for g in range(groups):
                at = kind * groups + g
                rows.append(before[at : at + 1] + run)
                run = run + total[at : at + 1]
            over = over + jnp.where(run > limit, 1.0, 0.0)
            position = jnp.concatenate(rows, axis=0).astype(I32)
            flag = (mine, med0 > 0, med1 > 0)[kind] & (position < limit)
            slots.append(jnp.where(flag, position, -1))
        slot_g = slots[0]
        slot_m = jnp.where(slots[1] >= 0, slots[1], -1)
        slot_n = jnp.where(slots[2] >= 0, slots[2] + MED_ROWS, -1)
        grad_iota = lax.broadcasted_iota(I32, (GRAD_ROWS, LANES), 0)
        med_iota = lax.broadcasted_iota(I32, (2 * MED_ROWS, LANES), 0)
        codes = jnp.zeros((8, SEL), F32)
        zeros = jnp.zeros((5, LANES), F32)
        either = med0 + med1
        for g in range(groups):
            at = slice(g, g + 1)
            top = (slot_g[at] == grad_iota).astype(F32)
            low = ((slot_m[at] == med_iota) | (slot_n[at] == med_iota)).astype(F32)
            block = jnp.concatenate([top, low], axis=0).astype(BF)
            sel[:, g * LANES : (g + 1) * LANES] = block
            fields = jnp.concatenate(
                [either[at], local_lo[at], local_hi[at], zeros], axis=0
            ).astype(BF)
            codes = codes + contract_last(fields, block)
        marks = jnp.broadcast_to(jnp.concatenate([over, over], axis=1), (8, SEL))
        third = lax.broadcasted_iota(I32, (8, SEL), 0) == 3
        code[...] = jnp.where(third, marks, codes).astype(BF)

    tables()
    codes = code[...]
    lines = jnp.concatenate([codes[:, :LANES], codes[:, LANES:]], axis=0)

    @pl.loop(0, flows)
    def _(k):
        fetch(k).wait()
        for chip in range(wide // SEL):
            block = held[k, :, chip * SEL : (chip + 1) * SEL]
            rows = jnp.dot(sel[...], block, preferred_element_type=F32).astype(BF)
            for c in range(2):
                to = k * 2 * (wide // SEL) + 2 * chip + c
                grad_ref[to, :GRAD_SLOTS, :] = rows[:GRAD_SLOTS, c * LANES : (c + 1) * LANES]
                grad_ref[to, GRAD_SLOTS:, :] = lines
                at = GRAD_ROWS + c * MED_ROWS
                med_ref[to, :, :] = jnp.concatenate([rows[at : at + MED_SLOTS], codes], axis=0)


def pick(where, assignment, medoid_ids, sketches, pts_count):
    rows, feats = sketches.shape
    wide = CHIPS * 2 * LANES
    flows = feats // wide
    near = pl.BlockSpec(memory_space=pltpu.VMEM)
    return pl.pallas_call(
        pick_kernel,
        in_specs=[
            pl.BlockSpec(memory_space=pltpu.SMEM),
            near,
            near,
            pl.BlockSpec(memory_space=pl.ANY),
        ],
        out_specs=[near, near],
        scratch_shapes=[
            pltpu.VMEM((SEL, rows), BF),
            pltpu.VMEM((8, SEL), BF),
            pltpu.VMEM((flows, rows, wide), BF),
            pltpu.SemaphoreType.DMA((flows,)),
        ],
        out_shape=[
            jax.ShapeDtypeStruct((pts_count, MED_ROWS, 2 * LANES), BF),
            jax.ShapeDtypeStruct((pts_count, GRAD_ROWS, LANES), BF),
        ],
        compiler_params=pltpu.CompilerParams(vmem_limit_bytes=24 * 2**20),
        cost_estimate=pl.CostEstimate(
            flops=2 * SEL * rows * feats, bytes_accessed=rows * feats * 2, transcendentals=0
        ),
        name="pick",
    )(where, assignment.reshape(-1, LANES), medoid_ids[None, :], sketches)


def place_kernel(where_ref, got_ref, a_ref, b_ref, flag_ref):
    core = where_ref[2]
    sources = got_ref.shape[0]
    count = 2 * a_ref.shape[0]
    total = jnp.zeros((count, got_ref.shape[2]), F32)
    marks = jnp.zeros((1, LANES), F32)
    per = 2 * LANES // MED_ROWS
    iota = lax.broadcasted_iota(I32, (count, per * MED_ROWS), 0)
    for g in range(sources // per):
        numbers = []
        for q in range(g * per, (g + 1) * per):
            lines = got_ref[q, MED_SLOTS : MED_SLOTS + 8, :].astype(F32)
            line = lines[0:1]
            marks = marks + lines[3:4, :LANES]
            a = line[:, GRAD_ROWS : GRAD_ROWS + MED_ROWS]
            b = line[:, GRAD_ROWS + MED_ROWS :]
            numbers.append(jnp.where(core == 0, a, b))
        number = jnp.concatenate(numbers, axis=1).astype(I32) - 1
        hot = (number == iota).astype(F32).astype(BF)
        block = got_ref[g * per : (g + 1) * per].reshape(per * MED_ROWS, got_ref.shape[2])
        total = total + jnp.dot(hot, block, preferred_element_type=F32)
    a_ref[...] = total[: count // 2].astype(BF)
    b_ref[...] = total[count // 2 :].astype(BF)
    flag_ref[...] = jnp.concatenate([marks, marks], axis=1)


def place(where, got, count):
    return pl.pallas_call(
        place_kernel,
        in_specs=[
            pl.BlockSpec(memory_space=pltpu.SMEM),
            pl.BlockSpec(memory_space=pltpu.VMEM),
        ],
        out_specs=[pl.BlockSpec(memory_space=pltpu.VMEM)] * 3,
        out_shape=[
            jax.ShapeDtypeStruct((count // 2, got.shape[2]), BF),
            jax.ShapeDtypeStruct((count // 2, got.shape[2]), BF),
            jax.ShapeDtypeStruct((1, 2 * LANES), F32),
        ],
        compiler_params=pltpu.CompilerParams(vmem_limit_bytes=8 * 2**20),
        cost_estimate=pl.CostEstimate(
            flops=2 * count * got.size, bytes_accessed=2 * got.size, transcendentals=0
        ),
        name="place",
    )(where, got)


def sums_kernel(first, steps, got_ref, *refs):
    prior, (sums_ref, count_ref) = refs[:-2], refs[-2:]
    feats = got_ref.shape[2]
    medoids = sums_ref.shape[1]
    tail = GRAD_ROWS - LANES
    iota_a = lax.broadcasted_iota(I32, (medoids, LANES), 0)
    iota_b = lax.broadcasted_iota(I32, (medoids, tail), 0)
    ones = jnp.ones((GRAD_ROWS, LANES), BF)

    per = 4

    def body(step, total):
        hots, blocks = [], []
        for k in range(per):
            q = (first + step) * per + k
            codes = got_ref[q, GRAD_SLOTS:, :].astype(F32).astype(I32)
            a = codes[1:2] - 1 + codes[2:3] * 256
            b = (codes[9:10] - 1 + codes[10:11] * 256)[:, :tail]
            hots.append((a == iota_a).astype(F32))
            hots.append((b == iota_b).astype(F32))
            blocks.append(jnp.concatenate([got_ref[q], ones], axis=1))
        hot = jnp.concatenate(hots, axis=1).astype(BF)
        return total + jnp.dot(
            hot, jnp.concatenate(blocks, axis=0), preferred_element_type=F32
        )

    total = lax.fori_loop(
        0, steps, body, jnp.zeros((medoids, feats + LANES), F32)
    )
    sums, counts = total[:, :feats].T, total[:, feats:].T[:1]
    if prior:
        sums, counts = prior[0][...] + sums, prior[1][...] + counts
    sums_ref[...] = sums
    count_ref[...] = counts


def sums(got, medoids, first, steps, prior=()):
    return pl.pallas_call(
        functools.partial(sums_kernel, first, steps),
        in_specs=[pl.BlockSpec(memory_space=pltpu.VMEM)] * (1 + len(prior)),
        out_specs=[pl.BlockSpec(memory_space=pltpu.VMEM)] * 2,
        out_shape=[
            jax.ShapeDtypeStruct((got.shape[2], medoids), F32),
            jax.ShapeDtypeStruct((1, medoids), F32),
        ],
        compiler_params=pltpu.CompilerParams(vmem_limit_bytes=16 * 2**20),
        cost_estimate=pl.CostEstimate(
            flops=4 * medoids * got.size, bytes_accessed=2 * got.size, transcendentals=0
        ),
        name="sums",
    )(got, *prior)


def score_kernel(scale, where_ref, assign_ref, mark_ref, near_ref, far_ref, *refs):
    parts, (near_out, far_out, held, arrived) = refs[:8], refs[8:]
    quarter, wide = parts[0].shape[1:]
    half = 2 * quarter
    x, y, base = where_ref[3], where_ref[4], where_ref[5]
    tile = 2 * LANES
    count = near_ref.shape[0] // tile

    def fetch(side, i):
        at = pl.ds(pl.multiple_of(i * tile, tile), tile)
        return pltpu.make_async_copy(
            (near_ref, far_ref)[side].at[at], held.at[side, at], arrived.at[side, i]
        )

    for side in range(2):
        for i in range(count):
            fetch(side, i).start()

    for side in range(2):

        @pl.loop(0, count)
        def _(i):
            fetch(side, i).wait()
            at = pl.ds(pl.multiple_of(i * tile, tile), tile)
            total = jnp.zeros((half, tile), F32)
            for kx in range(4):
                for ky in range(4):
                    block = ((x + 4 - kx) & 3) * 4 + ((y + 4 - ky) & 3)
                    columns = pl.ds(pl.multiple_of(block * wide, wide), wide)
                    total = total + contract_last(
                        jnp.concatenate([parts[ky][kx], parts[4 + kx][ky]], axis=0),
                        held[side, at, columns],
                    )
            scores = total * scale
            best = jnp.max(scores, axis=0, keepdims=True)
            row = lax.broadcasted_iota(I32, scores.shape, 0)
            local = assign_ref[side : side + 1, at] - base
            chosen = jnp.max(jnp.where(local == row, scores, NONE), axis=0, keepdims=True)
            out_ref = (near_out, far_out)[side]
            out_ref[:, at] = jnp.concatenate([best, chosen, mark_ref[...]], axis=0)


def scored(where, assignments, marks, near, far, parts):
    rows, feats = near.shape
    local = pl.BlockSpec(memory_space=pltpu.VMEM)
    away = pl.BlockSpec(memory_space=pl.ANY)
    return pl.pallas_call(
        functools.partial(score_kernel, 1.0 / feats),
        in_specs=[pl.BlockSpec(memory_space=pltpu.SMEM), local, local, away, away]
        + [local] * len(parts),
        out_specs=[local, local],
        scratch_shapes=[
            pltpu.VMEM((2, rows, feats), BF),
            pltpu.SemaphoreType.DMA((2, rows // (2 * LANES))),
        ],
        out_shape=[jax.ShapeDtypeStruct((3, rows), F32)] * 2,
        compiler_params=pltpu.CompilerParams(vmem_limit_bytes=32 * 2**20),
        cost_estimate=pl.CostEstimate(
            flops=4 * rows * feats * 256, bytes_accessed=rows * feats * 4, transcendentals=0
        ),
        name="scored",
    )(where, assignments, marks, near, far, *parts)


def closing_kernel(a_ref, b_ref, gap_ref, mark_ref):
    both = jnp.maximum(a_ref[...], b_ref[...])
    gap_ref[...] = both[0:1] - both[1:2]
    mark_ref[0, 0] = jnp.max(both[2:3, :LANES]).astype(I32)


def closing(a, b):
    return pl.pallas_call(
        closing_kernel,
        in_specs=[pl.BlockSpec(memory_space=pltpu.VMEM)] * 2,
        out_specs=[
            pl.BlockSpec(memory_space=pltpu.VMEM),
            pl.BlockSpec(memory_space=pltpu.SMEM),
        ],
        out_shape=[
            jax.ShapeDtypeStruct((1, a.shape[1]), F32),
            jax.ShapeDtypeStruct((1, 1), I32),
        ],
        compiler_params=pltpu.CompilerParams(vmem_limit_bytes=4 * 2**20),
        cost_estimate=pl.CostEstimate(
            flops=a.size, bytes_accessed=8 * a.size, transcendentals=0
        ),
        name="closing",
    )(a, b)


def cover_kernel(scale, got_ref, out_ref):
    total = jnp.zeros(got_ref.shape[1:], F32)
    for i in range(0, got_ref.shape[0], 2):
        total = total + jnp.maximum(got_ref[i], got_ref[i + 1])
    out_ref[0, 0] = jnp.sum(total) * scale


def cover(got):
    points = got.shape[0] // 2 * got.shape[2]
    return pl.pallas_call(
        functools.partial(cover_kernel, 1.0 / points),
        in_specs=[pl.BlockSpec(memory_space=pltpu.VMEM)],
        out_specs=pl.BlockSpec(memory_space=pltpu.SMEM),
        out_shape=jax.ShapeDtypeStruct((1, 1), F32),
        compiler_params=pltpu.CompilerParams(vmem_limit_bytes=4 * 2**20),
        cost_estimate=pl.CostEstimate(
            flops=got.size, bytes_accessed=4 * got.size, transcendentals=0
        ),
        name="cover",
    )(got)


def from_everyone(array, axis):
    size = lax.axis_size(axis)
    return lax.all_to_all(
        jnp.broadcast_to(array[None], (size, *array.shape)), axis, 0, 0, tiled=True
    )


def chip_of(p):
    return p // 8, (p // 2) % 4, p % 2


def shifted(array, dx, dy, dc):
    pairs = []
    for p in range(32):
        x, y, c = chip_of(p)
        pairs.append((p, (((x + dx) % 4) * 4 + (y + dy) % 4) * 2 + (c ^ dc)))
    return lax.ppermute(array, "pts", pairs)


def across(array, core, step, planes):
    pairs = [
        (p * planes + z, (p ^ core) * planes + (z ^ step))
        for p in range(32)
        for z in range(planes)
    ]
    return lax.ppermute(array, ("pts", *MED), pairs)


def general(sketches, assignment, medoid_ids):
    row_count, feat_width = sketches.shape
    medoid_count = medoid_ids.shape[0]
    pts_count = lax.axis_size("pts")
    part = feat_width // pts_count
    pts_index = lax.axis_index("pts")
    med_index = lax.axis_index(MED)
    local_assign = assignment - med_index * medoid_count
    chosen = local_assign[:, None] == jnp.arange(medoid_count, dtype=I32)[None, :]
    one_hot = chosen.astype(BF)
    offsets = medoid_ids - pts_index * row_count
    picking = offsets[:, None] == jnp.arange(row_count, dtype=I32)[None, :]
    terms = jnp.dot(picking.astype(BF), sketches, preferred_element_type=F32).astype(BF)
    terms = terms.reshape(medoid_count, pts_count, part).swapaxes(0, 1)
    piece = (
        lax.all_to_all(terms, "pts", 0, 0, tiled=True).astype(F32).sum(axis=0).astype(BF)
    )
    everything = from_everyone(piece, "pts").swapaxes(0, 1).reshape(medoid_count, feat_width)
    partial = lax.dot_general(
        sketches, one_hot, (((0,), (0,)), ((), ())), preferred_element_type=F32
    ).reshape(pts_count, part, medoid_count)
    gradient_sums = lax.all_to_all(partial, "pts", 0, 0, tiled=True).sum(axis=0)
    counts = from_everyone(jnp.sum(one_hot.astype(F32), axis=0), "pts").sum(axis=0)
    scores = contract_last(sketches, everything) * (1.0 / feat_width)
    best = jnp.max(scores, axis=1)
    taken = jnp.max(jnp.where(chosen, scores, NONE), axis=1)
    both = from_everyone(jnp.stack([best, taken]), MED).max(axis=0)
    cover = from_everyone(jnp.sum(both[0])[None], "pts").sum()
    return both[0] - both[1], cover / (row_count * pts_count), counts, gradient_sums


def shards(sketches, assignment, medoid_ids):
    row_count, _ = sketches.shape
    medoid_count = medoid_ids.shape[0]
    half = medoid_count // 2
    pts_count = lax.axis_size("pts")
    p = lax.axis_index("pts")
    m = lax.axis_index(MED)
    core = p % 2
    planes = lax.axis_size(MED)
    where = jnp.stack(
        [p * row_count, m, core, p // 8, (p // 2) % 4, m * medoid_count + core * half, m, m]
    ).astype(I32)

    far = shifted(sketches, 0, 0, 1)
    far_assignment = shifted(assignment, 0, 0, 1)
    med_send, grad_send = pick(
        where, assignment, medoid_ids, sketches, pts_count
    )
    med_got = lax.all_to_all(med_send, "pts", 0, 0, tiled=True)
    a, b, marks = place(where, med_got, half)
    pa = jnp.stack([a] + [shifted(a, k, 0, 0) for k in (1, 2, 3)])
    pb = jnp.stack([b] + [shifted(b, 0, k, 0) for k in (1, 2, 3)])
    qa = [pa, shifted(pa, 0, 1, 0)]
    qa = qa + [shifted(pa, 0, k, 0) for k in (2, 3)]
    qb = [pb] + [shifted(pb, k, 0, 0) for k in (1, 2, 3)]
    grad_got = lax.all_to_all(grad_send, "pts", 0, 0, tiled=True)
    assignments = jnp.stack([assignment, far_assignment])
    stats, theirs = scored(where, assignments, marks, sketches, far, qa + qb)
    stats = jnp.maximum(
        jnp.maximum(stats, across(stats, 0, 4, planes)),
        jnp.maximum(across(theirs, 1, 0, planes), across(theirs, 1, 4, planes)),
    )
    stats = jnp.maximum(stats, across(stats, 0, 2, planes))
    final = across(stats, 0, 1, planes)
    size = 2 * pts_count
    everyone = lax.all_to_all(
        jnp.broadcast_to(stats[None, :1], (size, 1, row_count)),
        ("pts", MED[1]),
        0,
        0,
        tiled=True,
    )
    gradient_sums, counts = sums(grad_got, medoid_count, 0, 8)
    gap, mark = closing(stats, final)
    full = mark[0, 0] > 0

    def fast():
        return gap[0], cover(everyone)[0, 0], counts[0], gradient_sums

    return lax.cond(full, lambda: general(sketches, assignment, medoid_ids), fast)


def solution(mesh):
    planes = mesh.shape["med"]
    mesh = jax.sharding.Mesh(
        mesh.devices.reshape(-1, planes // 2, 2), ("pts", *MED)
    )
    in_specs = (P("pts", None), P("pts"), P(MED))
    out_specs = (P("pts"), P(), P(MED), P("pts", MED))
    return jax.shard_map(
        shards, mesh=mesh, in_specs=in_specs, out_specs=out_specs, check_vma=False
    )
```

```python
import functools

import jax
import jax.numpy as jnp
from jax import lax
from jax.experimental import pallas as pl
from jax.experimental.pallas import tpu as pltpu
from jax.sharding import PartitionSpec as P


BF = jnp.bfloat16
F32 = jnp.float32
I32 = jnp.int32
LANES = 128
GRAD_ROWS = 192
GRAD_SLOTS = 176
MED_ROWS = 32
MED_SLOTS = 24
SEL = GRAD_ROWS + 2 * MED_ROWS
NONE = -1e30
LOST = 1e30
MED = ("zq", "zr")
CHIPS = 4


def contract_last(a, b):
    return lax.dot_general(a, b, (((1,), (1,)), ((), ())), preferred_element_type=F32)


def pick_kernel(where_ref, assign_ref, ids_ref, sk_ref, med_ref, grad_ref, sel, code, held, arrived):
    flows, _, wide = held.shape

    def fetch(k):
        at = pl.ds(pl.multiple_of(k * wide, wide), wide)
        return pltpu.make_async_copy(sk_ref.at[:, at], held.at[k], arrived.at[k])

    for k in range(flows):
        fetch(k).start()

    def tables():
        base = where_ref[0]
        plane = where_ref[1]
        groups = assign_ref.shape[0]
        half = ids_ref.shape[1] // 2
        off = ids_ref[...] - base
        inside = (off >= 0) & (off < groups * LANES)
        hi = jnp.where(inside, off >> 7, -1)
        lo = off & (LANES - 1)
        j = lax.broadcasted_iota(I32, (1, 2 * half), 1)
        first = j < half
        number = (jnp.where(first, j, j - half) + 1).astype(F32)
        row = lax.broadcasted_iota(I32, (2 * groups, 2 * half), 0)
        wanted = jnp.where(first, hi, hi + groups)
        wanted = jnp.where(hi >= 0, wanted, -1)
        table = jnp.where(wanted == row, number, 0.0).astype(BF)
        lane_hot = (lo == lax.broadcasted_iota(I32, (LANES, 2 * half), 0)).astype(F32).astype(BF)
        medoid = contract_last(table, lane_hot)
        med0, med1 = medoid[:groups], medoid[groups:]
        local = assign_ref[...] - plane * (2 * half)
        mine = (local >= 0) & (local < 2 * half)
        local_lo = jnp.where(mine, (local & 255) + 1, 0).astype(F32)
        local_hi = jnp.where(mine, local >> 8, 0).astype(F32)
        flags = jnp.concatenate(
            [mine.astype(F32), (med0 > 0).astype(F32), (med1 > 0).astype(F32)], axis=0
        ).astype(BF)
        k = lax.broadcasted_iota(I32, (LANES, LANES), 0)
        b = lax.broadcasted_iota(I32, (LANES, LANES), 1)
        before = jnp.dot(flags, (k < b).astype(F32).astype(BF), preferred_element_type=F32)
        total = jnp.dot(flags, jnp.ones((LANES, LANES), BF), preferred_element_type=F32)
        slots, over = [], jnp.zeros((1, LANES), F32)
        for kind, limit in enumerate((GRAD_SLOTS, MED_SLOTS, MED_SLOTS)):
            run = jnp.zeros((1, LANES), F32)
            rows = []
            for g in range(groups):
                at = kind * groups + g
                rows.append(before[at : at + 1] + run)
                run = run + total[at : at + 1]
            over = over + jnp.where(run > limit, 1.0, 0.0)
            position = jnp.concatenate(rows, axis=0).astype(I32)
            flag = (mine, med0 > 0, med1 > 0)[kind] & (position < limit)
            slots.append(jnp.where(flag, position, -1))
        slot_g = slots[0]
        slot_m = jnp.where(slots[1] >= 0, slots[1], -1)
        slot_n = jnp.where(slots[2] >= 0, slots[2] + MED_ROWS, -1)
        grad_iota = lax.broadcasted_iota(I32, (GRAD_ROWS, LANES), 0)
        med_iota = lax.broadcasted_iota(I32, (2 * MED_ROWS, LANES), 0)
        codes = jnp.zeros((8, SEL), F32)
        zeros = jnp.zeros((5, LANES), F32)
        either = med0 + med1
        for g in range(groups):
            at = slice(g, g + 1)
            top = (slot_g[at] == grad_iota).astype(F32)
            low = ((slot_m[at] == med_iota) | (slot_n[at] == med_iota)).astype(F32)
            block = jnp.concatenate([top, low], axis=0).astype(BF)
            sel[:, g * LANES : (g + 1) * LANES] = block
            fields = jnp.concatenate(
                [either[at], local_lo[at], local_hi[at], zeros], axis=0
            ).astype(BF)
            codes = codes + contract_last(fields, block)
        marks = jnp.broadcast_to(jnp.concatenate([over, over], axis=1), (8, SEL))
        third = lax.broadcasted_iota(I32, (8, SEL), 0) == 3
        code[...] = jnp.where(third, marks, codes).astype(BF)

    tables()
    codes = code[...]
    lines = jnp.concatenate([codes[:, :LANES], codes[:, LANES:]], axis=0)

    @pl.loop(0, flows)
    def _(k):
        fetch(k).wait()
        for chip in range(wide // SEL):
            block = held[k, :, chip * SEL : (chip + 1) * SEL]
            rows = jnp.dot(sel[...], block, preferred_element_type=F32).astype(BF)
            for c in range(2):
                to = k * 2 * (wide // SEL) + 2 * chip + c
                grad_ref[to, :GRAD_SLOTS, :] = rows[:GRAD_SLOTS, c * LANES : (c + 1) * LANES]
                grad_ref[to, GRAD_SLOTS:, :] = lines
                at = GRAD_ROWS + c * MED_ROWS
                med_ref[to, :, :] = jnp.concatenate([rows[at : at + MED_SLOTS], codes], axis=0)


def pick(where, assignment, medoid_ids, sketches, pts_count):
    rows, feats = sketches.shape
    wide = CHIPS * 2 * LANES
    flows = feats // wide
    near = pl.BlockSpec(memory_space=pltpu.VMEM)
    return pl.pallas_call(
        pick_kernel,
        in_specs=[
            pl.BlockSpec(memory_space=pltpu.SMEM),
            near,
            near,
            pl.BlockSpec(memory_space=pl.ANY),
        ],
        out_specs=[near, near],
        scratch_shapes=[
            pltpu.VMEM((SEL, rows), BF),
            pltpu.VMEM((8, SEL), BF),
            pltpu.VMEM((flows, rows, wide), BF),
            pltpu.SemaphoreType.DMA((flows,)),
        ],
        out_shape=[
            jax.ShapeDtypeStruct((pts_count, MED_ROWS, 2 * LANES), BF),
            jax.ShapeDtypeStruct((pts_count, GRAD_ROWS, LANES), BF),
        ],
        compiler_params=pltpu.CompilerParams(vmem_limit_bytes=24 * 2**20),
        cost_estimate=pl.CostEstimate(
            flops=2 * SEL * rows * feats, bytes_accessed=rows * feats * 2, transcendentals=0
        ),
        name="pick",
    )(where, assignment.reshape(-1, LANES), medoid_ids[None, :], sketches)


def place_kernel(where_ref, got_ref, a_ref, b_ref, flag_ref):
    core = where_ref[2]
    sources = got_ref.shape[0]
    count = 2 * a_ref.shape[0]
    total = jnp.zeros((count, got_ref.shape[2]), F32)
    marks = jnp.zeros((1, LANES), F32)
    per = 2 * LANES // MED_ROWS
    iota = lax.broadcasted_iota(I32, (count, per * MED_ROWS), 0)
    for g in range(sources // per):
        numbers = []
        for q in range(g * per, (g + 1) * per):
            lines = got_ref[q, MED_SLOTS : MED_SLOTS + 8, :].astype(F32)
            line = lines[0:1]
            marks = marks + lines[3:4, :LANES]
            a = line[:, GRAD_ROWS : GRAD_ROWS + MED_ROWS]
            b = line[:, GRAD_ROWS + MED_ROWS :]
            numbers.append(jnp.where(core == 0, a, b))
        number = jnp.concatenate(numbers, axis=1).astype(I32) - 1
        hot = (number == iota).astype(F32).astype(BF)
        block = got_ref[g * per : (g + 1) * per].reshape(per * MED_ROWS, got_ref.shape[2])
        total = total + jnp.dot(hot, block, preferred_element_type=F32)
    a_ref[...] = total[: count // 2].astype(BF)
    b_ref[...] = total[count // 2 :].astype(BF)
    flag_ref[...] = jnp.concatenate([marks, marks], axis=1)


def place(where, got, count):
    return pl.pallas_call(
        place_kernel,
        in_specs=[
            pl.BlockSpec(memory_space=pltpu.SMEM),
            pl.BlockSpec(memory_space=pltpu.VMEM),
        ],
        out_specs=[pl.BlockSpec(memory_space=pltpu.VMEM)] * 3,
        out_shape=[
            jax.ShapeDtypeStruct((count // 2, got.shape[2]), BF),
            jax.ShapeDtypeStruct((count // 2, got.shape[2]), BF),
            jax.ShapeDtypeStruct((1, 2 * LANES), F32),
        ],
        compiler_params=pltpu.CompilerParams(vmem_limit_bytes=8 * 2**20),
        cost_estimate=pl.CostEstimate(
            flops=2 * count * got.size, bytes_accessed=2 * got.size, transcendentals=0
        ),
        name="place",
    )(where, got)


def sums_kernel(first, steps, got_ref, *refs):
    prior, (sums_ref, count_ref) = refs[:-2], refs[-2:]
    feats = got_ref.shape[2]
    medoids = sums_ref.shape[1]
    tail = GRAD_ROWS - LANES
    iota_a = lax.broadcasted_iota(I32, (medoids, LANES), 0)
    iota_b = lax.broadcasted_iota(I32, (medoids, tail), 0)
    ones = jnp.ones((GRAD_ROWS, LANES), BF)

    per = 4

    def body(step, total):
        hots, blocks = [], []
        for k in range(per):
            q = (first + step) * per + k
            codes = got_ref[q, GRAD_SLOTS:, :].astype(F32).astype(I32)
            a = codes[1:2] - 1 + codes[2:3] * 256
            b = (codes[9:10] - 1 + codes[10:11] * 256)[:, :tail]
            hots.append((a == iota_a).astype(F32))
            hots.append((b == iota_b).astype(F32))
            blocks.append(jnp.concatenate([got_ref[q], ones], axis=1))
        hot = jnp.concatenate(hots, axis=1).astype(BF)
        return total + jnp.dot(
            hot, jnp.concatenate(blocks, axis=0), preferred_element_type=F32
        )

    total = lax.fori_loop(
        0, steps, body, jnp.zeros((medoids, feats + LANES), F32)
    )
    sums, counts = total[:, :feats].T, total[:, feats:].T[:1]
    if prior:
        sums, counts = prior[0][...] + sums, prior[1][...] + counts
    sums_ref[...] = sums
    count_ref[...] = counts


def sums(got, medoids, first, steps, prior=()):
    return pl.pallas_call(
        functools.partial(sums_kernel, first, steps),
        in_specs=[pl.BlockSpec(memory_space=pltpu.VMEM)] * (1 + len(prior)),
        out_specs=[pl.BlockSpec(memory_space=pltpu.VMEM)] * 2,
        out_shape=[
            jax.ShapeDtypeStruct((got.shape[2], medoids), F32),
            jax.ShapeDtypeStruct((1, medoids), F32),
        ],
        compiler_params=pltpu.CompilerParams(vmem_limit_bytes=16 * 2**20),
        cost_estimate=pl.CostEstimate(
            flops=4 * medoids * got.size, bytes_accessed=2 * got.size, transcendentals=0
        ),
        name="sums",
    )(got, *prior)


def score_kernel(scale, where_ref, assign_ref, mark_ref, near_ref, far_ref, *refs):
    parts, (out_ref, held, arrived) = refs[:8], refs[8:]
    lost = mark_ref[...] > 0
    quarter, wide = parts[0].shape[1:]
    half = 2 * quarter
    x, y, base = where_ref[3], where_ref[4], where_ref[5]
    tile = 2 * LANES
    count = near_ref.shape[0] // tile

    def fetch(side, i):
        at = pl.ds(pl.multiple_of(i * tile, tile), tile)
        return pltpu.make_async_copy(
            (near_ref, far_ref)[side].at[at], held.at[side, at], arrived.at[side, i]
        )

    for side in range(2):
        for i in range(count):
            fetch(side, i).start()

    for side in range(2):

        @pl.loop(0, count)
        def _(i):
            fetch(side, i).wait()
            at = pl.ds(pl.multiple_of(i * tile, tile), tile)
            total = jnp.zeros((half, tile), F32)
            for kx in range(4):
                for ky in range(4):
                    block = ((x + 4 - kx) & 3) * 4 + ((y + 4 - ky) & 3)
                    columns = pl.ds(pl.multiple_of(block * wide, wide), wide)
                    total = total + contract_last(
                        jnp.concatenate([parts[ky][kx], parts[4 + kx][ky]], axis=0),
                        held[side, at, columns],
                    )
            scores = total * scale
            best = jnp.max(scores, axis=0, keepdims=True)
            row = lax.broadcasted_iota(I32, scores.shape, 0)
            local = assign_ref[side : side + 1, at] - base
            chosen = jnp.max(jnp.where(local == row, scores, NONE), axis=0, keepdims=True)
            out_ref[side : side + 1, at] = best
            out_ref[2 + side : 3 + side, at] = jnp.where(lost, LOST, chosen)


def scored(where, assignments, marks, near, far, parts):
    rows, feats = near.shape
    local = pl.BlockSpec(memory_space=pltpu.VMEM)
    away = pl.BlockSpec(memory_space=pl.ANY)
    return pl.pallas_call(
        functools.partial(score_kernel, 1.0 / feats),
        in_specs=[pl.BlockSpec(memory_space=pltpu.SMEM), local, local, away, away]
        + [local] * len(parts),
        out_specs=local,
        scratch_shapes=[
            pltpu.VMEM((2, rows, feats), BF),
            pltpu.SemaphoreType.DMA((2, rows // (2 * LANES))),
        ],
        out_shape=jax.ShapeDtypeStruct((4, rows), F32),
        compiler_params=pltpu.CompilerParams(vmem_limit_bytes=32 * 2**20),
        cost_estimate=pl.CostEstimate(
            flops=4 * rows * feats * 256, bytes_accessed=rows * feats * 4, transcendentals=0
        ),
        name="scored",
    )(where, assignments, marks, near, far, *parts)


def closing_kernel(a_ref, b_ref, c_ref, d_ref, gap_ref, mark_ref):
    same = jnp.maximum(a_ref[...], b_ref[...])
    partner = jnp.maximum(c_ref[...], d_ref[...])
    best = jnp.maximum(same[0:1], partner[1:2])
    chosen = jnp.maximum(same[2:3], partner[3:4])
    gap_ref[...] = best - chosen
    mark_ref[0, 0] = jnp.where(jnp.max(chosen) > 0.5 * LOST, 1, 0)


def closing(a, b, c, d):
    return pl.pallas_call(
        closing_kernel,
        in_specs=[pl.BlockSpec(memory_space=pltpu.VMEM)] * 4,
        out_specs=[
            pl.BlockSpec(memory_space=pltpu.VMEM),
            pl.BlockSpec(memory_space=pltpu.SMEM),
        ],
        out_shape=[
            jax.ShapeDtypeStruct((1, a.shape[1]), F32),
            jax.ShapeDtypeStruct((1, 1), I32),
        ],
        compiler_params=pltpu.CompilerParams(vmem_limit_bytes=4 * 2**20),
        cost_estimate=pl.CostEstimate(
            flops=a.size, bytes_accessed=16 * a.size, transcendentals=0
        ),
        name="closing",
    )(a, b, c, d)


def cover_kernel(scale, got_ref, out_ref):
    total = jnp.zeros((1, got_ref.shape[2]), F32)
    for i in range(0, got_ref.shape[0], 4):
        one = jnp.maximum(got_ref[i], got_ref[i + 1])
        two = jnp.maximum(got_ref[i + 2], got_ref[i + 3])
        total = total + jnp.maximum(one[0:1], two[1:2]) + jnp.maximum(one[1:2], two[0:1])
    out_ref[0, 0] = jnp.sum(total) * scale


def cover(got):
    points = got.shape[0] // 2 * got.shape[2]
    return pl.pallas_call(
        functools.partial(cover_kernel, 1.0 / points),
        in_specs=[pl.BlockSpec(memory_space=pltpu.VMEM)],
        out_specs=pl.BlockSpec(memory_space=pltpu.SMEM),
        out_shape=jax.ShapeDtypeStruct((1, 1), F32),
        compiler_params=pltpu.CompilerParams(vmem_limit_bytes=4 * 2**20),
        cost_estimate=pl.CostEstimate(
            flops=got.size, bytes_accessed=4 * got.size, transcendentals=0
        ),
        name="cover",
    )(got)


def from_everyone(array, axis):
    size = lax.axis_size(axis)
    return lax.all_to_all(
        jnp.broadcast_to(array[None], (size, *array.shape)), axis, 0, 0, tiled=True
    )


def chip_of(p):
    return p // 8, (p // 2) % 4, p % 2


def shifted(array, dx, dy, dc):
    pairs = []
    for p in range(32):
        x, y, c = chip_of(p)
        pairs.append((p, (((x + dx) % 4) * 4 + (y + dy) % 4) * 2 + (c ^ dc)))
    return lax.ppermute(array, "pts", pairs)


def across(array, core, step, planes):
    pairs = [
        (p * planes + z, (p ^ core) * planes + (z ^ step))
        for p in range(32)
        for z in range(planes)
    ]
    return lax.ppermute(array, ("pts", *MED), pairs)


def general(sketches, assignment, medoid_ids):
    row_count, feat_width = sketches.shape
    medoid_count = medoid_ids.shape[0]
    pts_count = lax.axis_size("pts")
    part = feat_width // pts_count
    pts_index = lax.axis_index("pts")
    med_index = lax.axis_index(MED)
    local_assign = assignment - med_index * medoid_count
    chosen = local_assign[:, None] == jnp.arange(medoid_count, dtype=I32)[None, :]
    one_hot = chosen.astype(BF)
    offsets = medoid_ids - pts_index * row_count
    picking = offsets[:, None] == jnp.arange(row_count, dtype=I32)[None, :]
    terms = jnp.dot(picking.astype(BF), sketches, preferred_element_type=F32).astype(BF)
    terms = terms.reshape(medoid_count, pts_count, part).swapaxes(0, 1)
    piece = (
        lax.all_to_all(terms, "pts", 0, 0, tiled=True).astype(F32).sum(axis=0).astype(BF)
    )
    everything = from_everyone(piece, "pts").swapaxes(0, 1).reshape(medoid_count, feat_width)
    partial = lax.dot_general(
        sketches, one_hot, (((0,), (0,)), ((), ())), preferred_element_type=F32
    ).reshape(pts_count, part, medoid_count)
    gradient_sums = lax.all_to_all(partial, "pts", 0, 0, tiled=True).sum(axis=0)
    counts = from_everyone(jnp.sum(one_hot.astype(F32), axis=0), "pts").sum(axis=0)
    scores = contract_last(sketches, everything) * (1.0 / feat_width)
    best = jnp.max(scores, axis=1)
    taken = jnp.max(jnp.where(chosen, scores, NONE), axis=1)
    both = from_everyone(jnp.stack([best, taken]), MED).max(axis=0)
    cover = from_everyone(jnp.sum(both[0])[None], "pts").sum()
    return both[0] - both[1], cover / (row_count * pts_count), counts, gradient_sums


def shards(sketches, assignment, medoid_ids):
    row_count, _ = sketches.shape
    medoid_count = medoid_ids.shape[0]
    half = medoid_count // 2
    pts_count = lax.axis_size("pts")
    p = lax.axis_index("pts")
    m = lax.axis_index(MED)
    core = p % 2
    planes = lax.axis_size(MED)
    where = jnp.stack(
        [p * row_count, m, core, p // 8, (p // 2) % 4, m * medoid_count + core * half, m, m]
    ).astype(I32)

    far = shifted(sketches, 0, 0, 1)
    far_assignment = shifted(assignment, 0, 0, 1)
    med_send, grad_send = pick(
        where, assignment, medoid_ids, sketches, pts_count
    )
    med_got = lax.all_to_all(med_send, "pts", 0, 0, tiled=True)
    a, b, marks = place(where, med_got, half)
    pa = jnp.stack([a] + [shifted(a, k, 0, 0) for k in (1, 2, 3)])
    pb = jnp.stack([b] + [shifted(b, 0, k, 0) for k in (1, 2, 3)])
    qa = [pa, shifted(pa, 0, 1, 0)]
    qa = qa + [shifted(pa, 0, k, 0) for k in (2, 3)]
    qb = [pb] + [shifted(pb, k, 0, 0) for k in (1, 2, 3)]
    grad_got = lax.all_to_all(grad_send, "pts", 0, 0, tiled=True)
    assignments = jnp.stack([assignment, far_assignment])
    stats = scored(where, assignments, marks, sketches, far, qa + qb)
    stats = jnp.maximum(stats, across(stats, 0, 4, planes))
    stats = jnp.maximum(stats, across(stats, 0, 2, planes))
    size = 2 * pts_count
    everyone = lax.all_to_all(
        jnp.broadcast_to(stats[None, :2], (size, 2, row_count)),
        ("pts", MED[1]),
        0,
        0,
        tiled=True,
    )
    plane = across(stats, 0, 1, planes)
    partner = across(stats, 1, 0, planes)
    both = across(stats, 1, 1, planes)
    gradient_sums, counts = sums(grad_got, medoid_count, 0, 8)
    gap, mark = closing(stats, plane, partner, both)
    full = mark[0, 0] > 0

    def fast():
        return gap[0], cover(everyone)[0, 0], counts[0], gradient_sums

    return lax.cond(full, lambda: general(sketches, assignment, medoid_ids), fast)


def solution(mesh):
    planes = mesh.shape["med"]
    mesh = jax.sharding.Mesh(
        mesh.devices.reshape(-1, planes // 2, 2), ("pts", *MED)
    )
    in_specs = (P("pts", None), P("pts"), P(MED))
    out_specs = (P("pts"), P(), P(MED), P("pts", MED))
    return jax.shard_map(
        shards, mesh=mesh, in_specs=in_specs, out_specs=out_specs, check_vma=False
    )
```

```python
import functools

import jax
import jax.numpy as jnp
from jax import lax
from jax.experimental import pallas as pl
from jax.experimental.pallas import tpu as pltpu
from jax.sharding import PartitionSpec as P


BF = jnp.bfloat16
F32 = jnp.float32
I32 = jnp.int32
LANES = 128
GRAD_ROWS = 192
GRAD_SLOTS = 176
MED_ROWS = 32
MED_SLOTS = 24
SEL = GRAD_ROWS + 2 * MED_ROWS
NONE = -1e30
LOST = 1e30
PTS = ("chip", "core")
MED = ("zq", "zr")
CHIPS = 4


def contract_last(a, b):
    return lax.dot_general(a, b, (((1,), (1,)), ((), ())), preferred_element_type=F32)


def pick_kernel(where_ref, assign_ref, ids_ref, sk_ref, med_ref, grad_ref, sel, code, held, arrived):
    flows, _, wide = held.shape

    def fetch(k):
        at = pl.ds(pl.multiple_of(k * wide, wide), wide)
        return pltpu.make_async_copy(sk_ref.at[:, at], held.at[k], arrived.at[k])

    for k in range(flows):
        fetch(k).start()

    def tables():
        base = where_ref[0]
        plane = where_ref[1]
        groups = assign_ref.shape[0]
        half = ids_ref.shape[1] // 2
        off = ids_ref[...] - base
        inside = (off >= 0) & (off < groups * LANES)
        hi = jnp.where(inside, off >> 7, -1)
        lo = off & (LANES - 1)
        j = lax.broadcasted_iota(I32, (1, 2 * half), 1)
        first = j < half
        number = (jnp.where(first, j, j - half) + 1).astype(F32)
        row = lax.broadcasted_iota(I32, (2 * groups, 2 * half), 0)
        wanted = jnp.where(first, hi, hi + groups)
        wanted = jnp.where(hi >= 0, wanted, -1)
        table = jnp.where(wanted == row, number, 0.0).astype(BF)
        lane_hot = (lo == lax.broadcasted_iota(I32, (LANES, 2 * half), 0)).astype(F32).astype(BF)
        medoid = contract_last(table, lane_hot)
        med0, med1 = medoid[:groups], medoid[groups:]
        local = assign_ref[...] - plane * (2 * half)
        mine = (local >= 0) & (local < 2 * half)
        local_lo = jnp.where(mine, (local & 255) + 1, 0).astype(F32)
        local_hi = jnp.where(mine, local >> 8, 0).astype(F32)
        flags = jnp.concatenate(
            [mine.astype(F32), (med0 > 0).astype(F32), (med1 > 0).astype(F32)], axis=0
        ).astype(BF)
        k = lax.broadcasted_iota(I32, (LANES, LANES), 0)
        b = lax.broadcasted_iota(I32, (LANES, LANES), 1)
        before = jnp.dot(flags, (k < b).astype(F32).astype(BF), preferred_element_type=F32)
        total = jnp.dot(flags, jnp.ones((LANES, LANES), BF), preferred_element_type=F32)
        slots, over = [], jnp.zeros((1, LANES), F32)
        for kind, limit in enumerate((GRAD_SLOTS, MED_SLOTS, MED_SLOTS)):
            run = jnp.zeros((1, LANES), F32)
            rows = []
            for g in range(groups):
                at = kind * groups + g
                rows.append(before[at : at + 1] + run)
                run = run + total[at : at + 1]
            over = over + jnp.where(run > limit, 1.0, 0.0)
            position = jnp.concatenate(rows, axis=0).astype(I32)
            flag = (mine, med0 > 0, med1 > 0)[kind] & (position < limit)
            slots.append(jnp.where(flag, position, -1))
        slot_g = slots[0]
        slot_m = jnp.where(slots[1] >= 0, slots[1], -1)
        slot_n = jnp.where(slots[2] >= 0, slots[2] + MED_ROWS, -1)
        grad_iota = lax.broadcasted_iota(I32, (GRAD_ROWS, LANES), 0)
        med_iota = lax.broadcasted_iota(I32, (2 * MED_ROWS, LANES), 0)
        codes = jnp.zeros((8, SEL), F32)
        zeros = jnp.zeros((5, LANES), F32)
        either = med0 + med1
        for g in range(groups):
            at = slice(g, g + 1)
            top = (slot_g[at] == grad_iota).astype(F32)
            low = ((slot_m[at] == med_iota) | (slot_n[at] == med_iota)).astype(F32)
            block = jnp.concatenate([top, low], axis=0).astype(BF)
            sel[:, g * LANES : (g + 1) * LANES] = block
            fields = jnp.concatenate(
                [either[at], local_lo[at], local_hi[at], zeros], axis=0
            ).astype(BF)
            codes = codes + contract_last(fields, block)
        marks = jnp.broadcast_to(jnp.concatenate([over, over], axis=1), (8, SEL))
        third = lax.broadcasted_iota(I32, (8, SEL), 0) == 3
        code[...] = jnp.where(third, marks, codes).astype(BF)

    tables()
    codes = code[...]
    lines = jnp.concatenate([codes[:, :LANES], codes[:, LANES:]], axis=0)

    @pl.loop(0, flows)
    def _(k):
        fetch(k).wait()
        for chip in range(wide // SEL):
            block = held[k, :, chip * SEL : (chip + 1) * SEL]
            rows = jnp.dot(sel[...], block, preferred_element_type=F32).astype(BF)
            for c in range(2):
                to = k * 2 * (wide // SEL) + 2 * chip + c
                grad_ref[to, :GRAD_SLOTS, :] = rows[:GRAD_SLOTS, c * LANES : (c + 1) * LANES]
                grad_ref[to, GRAD_SLOTS:, :] = lines
                at = GRAD_ROWS + c * MED_ROWS
                med_ref[to, :, :] = jnp.concatenate([rows[at : at + MED_SLOTS], codes], axis=0)


def pick(where, assignment, medoid_ids, sketches, pts_count):
    rows, feats = sketches.shape
    wide = CHIPS * 2 * LANES
    flows = feats // wide
    near = pl.BlockSpec(memory_space=pltpu.VMEM)
    return pl.pallas_call(
        pick_kernel,
        in_specs=[
            pl.BlockSpec(memory_space=pltpu.SMEM),
            near,
            near,
            pl.BlockSpec(memory_space=pl.ANY),
        ],
        out_specs=[near, near],
        scratch_shapes=[
            pltpu.VMEM((SEL, rows), BF),
            pltpu.VMEM((8, SEL), BF),
            pltpu.VMEM((flows, rows, wide), BF),
            pltpu.SemaphoreType.DMA((flows,)),
        ],
        out_shape=[
            jax.ShapeDtypeStruct((pts_count, MED_ROWS, 2 * LANES), BF),
            jax.ShapeDtypeStruct((pts_count, GRAD_ROWS, LANES), BF),
        ],
        compiler_params=pltpu.CompilerParams(vmem_limit_bytes=24 * 2**20),
        cost_estimate=pl.CostEstimate(
            flops=2 * SEL * rows * feats, bytes_accessed=rows * feats * 2, transcendentals=0
        ),
        name="pick",
    )(where, assignment.reshape(-1, LANES), medoid_ids[None, :], sketches)


def place_kernel(where_ref, got_ref, a_ref, b_ref, flag_ref):
    core = where_ref[2]
    sources = got_ref.shape[0]
    count = 2 * a_ref.shape[0]
    total = jnp.zeros((count, got_ref.shape[2]), F32)
    marks = jnp.zeros((1, LANES), F32)
    per = 2 * LANES // MED_ROWS
    iota = lax.broadcasted_iota(I32, (count, per * MED_ROWS), 0)
    for g in range(sources // per):
        numbers = []
        for q in range(g * per, (g + 1) * per):
            lines = got_ref[q, MED_SLOTS : MED_SLOTS + 8, :].astype(F32)
            line = lines[0:1]
            marks = marks + lines[3:4, :LANES]
            a = line[:, GRAD_ROWS : GRAD_ROWS + MED_ROWS]
            b = line[:, GRAD_ROWS + MED_ROWS :]
            numbers.append(jnp.where(core == 0, a, b))
        number = jnp.concatenate(numbers, axis=1).astype(I32) - 1
        hot = (number == iota).astype(F32).astype(BF)
        block = got_ref[g * per : (g + 1) * per].reshape(per * MED_ROWS, got_ref.shape[2])
        total = total + jnp.dot(hot, block, preferred_element_type=F32)
    a_ref[...] = total[: count // 2].astype(BF)
    b_ref[...] = total[count // 2 :].astype(BF)
    flag_ref[...] = jnp.concatenate([marks, marks], axis=1)


def place(where, got, count):
    return pl.pallas_call(
        place_kernel,
        in_specs=[
            pl.BlockSpec(memory_space=pltpu.SMEM),
            pl.BlockSpec(memory_space=pltpu.VMEM),
        ],
        out_specs=[pl.BlockSpec(memory_space=pltpu.VMEM)] * 3,
        out_shape=[
            jax.ShapeDtypeStruct((count // 2, got.shape[2]), BF),
            jax.ShapeDtypeStruct((count // 2, got.shape[2]), BF),
            jax.ShapeDtypeStruct((1, 2 * LANES), F32),
        ],
        compiler_params=pltpu.CompilerParams(vmem_limit_bytes=8 * 2**20),
        cost_estimate=pl.CostEstimate(
            flops=2 * count * got.size, bytes_accessed=2 * got.size, transcendentals=0
        ),
        name="place",
    )(where, got)


def sums_kernel(first, steps, got_ref, *refs):
    prior, (sums_ref, count_ref) = refs[:-2], refs[-2:]
    feats = got_ref.shape[2]
    medoids = sums_ref.shape[1]
    tail = GRAD_ROWS - LANES
    iota_a = lax.broadcasted_iota(I32, (medoids, LANES), 0)
    iota_b = lax.broadcasted_iota(I32, (medoids, tail), 0)
    ones = jnp.ones((GRAD_ROWS, LANES), BF)

    per = 4

    def body(step, total):
        hots, blocks = [], []
        for k in range(per):
            q = (first + step) * per + k
            codes = got_ref[q, GRAD_SLOTS:, :].astype(F32).astype(I32)
            a = codes[1:2] - 1 + codes[2:3] * 256
            b = (codes[9:10] - 1 + codes[10:11] * 256)[:, :tail]
            hots.append((a == iota_a).astype(F32))
            hots.append((b == iota_b).astype(F32))
            blocks.append(jnp.concatenate([got_ref[q], ones], axis=1))
        hot = jnp.concatenate(hots, axis=1).astype(BF)
        return total + jnp.dot(
            hot, jnp.concatenate(blocks, axis=0), preferred_element_type=F32
        )

    total = lax.fori_loop(
        0, steps, body, jnp.zeros((medoids, feats + LANES), F32)
    )
    sums, counts = total[:, :feats].T, total[:, feats:].T[:1]
    if prior:
        sums, counts = prior[0][...] + sums, prior[1][...] + counts
    sums_ref[...] = sums
    count_ref[...] = counts


def sums(got, medoids, first, steps, prior=()):
    return pl.pallas_call(
        functools.partial(sums_kernel, first, steps),
        in_specs=[pl.BlockSpec(memory_space=pltpu.VMEM)] * (1 + len(prior)),
        out_specs=[pl.BlockSpec(memory_space=pltpu.VMEM)] * 2,
        out_shape=[
            jax.ShapeDtypeStruct((got.shape[2], medoids), F32),
            jax.ShapeDtypeStruct((1, medoids), F32),
        ],
        compiler_params=pltpu.CompilerParams(vmem_limit_bytes=16 * 2**20),
        cost_estimate=pl.CostEstimate(
            flops=4 * medoids * got.size, bytes_accessed=2 * got.size, transcendentals=0
        ),
        name="sums",
    )(got, *prior)


def score_kernel(scale, where_ref, assign_ref, mark_ref, near_ref, far_ref, *refs):
    parts, (out_ref, held, arrived) = refs[:8], refs[8:]
    lost = mark_ref[...] > 0
    quarter, wide = parts[0].shape[1:]
    half = 2 * quarter
    x, y, base = where_ref[3], where_ref[4], where_ref[5]
    tile = 2 * LANES
    count = near_ref.shape[0] // tile

    def fetch(side, i):
        at = pl.ds(pl.multiple_of(i * tile, tile), tile)
        return pltpu.make_async_copy(
            (near_ref, far_ref)[side].at[at], held.at[side, at], arrived.at[side, i]
        )

    for side in range(2):
        for i in range(count):
            fetch(side, i).start()

    for side in range(2):

        @pl.loop(0, count)
        def _(i):
            fetch(side, i).wait()
            at = pl.ds(pl.multiple_of(i * tile, tile), tile)
            total = jnp.zeros((half, tile), F32)
            for kx in range(4):
                for ky in range(4):
                    block = ((x + 4 - kx) & 3) * 4 + ((y + 4 - ky) & 3)
                    columns = pl.ds(pl.multiple_of(block * wide, wide), wide)
                    total = total + contract_last(
                        jnp.concatenate([parts[ky][kx], parts[4 + kx][ky]], axis=0),
                        held[side, at, columns],
                    )
            scores = total * scale
            best = jnp.max(scores, axis=0, keepdims=True)
            row = lax.broadcasted_iota(I32, scores.shape, 0)
            local = assign_ref[side : side + 1, at] - base
            chosen = jnp.max(jnp.where(local == row, scores, NONE), axis=0, keepdims=True)
            out_ref[side : side + 1, at] = best
            out_ref[2 + side : 3 + side, at] = jnp.where(lost, LOST, chosen)


def scored(where, assignments, marks, near, far, parts):
    rows, feats = near.shape
    local = pl.BlockSpec(memory_space=pltpu.VMEM)
    away = pl.BlockSpec(memory_space=pl.ANY)
    return pl.pallas_call(
        functools.partial(score_kernel, 1.0 / feats),
        in_specs=[pl.BlockSpec(memory_space=pltpu.SMEM), local, local, away, away]
        + [local] * len(parts),
        out_specs=local,
        scratch_shapes=[
            pltpu.VMEM((2, rows, feats), BF),
            pltpu.SemaphoreType.DMA((2, rows // (2 * LANES))),
        ],
        out_shape=jax.ShapeDtypeStruct((4, rows), F32),
        compiler_params=pltpu.CompilerParams(vmem_limit_bytes=32 * 2**20),
        cost_estimate=pl.CostEstimate(
            flops=4 * rows * feats * 256, bytes_accessed=rows * feats * 4, transcendentals=0
        ),
        name="scored",
    )(where, assignments, marks, near, far, *parts)


def merge_kernel(a_ref, b_ref, c_ref, d_ref, all_ref, send_ref):
    same = jnp.maximum(a_ref[...], b_ref[...])
    partner = jnp.maximum(c_ref[...], d_ref[...])
    turned = jnp.concatenate([partner[1:2], partner[0:1], partner[3:4], partner[2:3]], axis=0)
    both = jnp.maximum(same, turned)
    all_ref[...] = both
    for i in range(send_ref.shape[0]):
        send_ref[i] = both[:2]


def merge(a, b, c, d, copies):
    return pl.pallas_call(
        merge_kernel,
        in_specs=[pl.BlockSpec(memory_space=pltpu.VMEM)] * 4,
        out_specs=[pl.BlockSpec(memory_space=pltpu.VMEM)] * 2,
        out_shape=[
            jax.ShapeDtypeStruct(a.shape, F32),
            jax.ShapeDtypeStruct((copies, 2, a.shape[1]), F32),
        ],
        compiler_params=pltpu.CompilerParams(vmem_limit_bytes=4 * 2**20),
        cost_estimate=pl.CostEstimate(
            flops=4 * a.size, bytes_accessed=4 * copies * a.size, transcendentals=0
        ),
        name="merge",
    )(a, b, c, d)


def closing_kernel(a_ref, b_ref, gap_ref, mark_ref):
    both = jnp.maximum(a_ref[...], b_ref[...])
    gap_ref[...] = both[0:1] - both[2:3]
    mark_ref[0, 0] = jnp.where(jnp.max(both[2:3]) > 0.5 * LOST, 1, 0)


def closing(a, b):
    return pl.pallas_call(
        closing_kernel,
        in_specs=[pl.BlockSpec(memory_space=pltpu.VMEM)] * 2,
        out_specs=[
            pl.BlockSpec(memory_space=pltpu.VMEM),
            pl.BlockSpec(memory_space=pltpu.SMEM),
        ],
        out_shape=[
            jax.ShapeDtypeStruct((1, a.shape[1]), F32),
            jax.ShapeDtypeStruct((1, 1), I32),
        ],
        compiler_params=pltpu.CompilerParams(vmem_limit_bytes=4 * 2**20),
        cost_estimate=pl.CostEstimate(
            flops=a.size, bytes_accessed=8 * a.size, transcendentals=0
        ),
        name="closing",
    )(a, b)


def cover_kernel(scale, got_ref, out_ref):
    total = jnp.zeros((1, got_ref.shape[2]), F32)
    for i in range(0, got_ref.shape[0], 2):
        best = jnp.maximum(got_ref[i], got_ref[i + 1])
        total = total + (best[0:1] + best[1:2])
    out_ref[0, 0] = jnp.sum(total) * scale


def cover(got):
    points = got.size // 2
    return pl.pallas_call(
        functools.partial(cover_kernel, 1.0 / points),
        in_specs=[pl.BlockSpec(memory_space=pltpu.VMEM)],
        out_specs=pl.BlockSpec(memory_space=pltpu.SMEM),
        out_shape=jax.ShapeDtypeStruct((1, 1), F32),
        compiler_params=pltpu.CompilerParams(vmem_limit_bytes=4 * 2**20),
        cost_estimate=pl.CostEstimate(
            flops=got.size, bytes_accessed=4 * got.size, transcendentals=0
        ),
        name="cover",
    )(got)


def from_everyone(array, axis):
    size = lax.axis_size(axis)
    return lax.all_to_all(
        jnp.broadcast_to(array[None], (size, *array.shape)), axis, 0, 0, tiled=True
    )


def chip_of(p):
    return p // 8, (p // 2) % 4, p % 2


def shifted(array, dx, dy, dc):
    pairs = []
    for p in range(32):
        x, y, c = chip_of(p)
        pairs.append((p, (((x + dx) % 4) * 4 + (y + dy) % 4) * 2 + (c ^ dc)))
    return lax.ppermute(array, PTS, pairs)


def across(array, core, step, planes):
    pairs = [
        (p * planes + z, (p ^ core) * planes + (z ^ step))
        for p in range(32)
        for z in range(planes)
    ]
    return lax.ppermute(array, (*PTS, *MED), pairs)


def general(sketches, assignment, medoid_ids):
    row_count, feat_width = sketches.shape
    medoid_count = medoid_ids.shape[0]
    pts_count = lax.axis_size(PTS)
    part = feat_width // pts_count
    pts_index = lax.axis_index(PTS)
    med_index = lax.axis_index(MED)
    local_assign = assignment - med_index * medoid_count
    chosen = local_assign[:, None] == jnp.arange(medoid_count, dtype=I32)[None, :]
    one_hot = chosen.astype(BF)
    offsets = medoid_ids - pts_index * row_count
    picking = offsets[:, None] == jnp.arange(row_count, dtype=I32)[None, :]
    terms = jnp.dot(picking.astype(BF), sketches, preferred_element_type=F32).astype(BF)
    terms = terms.reshape(medoid_count, pts_count, part).swapaxes(0, 1)
    piece = (
        lax.all_to_all(terms, PTS, 0, 0, tiled=True).astype(F32).sum(axis=0).astype(BF)
    )
    everything = from_everyone(piece, PTS).swapaxes(0, 1).reshape(medoid_count, feat_width)
    partial = lax.dot_general(
        sketches, one_hot, (((0,), (0,)), ((), ())), preferred_element_type=F32
    ).reshape(pts_count, part, medoid_count)
    gradient_sums = lax.all_to_all(partial, PTS, 0, 0, tiled=True).sum(axis=0)
    counts = from_everyone(jnp.sum(one_hot.astype(F32), axis=0), PTS).sum(axis=0)
    scores = contract_last(sketches, everything) * (1.0 / feat_width)
    best = jnp.max(scores, axis=1)
    taken = jnp.max(jnp.where(chosen, scores, NONE), axis=1)
    both = from_everyone(jnp.stack([best, taken]), MED).max(axis=0)
    cover = from_everyone(jnp.sum(both[0])[None], PTS).sum()
    return both[0] - both[1], cover / (row_count * pts_count), counts, gradient_sums


def shards(sketches, assignment, medoid_ids):
    row_count, _ = sketches.shape
    medoid_count = medoid_ids.shape[0]
    half = medoid_count // 2
    pts_count = lax.axis_size(PTS)
    p = lax.axis_index(PTS)
    m = lax.axis_index(MED)
    core = p % 2
    planes = lax.axis_size(MED)
    where = jnp.stack(
        [p * row_count, m, core, p // 8, (p // 2) % 4, m * medoid_count + core * half, m, m]
    ).astype(I32)

    far = shifted(sketches, 0, 0, 1)
    far_assignment = shifted(assignment, 0, 0, 1)
    med_send, grad_send = pick(
        where, assignment, medoid_ids, sketches, pts_count
    )
    med_got = lax.all_to_all(med_send, PTS, 0, 0, tiled=True)
    a, b, marks = place(where, med_got, half)
    pa = jnp.stack([a] + [shifted(a, k, 0, 0) for k in (1, 2, 3)])
    pb = jnp.stack([b] + [shifted(b, 0, k, 0) for k in (1, 2, 3)])
    qa = [pa, shifted(pa, 0, 1, 0)]
    qa = qa + [shifted(pa, 0, k, 0) for k in (2, 3)]
    qb = [pb] + [shifted(pb, k, 0, 0) for k in (1, 2, 3)]
    grad_got = lax.all_to_all(grad_send, PTS, 0, 0, tiled=True)
    assignments = jnp.stack([assignment, far_assignment])
    stats = scored(where, assignments, marks, sketches, far, qa + qb)
    stats = jnp.maximum(stats, across(stats, 0, 4, planes))
    near = across(stats, 0, 2, planes)
    partner, both = across(stats, 1, 0, planes), across(stats, 1, 2, planes)
    stats, send = merge(stats, near, partner, both, pts_count)
    everyone = lax.all_to_all(send, (PTS[0], MED[1]), 0, 0, tiled=True)
    plane = across(stats, 0, 1, planes)
    gradient_sums, counts = sums(grad_got, medoid_count, 0, 8)
    gap, mark = closing(stats, plane)
    full = mark[0, 0] > 0

    def fast():
        return gap[0], cover(everyone)[0, 0], counts[0], gradient_sums

    return lax.cond(full, lambda: general(sketches, assignment, medoid_ids), fast)


def solution(mesh):
    planes = mesh.shape["med"]
    mesh = jax.sharding.Mesh(
        mesh.devices.reshape(-1, 2, planes // 2, 2), (*PTS, *MED)
    )
    in_specs = (P(PTS, None), P(PTS), P(MED))
    out_specs = (P(PTS), P(), P(MED), P(PTS, MED))
    return jax.shard_map(
        shards, mesh=mesh, in_specs=in_specs, out_specs=out_specs, check_vma=False
    )
```

```python
import functools

import jax
import jax.numpy as jnp
from jax import lax
from jax.experimental import pallas as pl
from jax.experimental.pallas import tpu as pltpu
from jax.sharding import PartitionSpec as P


BF = jnp.bfloat16
F32 = jnp.float32
I32 = jnp.int32
LANES = 128
GRAD_ROWS = 192
GRAD_SLOTS = 176
MED_ROWS = 32
MED_SLOTS = 24
SEL = GRAD_ROWS + 2 * MED_ROWS
NONE = -1e30
LOST = 1e30
PTS = ("chip", "core")
MED = ("zr", "zq")
CHIPS = 2


def contract_last(a, b):
    return lax.dot_general(a, b, (((1,), (1,)), ((), ())), preferred_element_type=F32)


def pick_kernel(where_ref, assign_ref, ids_ref, sk_ref, med_ref, grad_ref, sel, code, held, arrived):
    flows, _, wide = held.shape

    def fetch(k):
        at = pl.ds(pl.multiple_of(k * wide, wide), wide)
        return pltpu.make_async_copy(sk_ref.at[:, at], held.at[k], arrived.at[k])

    for k in range(flows):
        fetch(k).start()

    def tables():
        base = where_ref[0]
        plane = where_ref[1]
        groups = assign_ref.shape[0]
        half = ids_ref.shape[1] // 2
        off = ids_ref[...] - base
        inside = (off >= 0) & (off < groups * LANES)
        hi = jnp.where(inside, off >> 7, -1)
        lo = off & (LANES - 1)
        j = lax.broadcasted_iota(I32, (1, 2 * half), 1)
        first = j < half
        number = (jnp.where(first, j, j - half) + 1).astype(F32)
        row = lax.broadcasted_iota(I32, (2 * groups, 2 * half), 0)
        wanted = jnp.where(first, hi, hi + groups)
        wanted = jnp.where(hi >= 0, wanted, -1)
        table = jnp.where(wanted == row, number, 0.0).astype(BF)
        lane_hot = (lo == lax.broadcasted_iota(I32, (LANES, 2 * half), 0)).astype(F32).astype(BF)
        medoid = contract_last(table, lane_hot)
        med0, med1 = medoid[:groups], medoid[groups:]
        local = assign_ref[...] - plane * (2 * half)
        mine = (local >= 0) & (local < 2 * half)
        local_lo = jnp.where(mine, (local & 255) + 1, 0).astype(F32)
        local_hi = jnp.where(mine, local >> 8, 0).astype(F32)
        flags = jnp.concatenate(
            [mine.astype(F32), (med0 > 0).astype(F32), (med1 > 0).astype(F32)], axis=0
        ).astype(BF)
        k = lax.broadcasted_iota(I32, (LANES, LANES), 0)
        b = lax.broadcasted_iota(I32, (LANES, LANES), 1)
        before = jnp.dot(flags, (k < b).astype(F32).astype(BF), preferred_element_type=F32)
        total = jnp.dot(flags, jnp.ones((LANES, LANES), BF), preferred_element_type=F32)
        slots, over = [], jnp.zeros((1, LANES), F32)
        for kind, limit in enumerate((GRAD_SLOTS, MED_SLOTS, MED_SLOTS)):
            run = jnp.zeros((1, LANES), F32)
            rows = []
            for g in range(groups):
                at = kind * groups + g
                rows.append(before[at : at + 1] + run)
                run = run + total[at : at + 1]
            over = over + jnp.where(run > limit, 1.0, 0.0)
            position = jnp.concatenate(rows, axis=0).astype(I32)
            flag = (mine, med0 > 0, med1 > 0)[kind] & (position < limit)
            slots.append(jnp.where(flag, position, -1))
        slot_g = slots[0]
        slot_m = jnp.where(slots[1] >= 0, slots[1], -1)
        slot_n = jnp.where(slots[2] >= 0, slots[2] + MED_ROWS, -1)
        grad_iota = lax.broadcasted_iota(I32, (GRAD_ROWS, LANES), 0)
        med_iota = lax.broadcasted_iota(I32, (2 * MED_ROWS, LANES), 0)
        codes = jnp.zeros((8, SEL), F32)
        zeros = jnp.zeros((5, LANES), F32)
        either = med0 + med1
        for g in range(groups):
            at = slice(g, g + 1)
            top = (slot_g[at] == grad_iota).astype(F32)
            low = ((slot_m[at] == med_iota) | (slot_n[at] == med_iota)).astype(F32)
            block = jnp.concatenate([top, low], axis=0).astype(BF)
            sel[:, g * LANES : (g + 1) * LANES] = block
            fields = jnp.concatenate(
                [either[at], local_lo[at], local_hi[at], zeros], axis=0
            ).astype(BF)
            codes = codes + contract_last(fields, block)
        marks = jnp.broadcast_to(jnp.concatenate([over, over], axis=1), (8, SEL))
        third = lax.broadcasted_iota(I32, (8, SEL), 0) == 3
        code[...] = jnp.where(third, marks, codes).astype(BF)

    tables()
    codes = code[...]
    lines = jnp.concatenate([codes[:, :LANES], codes[:, LANES:]], axis=0)

    @pl.loop(0, flows)
    def _(k):
        fetch(k).wait()
        for chip in range(wide // SEL):
            block = held[k, :, chip * SEL : (chip + 1) * SEL]
            rows = jnp.dot(sel[...], block, preferred_element_type=F32).astype(BF)
            for c in range(2):
                to = k * 2 * (wide // SEL) + 2 * chip + c
                grad_ref[to, :GRAD_SLOTS, :] = rows[:GRAD_SLOTS, c * LANES : (c + 1) * LANES]
                grad_ref[to, GRAD_SLOTS:, :] = lines
                at = GRAD_ROWS + c * MED_ROWS
                med_ref[to, :, :] = jnp.concatenate([rows[at : at + MED_SLOTS], codes], axis=0)


def pick(where, assignment, medoid_ids, sketches, pts_count):
    rows, feats = sketches.shape
    wide = CHIPS * 2 * LANES
    flows = feats // wide
    near = pl.BlockSpec(memory_space=pltpu.VMEM)
    return pl.pallas_call(
        pick_kernel,
        in_specs=[
            pl.BlockSpec(memory_space=pltpu.SMEM),
            near,
            near,
            pl.BlockSpec(memory_space=pl.ANY),
        ],
        out_specs=[near, near],
        scratch_shapes=[
            pltpu.VMEM((SEL, rows), BF),
            pltpu.VMEM((8, SEL), BF),
            pltpu.VMEM((flows, rows, wide), BF),
            pltpu.SemaphoreType.DMA((flows,)),
        ],
        out_shape=[
            jax.ShapeDtypeStruct((pts_count, MED_ROWS, 2 * LANES), BF),
            jax.ShapeDtypeStruct((pts_count, GRAD_ROWS, LANES), BF),
        ],
        compiler_params=pltpu.CompilerParams(vmem_limit_bytes=24 * 2**20),
        cost_estimate=pl.CostEstimate(
            flops=2 * SEL * rows * feats, bytes_accessed=rows * feats * 2, transcendentals=0
        ),
        name="pick",
    )(where, assignment.reshape(-1, LANES), medoid_ids[None, :], sketches)


def place_kernel(where_ref, got_ref, a_ref, b_ref, flag_ref):
    core = where_ref[2]
    sources = got_ref.shape[0]
    count = 2 * a_ref.shape[0]
    total = jnp.zeros((count, got_ref.shape[2]), F32)
    marks = jnp.zeros((1, LANES), F32)
    per = 2 * LANES // MED_ROWS
    iota = lax.broadcasted_iota(I32, (count, per * MED_ROWS), 0)
    for g in range(sources // per):
        numbers = []
        for q in range(g * per, (g + 1) * per):
            lines = got_ref[q, MED_SLOTS : MED_SLOTS + 8, :].astype(F32)
            line = lines[0:1]
            marks = marks + lines[3:4, :LANES]
            a = line[:, GRAD_ROWS : GRAD_ROWS + MED_ROWS]
            b = line[:, GRAD_ROWS + MED_ROWS :]
            numbers.append(jnp.where(core == 0, a, b))
        number = jnp.concatenate(numbers, axis=1).astype(I32) - 1
        hot = (number == iota).astype(F32).astype(BF)
        block = got_ref[g * per : (g + 1) * per].reshape(per * MED_ROWS, got_ref.shape[2])
        total = total + jnp.dot(hot, block, preferred_element_type=F32)
    a_ref[...] = total[: count // 2].astype(BF)
    b_ref[...] = total[count // 2 :].astype(BF)
    flag_ref[...] = jnp.concatenate([marks, marks], axis=1)


def place(where, got, count):
    return pl.pallas_call(
        place_kernel,
        in_specs=[
            pl.BlockSpec(memory_space=pltpu.SMEM),
            pl.BlockSpec(memory_space=pltpu.VMEM),
        ],
        out_specs=[pl.BlockSpec(memory_space=pltpu.VMEM)] * 3,
        out_shape=[
            jax.ShapeDtypeStruct((count // 2, got.shape[2]), BF),
            jax.ShapeDtypeStruct((count // 2, got.shape[2]), BF),
            jax.ShapeDtypeStruct((1, 2 * LANES), F32),
        ],
        compiler_params=pltpu.CompilerParams(vmem_limit_bytes=8 * 2**20),
        cost_estimate=pl.CostEstimate(
            flops=2 * count * got.size, bytes_accessed=2 * got.size, transcendentals=0
        ),
        name="place",
    )(where, got)


def sums_kernel(first, steps, got_ref, *refs):
    prior, (sums_ref, count_ref) = refs[:-2], refs[-2:]
    feats = got_ref.shape[2]
    medoids = sums_ref.shape[1]
    tail = GRAD_ROWS - LANES
    iota_a = lax.broadcasted_iota(I32, (medoids, LANES), 0)
    iota_b = lax.broadcasted_iota(I32, (medoids, tail), 0)
    ones = jnp.ones((GRAD_ROWS, LANES), BF)

    per = 4

    def body(step, total):
        hots, blocks = [], []
        for k in range(per):
            q = (first + step) * per + k
            codes = got_ref[q, GRAD_SLOTS:, :].astype(F32).astype(I32)
            a = codes[1:2] - 1 + codes[2:3] * 256
            b = (codes[9:10] - 1 + codes[10:11] * 256)[:, :tail]
            hots.append((a == iota_a).astype(F32))
            hots.append((b == iota_b).astype(F32))
            blocks.append(jnp.concatenate([got_ref[q], ones], axis=1))
        hot = jnp.concatenate(hots, axis=1).astype(BF)
        return total + jnp.dot(
            hot, jnp.concatenate(blocks, axis=0), preferred_element_type=F32
        )

    total = lax.fori_loop(
        0, steps, body, jnp.zeros((medoids, feats + LANES), F32)
    )
    sums, counts = total[:, :feats].T, total[:, feats:].T[:1]
    if prior:
        sums, counts = prior[0][...] + sums, prior[1][...] + counts
    sums_ref[...] = sums
    count_ref[...] = counts


def sums(got, medoids, first, steps, prior=()):
    return pl.pallas_call(
        functools.partial(sums_kernel, first, steps),
        in_specs=[pl.BlockSpec(memory_space=pltpu.VMEM)] * (1 + len(prior)),
        out_specs=[pl.BlockSpec(memory_space=pltpu.VMEM)] * 2,
        out_shape=[
            jax.ShapeDtypeStruct((got.shape[2], medoids), F32),
            jax.ShapeDtypeStruct((1, medoids), F32),
        ],
        compiler_params=pltpu.CompilerParams(vmem_limit_bytes=16 * 2**20),
        cost_estimate=pl.CostEstimate(
            flops=4 * medoids * got.size, bytes_accessed=2 * got.size, transcendentals=0
        ),
        name="sums",
    )(got, *prior)


def score_kernel(scale, where_ref, assign_ref, mark_ref, near_ref, far_ref, *refs):
    parts, (out_ref, held, arrived) = refs[:8], refs[8:]
    lost = mark_ref[...] > 0
    quarter, wide = parts[0].shape[1:]
    half = 2 * quarter
    x, y, base = where_ref[3], where_ref[4], where_ref[5]
    tile = 2 * LANES
    count = near_ref.shape[0] // tile

    def fetch(side, i):
        at = pl.ds(pl.multiple_of(i * tile, tile), tile)
        return pltpu.make_async_copy(
            (near_ref, far_ref)[side].at[at], held.at[side, at], arrived.at[side, i]
        )

    for side in range(2):
        for i in range(count):
            fetch(side, i).start()

    for side in range(2):

        @pl.loop(0, count)
        def _(i):
            fetch(side, i).wait()
            at = pl.ds(pl.multiple_of(i * tile, tile), tile)
            total = jnp.zeros((half, tile), F32)
            for kx in range(4):
                for ky in range(4):
                    block = ((x + 4 - kx) & 3) * 4 + ((y + 4 - ky) & 3)
                    columns = pl.ds(pl.multiple_of(block * wide, wide), wide)
                    total = total + contract_last(
                        jnp.concatenate([parts[ky][kx], parts[4 + kx][ky]], axis=0),
                        held[side, at, columns],
                    )
            scores = total * scale
            best = jnp.max(scores, axis=0, keepdims=True)
            row = lax.broadcasted_iota(I32, scores.shape, 0)
            local = assign_ref[side : side + 1, at] - base
            chosen = jnp.max(jnp.where(local == row, scores, NONE), axis=0, keepdims=True)
            out_ref[side : side + 1, at] = best
            out_ref[2 + side : 3 + side, at] = jnp.where(lost, LOST, chosen)


def scored(where, assignments, marks, near, far, parts):
    rows, feats = near.shape
    local = pl.BlockSpec(memory_space=pltpu.VMEM)
    away = pl.BlockSpec(memory_space=pl.ANY)
    return pl.pallas_call(
        functools.partial(score_kernel, 1.0 / feats),
        in_specs=[pl.BlockSpec(memory_space=pltpu.SMEM), local, local, away, away]
        + [local] * len(parts),
        out_specs=local,
        scratch_shapes=[
            pltpu.VMEM((2, rows, feats), BF),
            pltpu.SemaphoreType.DMA((2, rows // (2 * LANES))),
        ],
        out_shape=jax.ShapeDtypeStruct((4, rows), F32),
        compiler_params=pltpu.CompilerParams(vmem_limit_bytes=32 * 2**20),
        cost_estimate=pl.CostEstimate(
            flops=4 * rows * feats * 256, bytes_accessed=rows * feats * 4, transcendentals=0
        ),
        name="scored",
    )(where, assignments, marks, near, far, *parts)


def merge_kernel(a_ref, b_ref, c_ref, d_ref, all_ref, send_ref):
    same = jnp.maximum(a_ref[...], b_ref[...])
    partner = jnp.maximum(c_ref[...], d_ref[...])
    turned = jnp.concatenate([partner[1:2], partner[0:1], partner[3:4], partner[2:3]], axis=0)
    both = jnp.maximum(same, turned)
    all_ref[...] = both
    for i in range(send_ref.shape[0]):
        send_ref[i] = both[:2]


def merge(a, b, c, d, copies):
    return pl.pallas_call(
        merge_kernel,
        in_specs=[pl.BlockSpec(memory_space=pltpu.VMEM)] * 4,
        out_specs=[pl.BlockSpec(memory_space=pltpu.VMEM)] * 2,
        out_shape=[
            jax.ShapeDtypeStruct(a.shape, F32),
            jax.ShapeDtypeStruct((copies, 2, a.shape[1]), F32),
        ],
        compiler_params=pltpu.CompilerParams(vmem_limit_bytes=4 * 2**20),
        cost_estimate=pl.CostEstimate(
            flops=4 * a.size, bytes_accessed=4 * copies * a.size, transcendentals=0
        ),
        name="merge",
    )(a, b, c, d)


def closing_kernel(a_ref, b_ref, gap_ref, mark_ref):
    both = jnp.maximum(a_ref[...], b_ref[...])
    gap_ref[...] = both[0:1] - both[2:3]
    mark_ref[0, 0] = jnp.where(jnp.max(both[2:3]) > 0.5 * LOST, 1, 0)


def closing(a, b):
    return pl.pallas_call(
        closing_kernel,
        in_specs=[pl.BlockSpec(memory_space=pltpu.VMEM)] * 2,
        out_specs=[
            pl.BlockSpec(memory_space=pltpu.VMEM),
            pl.BlockSpec(memory_space=pltpu.SMEM),
        ],
        out_shape=[
            jax.ShapeDtypeStruct((1, a.shape[1]), F32),
            jax.ShapeDtypeStruct((1, 1), I32),
        ],
        compiler_params=pltpu.CompilerParams(vmem_limit_bytes=4 * 2**20),
        cost_estimate=pl.CostEstimate(
            flops=a.size, bytes_accessed=8 * a.size, transcendentals=0
        ),
        name="closing",
    )(a, b)


def cover_kernel(scale, got_ref, out_ref):
    total = jnp.zeros((1, got_ref.shape[2]), F32)
    for i in range(0, got_ref.shape[0], 2):
        best = jnp.maximum(got_ref[i], got_ref[i + 1])
        total = total + (best[0:1] + best[1:2])
    out_ref[0, 0] = jnp.sum(total) * scale


def cover(got):
    points = got.size // 2
    return pl.pallas_call(
        functools.partial(cover_kernel, 1.0 / points),
        in_specs=[pl.BlockSpec(memory_space=pltpu.VMEM)],
        out_specs=pl.BlockSpec(memory_space=pltpu.SMEM),
        out_shape=jax.ShapeDtypeStruct((1, 1), F32),
        compiler_params=pltpu.CompilerParams(vmem_limit_bytes=4 * 2**20),
        cost_estimate=pl.CostEstimate(
            flops=got.size, bytes_accessed=4 * got.size, transcendentals=0
        ),
        name="cover",
    )(got)


def from_everyone(array, axis):
    size = lax.axis_size(axis)
    return lax.all_to_all(
        jnp.broadcast_to(array[None], (size, *array.shape)), axis, 0, 0, tiled=True
    )


def chip_of(p):
    return p // 8, (p // 2) % 4, p % 2


def shifted(array, dx, dy, dc):
    pairs = []
    for p in range(32):
        x, y, c = chip_of(p)
        pairs.append((p, (((x + dx) % 4) * 4 + (y + dy) % 4) * 2 + (c ^ dc)))
    return lax.ppermute(array, PTS, pairs)


def across(array, core, step, planes):
    pairs = [
        (p * planes + z, (p ^ core) * planes + (z ^ step))
        for p in range(32)
        for z in range(planes)
    ]
    return lax.ppermute(array, (*PTS, *MED), pairs)


def general(sketches, assignment, medoid_ids):
    row_count, feat_width = sketches.shape
    medoid_count = medoid_ids.shape[0]
    pts_count = lax.axis_size(PTS)
    part = feat_width // pts_count
    pts_index = lax.axis_index(PTS)
    med_index = lax.axis_index(MED)
    local_assign = assignment - med_index * medoid_count
    chosen = local_assign[:, None] == jnp.arange(medoid_count, dtype=I32)[None, :]
    one_hot = chosen.astype(BF)
    offsets = medoid_ids - pts_index * row_count
    picking = offsets[:, None] == jnp.arange(row_count, dtype=I32)[None, :]
    terms = jnp.dot(picking.astype(BF), sketches, preferred_element_type=F32).astype(BF)
    terms = terms.reshape(medoid_count, pts_count, part).swapaxes(0, 1)
    piece = (
        lax.all_to_all(terms, PTS, 0, 0, tiled=True).astype(F32).sum(axis=0).astype(BF)
    )
    everything = from_everyone(piece, PTS).swapaxes(0, 1).reshape(medoid_count, feat_width)
    partial = lax.dot_general(
        sketches, one_hot, (((0,), (0,)), ((), ())), preferred_element_type=F32
    ).reshape(pts_count, part, medoid_count)
    gradient_sums = lax.all_to_all(partial, PTS, 0, 0, tiled=True).sum(axis=0)
    counts = from_everyone(jnp.sum(one_hot.astype(F32), axis=0), PTS).sum(axis=0)
    scores = contract_last(sketches, everything) * (1.0 / feat_width)
    best = jnp.max(scores, axis=1)
    taken = jnp.max(jnp.where(chosen, scores, NONE), axis=1)
    both = from_everyone(jnp.stack([best, taken]), MED).max(axis=0)
    cover = from_everyone(jnp.sum(both[0])[None], PTS).sum()
    return both[0] - both[1], cover / (row_count * pts_count), counts, gradient_sums


def shards(sketches, assignment, medoid_ids):
    row_count, _ = sketches.shape
    medoid_count = medoid_ids.shape[0]
    half = medoid_count // 2
    pts_count = lax.axis_size(PTS)
    p = lax.axis_index(PTS)
    m = lax.axis_index(MED)
    core = p % 2
    planes = lax.axis_size(MED)
    where = jnp.stack(
        [p * row_count, m, core, p // 8, (p // 2) % 4, m * medoid_count + core * half, m, m]
    ).astype(I32)

    far = shifted(sketches, 0, 0, 1)
    far_assignment = shifted(assignment, 0, 0, 1)
    med_send, grad_send = pick(
        where, assignment, medoid_ids, sketches, pts_count
    )
    med_got = lax.all_to_all(med_send, PTS, 0, 0, tiled=True)
    a, b, marks = place(where, med_got, half)
    pa = jnp.stack([a] + [shifted(a, k, 0, 0) for k in (1, 2, 3)])
    pb = jnp.stack([b] + [shifted(b, 0, k, 0) for k in (1, 2, 3)])
    qa = [pa, shifted(pa, 0, 1, 0)]
    qa = qa + [shifted(pa, 0, k, 0) for k in (2, 3)]
    qb = [pb] + [shifted(pb, k, 0, 0) for k in (1, 2, 3)]
    grad_got = lax.all_to_all(grad_send, PTS, 0, 0, tiled=True)
    assignments = jnp.stack([assignment, far_assignment])
    stats = scored(where, assignments, marks, sketches, far, qa + qb)
    stats = jnp.maximum(stats, across(stats, 0, 1, planes))
    near = across(stats, 0, 2, planes)
    partner, both = across(stats, 1, 0, planes), across(stats, 1, 2, planes)
    stats, send = merge(stats, near, partner, both, pts_count)
    everyone = lax.all_to_all(send, (PTS[0], MED[0]), 0, 0, tiled=True)
    plane = across(stats, 0, planes // 2, planes)
    gradient_sums, counts = sums(grad_got, medoid_count, 0, 8)
    gap, mark = closing(stats, plane)
    full = mark[0, 0] > 0

    def fast():
        return gap[0], cover(everyone)[0, 0], counts[0], gradient_sums

    return lax.cond(full, lambda: general(sketches, assignment, medoid_ids), fast)


def solution(mesh):
    planes = mesh.shape["med"]
    mesh = jax.sharding.Mesh(
        mesh.devices.reshape(-1, 2, 2, planes // 2), (*PTS, *MED)
    )
    in_specs = (P(PTS, None), P(PTS), P(MED))
    out_specs = (P(PTS), P(), P(MED), P(PTS, MED))
    return jax.shard_map(
        shards, mesh=mesh, in_specs=in_specs, out_specs=out_specs, check_vma=False
    )
```
